256 devices in a mesh: group: 2 (over core), gx: 16 (over y, x), gy: 8 (over z).
Axes of the slice: x: 4, y: 4, z: 8, core: 2. Of those that a mesh axis runs over, the one named last changes fastest.
Arguments:
- forcing: float32 [2, 80, 128, 2048], P('group', None, 'gx', 'gy'), may hold values from -24 to 24
- conduct: bfloat16 [2, 80, 128, 2048], P('group', None, 'gx', 'gy'), may hold values from 0.25 to 4
- diag_add: bfloat16 [2, 80, 128, 2048], P('group', None, 'gx', 'gy'), may hold values from 0.049804688 to 0.5
- ice_mask: int32 [128, 2048], P('gx', 'gy'), may hold values 0 or 1
- grounded: int32 [128, 2048], P('gx', 'gy'), may hold values 0 or 1
Outputs:
- solution: float32 [2, 80, 128, 2048], P('group', None, 'gx', 'gy')
- residual: float32 [2, 80, 128, 2048], P('group', None, 'gx', 'gy')
The draws below stay inside these ranges and needn't reach their ends.
All inputs are finite; a program needn't handle non-finite values. No bound on the sum of `ice_mask` or of `grounded` on one device may be relied on, other than what follows from the above.
Results may differ from the reference program's by a relative error of at most 0.0003.
Values sent between devices are 32-bit elements; how exact they have to be, the bound alone decides.
A program may use at most 64 MiB of HBM per device.

```python
import math
import jax
import jax.numpy as jnp
from jax import lax

LAYERS = 80
ITERS = 6
NX = 128
NY = 2048


def place_ends(result, own_key, low, high):
    longest = result.shape.index(max(result.shape))
    spots = []
    for shift in (0, 1):
        where = [jax.random.randint(jax.random.fold_in(own_key, axis), (), 0, length) for axis, length in enumerate(result.shape)]
        where[longest] = (where[longest] + shift) % result.shape[longest]
        spots.append(tuple(where))
    return result.at[spots[0]].set(low).at[spots[1]].set(high)


def steps_of(key, dims, cuts, low, largest):
    def one(dim, parts):
        steps = jax.random.uniform(jax.random.fold_in(jax.random.fold_in(key, 6), dim), (parts,), jnp.float32, low / len(cuts), largest / len(cuts))
        return jnp.repeat(jnp.exp(steps), dims[dim] // parts).reshape((-1,) + (1,) * (len(dims) - dim - 1))

    loudness = one(*cuts[0])
    for cut in cuts[1:]:
        loudness = loudness * one(*cut)
    return loudness


def noise(stream_key, shape, scale, most, pieces=(), held_as=jnp.bfloat16):
    entries = jax.random.normal(stream_key, shape, jnp.float32) * scale
    if len(pieces) > 0:
        entries = steps_of(stream_key, shape, pieces, -0.22, 0.18) * entries
    return jnp.clip(entries, min=-most, max=most).astype(held_as)


def setup_inputs(seed: int = 0) -> dict:
    streams_of = jax.random.split(jax.random.key(seed), 6)
    forcing = noise(streams_of[0], (2, LAYERS, NX, NY), 4.0, 24.0, ((0, 2), (2, 16), (3, 8)), jnp.float32)
    conduct = jnp.clip(jnp.exp(math.log(4.0) - 2.7725887 * jax.random.uniform(streams_of[1], (2, LAYERS, NX, NY), jnp.float32) ** steps_of(streams_of[1], (2, LAYERS, NX, NY), ((0, 2), (2, 16), (3, 8)), -0.2, 0.2)), 0.25, 4.0).astype(jnp.bfloat16)
    diag_add = jnp.clip(jnp.exp(math.log(0.5) - 2.306499 * jax.random.uniform(streams_of[2], (2, LAYERS, NX, NY), jnp.float32) ** steps_of(streams_of[2], (2, LAYERS, NX, NY), ((0, 2), (2, 16), (3, 8)), -0.2, 0.2)), 0.049804688, 0.5).astype(jnp.bfloat16)
    ice_mask = place_ends((jax.random.randint(streams_of[3], (NX, NY), 0, 8) < 7).astype(jnp.int32), jax.random.fold_in(streams_of[3], 1), 0, 1)
    grounded = place_ends((jax.random.randint(streams_of[4], (NX, NY), 0, 8) < 3).astype(jnp.int32), jax.random.fold_in(streams_of[4], 1), 0, 1)
    return dict(forcing=forcing, conduct=conduct, diag_add=diag_add, ice_mask=ice_mask, grounded=grounded)


far_weight = 0.25
cross_weight = 0.5
vertical_weight = 4.0
friction_gain = 8.0
NEIGHBOURS = ((1, 0, 1.0), (-1, 0, 1.0), (0, 1, 1.0), (0, -1, 1.0), (2, 0, far_weight), (-2, 0, far_weight), (0, 2, far_weight), (0, -2, far_weight), (1, 1, cross_weight), (1, -1, cross_weight), (-1, 1, cross_weight), (-1, -1, cross_weight))

def beside_sum(padded, extent_x, extent_y):
    summed = jnp.zeros((padded.shape[0], extent_x, extent_y), jnp.float32)
    for shift_x, shift_y, weight in NEIGHBOURS:
        summed = summed + weight * padded[:, 2 + shift_x:2 + shift_x + extent_x, 2 + shift_y:2 + shift_y + extent_y]
    return summed

def vertical_sum(values):
    zeroes = jnp.zeros_like(values[:1])
    return jnp.concatenate([values[1:], zeroes], 0) + jnp.concatenate([zeroes, values[:-1]], 0)

def spread(values):
    padded = jnp.pad(values, ((0, 0), (2, 2), (2, 2)))
    return beside_sum(padded, values.shape[1], values.shape[2]) + vertical_weight * vertical_sum(values)

def group_setup(group_id, forcing, conduct, diag_add, ice_mask, grounded):
    ice_cells = ice_mask.astype(jnp.float32)
    ground_cells = grounded.astype(jnp.float32)
    if group_id == 0:
        active = ice_cells
    else:
        active = ice_cells * (1.0 - ground_cells)
    layers = forcing.shape[1]
    coupling = jnp.sqrt(conduct[group_id].astype(jnp.float32)) * active
    base_diag = diag_add[group_id].astype(jnp.float32)
    if group_id == 0:
        base_diag = base_diag.at[0].add(friction_gain * ground_cells * ice_cells)
    diagonal = base_diag + coupling * spread(coupling)
    edge_layer = 0 if group_id == 0 else layers - 1
    shared_value = active * lax.optimization_barrier(jnp.mean(forcing[group_id], axis=0))
    shared_weight = coupling[edge_layer]
    return (active, coupling, diagonal, edge_layer, shared_value, shared_weight)

def solve(source, coupling, diagonal):
    inverse = 1.0 / diagonal
    solution = jnp.zeros_like(source)
    residual = source
    precond = inverse * residual
    direction = precond
    norm_now = jnp.sum(residual * precond)
    for iteration in range(ITERS):
        applied = diagonal * direction - coupling * spread(coupling * direction)
        step_size = norm_now / jnp.sum(direction * applied)
        solution = solution + step_size * direction
        residual = residual - step_size * applied
        if iteration + 1 < ITERS:
            precond = inverse * residual
            norm_next = jnp.sum(residual * precond)
            direction = precond + norm_next / norm_now * direction
            norm_now = norm_next
    return (solution, residual)

def reference(forcing, conduct, diag_add, ice_mask, grounded):
    setups = [group_setup(group_id, forcing, conduct, diag_add, ice_mask, grounded) for group_id in (0, 1)]
    solutions = []
    residuals = []
    for group_id in (0, 1):
        active, coupling, diagonal, edge_layer, shared_value, shared_weight = setups[group_id]
        partner = setups[1 - group_id]
        source = active * forcing[group_id]
        source = source.at[edge_layer].add(active * partner[5] * partner[4])
        solution, residual = solve(source, coupling, diagonal)
        solutions.append(solution)
        residuals.append(residual)
    return (jnp.stack(solutions), jnp.stack(residuals))
```

```python
import functools

import jax
import jax.numpy as jnp
from jax import lax
from jax.experimental import pallas as pl
from jax.experimental.pallas import tpu as pltpu
from jax.sharding import PartitionSpec as P

ITERS = 6
FIELDS = ITERS + 1
LAYERS = 80
ROWS = 8
SUB = 8
LANES = 128
TILES = 2
CHUNKS = LAYERS // SUB
MESH = pl.DeviceIdType.MESH
F32 = jnp.float32

far_weight = 0.25
cross_weight = 0.5
vertical_weight = 4.0
friction_gain = 8.0

STEPS = ((-1, 0), (1, 0), (0, -1), (0, 1), (-1, -1), (-1, 1), (1, -1), (1, 1))


def roll(value, shift, axis=None):
    return pltpu.roll(value, shift % value.shape[-1 if axis is None else axis],
                      value.ndim - 1 if axis is None else axis)


def unskew(value, step, sub):
    for bit in (1, 2, 4):
        value = jnp.where((sub & bit) != 0, roll(value, -step * bit), value)
    return value


def kernel(
    nx, nz,
    forcing, conduct, diag_add, ice_mask, grounded, out_x, out_r,
    cbf, dbf, ice_v, ground_v, active_v, fs, cn, dn,
    wbuf, hx, hz, hc, pz, pc, ebuf, hbuf, icbuf, gbuf, hwbuf, acc,
    shared_out, shared_in, ar_own, ar_x, ar_own2, ar_z, xs, rs,
    in_sem, out_sem, send_sem, recv_sem, share_sem, ar_sem,
):
    g = lax.axis_index("group")
    x = lax.axis_index("gx")
    z = lax.axis_index("gy")

    lane2 = lax.broadcasted_iota(jnp.int32, (SUB, LANES), 1)
    sub2 = lax.broadcasted_iota(jnp.int32, (SUB, LANES), 0)
    lane3 = lax.broadcasted_iota(jnp.int32, (ROWS, SUB, LANES), 2)
    sub3 = lax.broadcasted_iota(jnp.int32, (ROWS, SUB, LANES), 1)
    lane1 = lax.broadcasted_iota(jnp.int32, (1, LANES), 1)

    def exists(d):
        dx, dz = STEPS[d]
        conds = []
        if dx < 0:
            conds.append(x > 0)
        if dx > 0:
            conds.append(x < nx - 1)
        if dz < 0:
            conds.append(z > 0)
        if dz > 0:
            conds.append(z < nz - 1)
        return functools.reduce(jnp.logical_and, conds)

    def at(d):
        dx, dz = STEPS[d]
        return (g, x + dx, z + dz)

    loads = [
        pltpu.make_async_copy(conduct, cbf, in_sem.at[0]),
        pltpu.make_async_copy(ice_mask, ice_v, in_sem.at[1]),
        pltpu.make_async_copy(grounded, ground_v, in_sem.at[2]),
        pltpu.make_async_copy(forcing.at[:, pl.ds(0, LANES)], fs.at[0], in_sem.at[3]),
        pltpu.make_async_copy(forcing.at[:, pl.ds(LANES, LANES)], fs.at[1], in_sem.at[4]),
        pltpu.make_async_copy(diag_add, dbf, in_sem.at[5]),
    ]
    for load in loads:
        load.start()

    def zero_rims(d):
        @pl.when(jnp.logical_not(exists(d)))
        def _():
            def body(e, carry):
                if d < 2:
                    for j in range(CHUNKS):
                        hx[e, j, d] = jnp.zeros((2, TILES, SUB, LANES), F32)
                elif d < 4:
                    hz[e, :, d - 2] = jnp.zeros((CHUNKS, SUB, LANES), F32)
                else:
                    hc[e, :, d - 4] = jnp.zeros((CHUNKS, 1, LANES), F32)
                return carry
            lax.fori_loop(0, FIELDS, body, 0)

    for d in range(8):
        zero_rims(d)

    barrier = pltpu.get_barrier_semaphore()

    def greet_x(i, carry):
        @pl.when(i != x)
        def _():
            pl.semaphore_signal(barrier, inc=1, device_id=(g, i, z), device_id_type=MESH)
        return carry

    def greet_z(i, carry):
        @pl.when(i != z)
        def _():
            pl.semaphore_signal(barrier, inc=1, device_id=(g, x, i), device_id_type=MESH)
        return carry

    lax.fori_loop(0, nx, greet_x, 0)
    lax.fori_loop(0, nz, greet_z, 0)
    pl.semaphore_signal(barrier, inc=1, device_id=(1 - g, x, z), device_id_type=MESH)
    for d in range(4, 8):
        @pl.when(exists(d))
        def _(d=d):
            pl.semaphore_signal(barrier, inc=1, device_id=at(d), device_id_type=MESH)

    acc[...] = jnp.zeros_like(acc)

    loads[0].wait()
    loads[1].wait()
    loads[2].wait()
    is_ice = jnp.where(g == 0, 1.0, 0.0).astype(F32)
    ice = ice_v[...].astype(F32)
    ground = ground_v[...].astype(F32)
    active_v[...] = ice * (1.0 - (1.0 - is_ice) * ground)

    def couple(i, carry):
        part = pl.ds(pl.multiple_of(i * SUB * ROWS, SUB * ROWS), SUB * ROWS)
        for t in range(TILES):
            columns = slice(t * LANES, (t + 1) * LANES)
            value = jnp.sqrt(cbf[part, columns].astype(F32)).reshape(SUB, ROWS, LANES)
            cn[t, part] = (value * active_v[:, columns][None]).reshape(SUB * ROWS, LANES)
        return carry

    lax.fori_loop(0, CHUNKS, couple, 0)

    beside_x = (x > 0).astype(jnp.int32) + (x < nx - 1).astype(jnp.int32)
    beside_z = (z > 0).astype(jnp.int32) + (z < nz - 1).astype(jnp.int32)
    pl.semaphore_wait(barrier, nx + nz - 1 + beside_x * beside_z)

    def pick(ref, j, t):
        return jnp.stack([ref[t, pl.ds(j * ROWS + r, SUB, stride=CHUNKS * ROWS), :] for r in range(ROWS)])

    def put(ref, j, t, value):
        for r in range(ROWS):
            ref[t, pl.ds(j * ROWS + r, SUB, stride=CHUNKS * ROWS), :] = value[r]

    def copies(e, j, d):
        if d == 0:
            src, dst = wbuf.at[e, j + 1, pl.ds(0, 2)], hx.at[e, j, 1]
        elif d == 1:
            src, dst = wbuf.at[e, j + 1, pl.ds(ROWS - 2, 2)], hx.at[e, j, 0]
        elif d < 4:
            src, dst = pz.at[e, j], hz.at[e, j, 3 - d]
        else:
            src, dst = pc.at[e, j], hc.at[e, j, 7 - d]
        opposite = (1, 0, 3, 2, 7, 6, 5, 4)[d]
        return pltpu.make_async_remote_copy(
            src_ref=src, dst_ref=dst, send_sem=send_sem.at[d],
            recv_sem=recv_sem.at[e, j, opposite], device_id=at(d), device_id_type=MESH)

    def store_field(e, j, parts):
        for t in range(TILES):
            wbuf[e, j + 1, :, t] = parts[t]

        @pl.when(j == 0)
        def _():
            for t in range(TILES):
                wbuf[e, CHUNKS + 1, :, t] = jnp.where(sub3 < SUB - 1, roll(parts[t], SUB - 1, 1), 0.0)

        @pl.when(j == CHUNKS - 1)
        def _():
            for t in range(TILES):
                wbuf[e, 0, :, t] = jnp.where(sub3 > 0, roll(parts[t], 1, 1), 0.0)

    def send_field(e, j, parts):
        rims = jnp.where(lane3 < 2, parts[0], jnp.where(lane3 >= LANES - 2, parts[1], 0.0))
        packed = roll(rims[0], 4)
        for r in range(1, ROWS):
            packed = packed + roll(rims[r], 4 * (r + 1))
        pz[e, j] = packed
        corner = (lane2 == 3) | (lane2 == 4) | (lane2 == 31) | (lane2 == 32)
        spreaded = pltpu.roll(jnp.where(corner, packed, 0.0), 0, 1, stride=2, stride_axis=0)
        pc[e, j] = jnp.sum(spreaded, axis=0, keepdims=True)
        for d in range(8):
            @pl.when(exists(d))
            def _(d=d):
                copies(e, j, d).start()

    def await_rims(e, j):
        for d in range(8):
            @pl.when(exists(d))
            def _(d=d):
                opposite = (1, 0, 3, 2, 7, 6, 5, 4)[d]
                copies(e, j, opposite).wait_recv()

    def spread(e, j):
        centre = [wbuf[e, j + 1, :, t] for t in range(TILES)]
        beside, mixed = [], []
        for t in range(TILES):
            wide = jnp.concatenate([hx[e, j, 0, :, t], centre[t], hx[e, j, 1, :, t]], axis=0)
            near = wide[1:9] + wide[3:11]
            far = wide[0:8] + wide[4:12]
            vertical = wbuf[e, j, :, t] + wbuf[e, j + 2, :, t]
            beside.append(near + far_weight * far + vertical_weight * vertical)
            mixed.append(centre[t] + cross_weight * near)
        first, last = lane3 == 0, lane3 == LANES - 1

        def from_left(pair):
            a, b = roll(pair[0], 1), roll(pair[1], 1)
            return [jnp.where(first, 0.0, a), jnp.where(first, a, b)]

        def from_right(pair):
            a, b = roll(pair[0], -1), roll(pair[1], -1)
            return [jnp.where(last, b, a), jnp.where(last, 0.0, b)]

        for shift in (from_left, from_right):
            once = shift(centre)
            twice = shift([mixed[t] + far_weight * once[t] for t in range(TILES)])
            beside = [beside[t] + twice[t] for t in range(TILES)]

        place = lane2 % 4
        rims = jnp.where(place < 2, roll(hz[e, j, 0], 2), roll(hz[e, j, 1], -2))
        crossed = rims + cross_weight * (roll(rims, 4) + roll(rims, -4))
        edge = far_weight * rims + jnp.where(
            place == 0, roll(crossed, -1), jnp.where(place == 3, roll(crossed, 1), 0.0))
        odd = lane1 % 2 == 1
        corners = jnp.where(
            lane1 >= 31,
            jnp.where(odd, hc[e, j, 0], hc[e, j, 1]),
            jnp.where(odd, hc[e, j, 2], hc[e, j, 3]))
        corners = unskew(jnp.broadcast_to(corners, (SUB, LANES)), 2, sub2)
        edge = edge + cross_weight * jnp.where(
            lane2 == 4, roll(corners, -27), jnp.where(
                lane2 == 3, roll(corners, -29), jnp.where(
                    lane2 == 32, roll(corners, 29), jnp.where(
                        lane2 == 31, roll(corners, 27), 0.0))))
        rows = jnp.stack([roll(edge, -4 * (r + 1)) for r in range(ROWS)])
        return [beside[0] + jnp.where(lane3 < 2, rows, 0.0),
                beside[1] + jnp.where(lane3 >= LANES - 2, rows, 0.0)]

    def dots(k, j, parts):
        for t in range(TILES):
            hwbuf[:, t] = hbuf[j, :, t] * parts[t]

        def body(i, carry):
            product = jnp.sum(hwbuf[...] * wbuf[i + 1, j + 1], axis=(0, 1))
            total = acc[k, i] + product
            acc[k, i] = total
            acc[i, k] = total
            return carry

        lax.fori_loop(0, k + 1, body, 0)

    def first(j, carry):
        parts = [pick(cn, j, t) for t in range(TILES)]
        store_field(0, j, parts)
        send_field(0, j, parts)
        return carry

    lax.fori_loop(0, CHUNKS, first, 0)

    loads[3].wait()
    loads[4].wait()
    edge = pl.ds(pl.multiple_of(g * ((LAYERS - 1) * ROWS), ROWS), ROWS)
    for t in range(TILES):
        mean = jnp.sum(fs[t].reshape(LAYERS, ROWS, LANES), axis=0) * (1.0 / LAYERS)
        value = active_v[:, t * LANES:(t + 1) * LANES] * mean
        shared_out[t] = value * cn[t, edge]
    share = pltpu.make_async_remote_copy(
        src_ref=shared_out, dst_ref=shared_in, send_sem=share_sem.at[0], recv_sem=share_sem.at[1],
        device_id=(1 - g, x, z), device_id_type=MESH)
    share.start()
    loads[5].wait()

    def widen(i, carry):
        part = pl.ds(pl.multiple_of(i * SUB * ROWS, SUB * ROWS), SUB * ROWS)
        for t in range(TILES):
            dn[t, part] = dbf[part, t * LANES:(t + 1) * LANES].astype(F32)
        return carry

    lax.fori_loop(0, CHUNKS, widen, 0)
    share.wait()
    for t in range(TILES):
        columns = slice(t * LANES, (t + 1) * LANES)
        friction = is_ice * friction_gain * (ground_v[:, columns].astype(F32) * ice_v[:, columns].astype(F32))
        dn[t, 0:ROWS] = dn[t, 0:ROWS] + friction
        fs[t, edge] = fs[t, edge] + shared_in[t]

    def second(j, carry):
        await_rims(0, j)
        spreads = spread(0, j)
        parts = []
        for t in range(TILES):
            c = wbuf[0, j + 1, :, t]
            diagonal = pick(dn, j, t) + c * spreads[t]
            ratio = c / diagonal
            inverse_c = jnp.where(c > 0.0, 1.0 / jnp.where(c > 0.0, c, 1.0), 0.0)
            back = diagonal * inverse_c
            ebuf[j, :, t] = ratio * c
            icbuf[j, :, t] = inverse_c
            gbuf[j, :, t] = back
            hbuf[j, :, t] = back * inverse_c
            parts.append(ratio * pick(fs, j, t))
        store_field(1, j, parts)
        send_field(1, j, parts)
        dots(0, j, parts)
        return carry

    lax.fori_loop(0, CHUNKS, second, 0)

    def stage(k, carry):
        gain = jnp.where(k == 1, 1.0, 2.0).astype(F32)
        keep = jnp.where(k == 1, 0.0, 1.0).astype(F32)

        def body(j, inner):
            await_rims(k, j)
            spreads = spread(k, j)
            parts = [gain * (ebuf[j, :, t] * spreads[t]) - keep * wbuf[k - 1, j + 1, :, t]
                     for t in range(TILES)]
            store_field(k + 1, j, parts)

            @pl.when(k < ITERS)
            def _():
                send_field(k + 1, j, parts)
            dots(k, j, parts)
            return inner

        return lax.fori_loop(0, CHUNKS, body, carry)

    lax.fori_loop(1, ITERS + 1, stage, 0)

    gram = jnp.zeros((SUB, LANES), F32)
    for k in range(FIELDS):
        column = jnp.sum(jnp.sum(acc[k], axis=1), axis=1, keepdims=True)
        gram = gram + jnp.where(lane2 == k, column, 0.0)
    row = jnp.sum(pltpu.roll(gram, 0, 1, stride=SUB, stride_axis=0), axis=0, keepdims=True)
    ar_own[...] = row

    def scatter(own, slots, count, me, device, sems):
        def one(i, carry):
            @pl.when(i != me)
            def _():
                pltpu.make_async_remote_copy(
                    src_ref=own, dst_ref=slots.at[me], send_sem=sems.at[0], recv_sem=sems.at[1],
                    device_id=device(i), device_id_type=MESH).start()
            return carry
        lax.fori_loop(0, count, one, 0)
        slots[me] = own[...]
        rest = slots.at[pl.ds(0, count - 1)]
        pltpu.make_async_copy(rest, rest, sems.at[1]).wait()
        return jnp.sum(slots[...], axis=0)

    ar_own2[...] = scatter(ar_own, ar_x, nx, x, lambda i: (g, i, z), ar_sem.at[0])
    total = scatter(ar_own2, ar_z, nz, z, lambda i: (g, x, i), ar_sem.at[1])

    gram = unskew(jnp.broadcast_to(total, (SUB, LANES)), SUB, sub2)
    gram = jnp.where((lane2 < FIELDS) & (sub2 < ITERS), gram, 0.0)
    system = gram - jnp.where(lane2 == 0, 1.0, 0.5) * roll(gram, -1) - 0.5 * roll(gram, 1)
    system = jnp.where(lane2 < ITERS, system, jnp.where(lane2 == ITERS, roll(gram, ITERS), 0.0))
    for p in range(ITERS):
        pivot_row = system[p:p + 1, :] / system[p:p + 1, p:p + 1]
        system = jnp.where(sub2 == p, pivot_row, system - system[:, p:p + 1] * pivot_row)
    a = [system[k:k + 1, ITERS:ITERS + 1] for k in range(ITERS)]
    b = [None] * FIELDS
    b[0] = 1.0 - a[0] + 0.5 * a[1]
    b[1] = a[0] - a[1] + 0.5 * a[2]
    for k in range(2, ITERS - 1):
        b[k] = 0.5 * (a[k - 1] + a[k + 1]) - a[k]
    b[ITERS - 1] = 0.5 * a[ITERS - 2] - a[ITERS - 1]
    b[ITERS] = 0.5 * a[ITERS - 1]
    a = [jnp.broadcast_to(v, (SUB, LANES)) for v in a]
    b = [jnp.broadcast_to(v, (SUB, LANES)) for v in b]

    def combine(j, carry):
        for t in range(TILES):
            fields = [wbuf[k + 1, j + 1, :, t] for k in range(FIELDS)]
            up = a[0][None] * fields[0]
            down = b[0][None] * fields[0]
            for k in range(1, ITERS):
                up = up + a[k][None] * fields[k]
                down = down + b[k][None] * fields[k]
            down = down + b[ITERS][None] * fields[ITERS]
            put(xs, j, t, icbuf[j, :, t] * up)
            put(rs, j, t, gbuf[j, :, t] * down)
        return carry

    lax.fori_loop(0, CHUNKS, combine, 0)
    stores = []
    for t in range(TILES):
        lanes = pl.ds(t * LANES, LANES)
        stores.append(pltpu.make_async_copy(xs.at[t], out_x.at[:, lanes], out_sem.at[t]))
        stores.append(pltpu.make_async_copy(rs.at[t], out_r.at[:, lanes], out_sem.at[2 + t]))
    for store in stores:
        store.start()

    for d in range(8):
        @pl.when(exists(d))
        def _(d=d):
            whole = hx.at[:, :, d] if d < 2 else hz.at[:, :, d - 2] if d < 4 else hc.at[:, :, d - 4]
            pltpu.make_async_copy(whole, whole, send_sem.at[d]).wait()
    sent = ar_x.at[pl.ds(0, nx - 1)]
    pltpu.make_async_copy(sent, sent, ar_sem.at[0, 0]).wait()
    sent = ar_z.at[pl.ds(0, nz - 1)]
    pltpu.make_async_copy(sent, sent, ar_sem.at[1, 0]).wait()
    for store in stores:
        store.wait()


def on_device(nx, nz, forcing, conduct, diag_add, ice_mask, grounded):
    field = (CHUNKS, ROWS, TILES, SUB, LANES)
    native = (TILES, LAYERS * ROWS, LANES)
    wide = TILES * LANES
    any_space = pl.BlockSpec(memory_space=pl.ANY)
    out = jax.ShapeDtypeStruct((LAYERS * ROWS, wide), F32)
    vmem = pltpu.VMEM
    flat = lambda array: array.reshape(LAYERS * ROWS, wide)
    outs = pl.pallas_call(
        functools.partial(kernel, nx, nz),
        out_shape=(out, out),
        in_specs=[any_space] * 5,
        out_specs=(any_space, any_space),
        scratch_shapes=[
            vmem((LAYERS * ROWS, wide), jnp.bfloat16),
            vmem((LAYERS * ROWS, wide), jnp.bfloat16),
            vmem((ROWS, wide), jnp.int32),
            vmem((ROWS, wide), jnp.int32),
            vmem((ROWS, wide), F32),
            vmem(native, F32),
            vmem(native, F32),
            vmem(native, F32),
            vmem((FIELDS + 1, CHUNKS + 2, ROWS, TILES, SUB, LANES), F32),
            vmem((FIELDS, CHUNKS, 2, 2, TILES, SUB, LANES), F32),
            vmem((FIELDS, CHUNKS, 2, SUB, LANES), F32),
            vmem((FIELDS, CHUNKS, 4, 1, LANES), F32),
            vmem((FIELDS, CHUNKS, SUB, LANES), F32),
            vmem((FIELDS, CHUNKS, 1, LANES), F32),
            vmem(field, F32),
            vmem(field, F32),
            vmem(field, F32),
            vmem(field, F32),
            vmem((ROWS, TILES, SUB, LANES), F32),
            vmem((SUB, SUB, SUB, LANES), F32),
            vmem((TILES, ROWS, LANES), F32),
            vmem((TILES, ROWS, LANES), F32),
            vmem((1, LANES), F32),
            vmem((nx, 1, LANES), F32),
            vmem((1, LANES), F32),
            vmem((nz, 1, LANES), F32),
            vmem(native, F32),
            vmem(native, F32),
            pltpu.SemaphoreType.DMA((6,)),
            pltpu.SemaphoreType.DMA((4,)),
            pltpu.SemaphoreType.DMA((8,)),
            pltpu.SemaphoreType.DMA((FIELDS, CHUNKS, 8)),
            pltpu.SemaphoreType.DMA((2,)),
            pltpu.SemaphoreType.DMA((2, 2)),
        ],
        compiler_params=pltpu.CompilerParams(collective_id=0, has_side_effects=True),
        name="coupled_solve",
    )(flat(forcing), flat(conduct), flat(diag_add), ice_mask, grounded)
    return tuple(v.reshape(1, LAYERS, ROWS, wide) for v in outs)


def solution(mesh):
    block = P("group", None, "gx", "gy")
    columns = P("gx", "gy")
    return jax.shard_map(
        functools.partial(on_device, mesh.shape["gx"], mesh.shape["gy"]),
        mesh=mesh,
        in_specs=(block, block, block, columns, columns),
        out_specs=(block, block),
        check_vma=False,
    )
```

```python
import functools

import jax
import jax.numpy as jnp
from jax import lax
from jax.experimental import pallas as pl
from jax.experimental.pallas import tpu as pltpu
from jax.sharding import PartitionSpec as P

ITERS = 6
FIELDS = ITERS + 1
COUPLING = FIELDS + 1
LAYERS = 80
ROWS = 8
SUB = 8
LANES = 128
TILES = 2
CHUNKS = LAYERS // SUB
MESH = pl.DeviceIdType.MESH
F32 = jnp.float32

far_weight = 0.25
cross_weight = 0.5
vertical_weight = 4.0
friction_gain = 8.0

STEPS = ((-1, 0), (1, 0), (0, -1), (0, 1), (-1, -1), (-1, 1), (1, -1), (1, 1))


def roll(value, shift, axis=None):
    return pltpu.roll(value, shift % value.shape[-1 if axis is None else axis],
                      value.ndim - 1 if axis is None else axis)


def far_first(count):
    return sorted(range(1, count), key=lambda i: -min(i, count - i))


def kernel(
    nx, nz,
    forcing, conduct, diag_add, ice_mask, grounded, out_x, out_r,
    cbf, dbf, ice_v, ground_v, active_v, fs, cn, dn,
    wbuf, hx, hz, hc, pz, pc, ebuf, hbuf, icbuf, gbuf, acc,
    shared_out, shared_in, ar_own, ar_x, ar_own2, ar_z,
    in_sem, send_sem, recv_sem, share_sem, ar_sem,
):
    g = lax.axis_index("group")
    x = lax.axis_index("gx")
    z = lax.axis_index("gy")

    lane2 = lax.broadcasted_iota(jnp.int32, (SUB, LANES), 1)
    sub2 = lax.broadcasted_iota(jnp.int32, (SUB, LANES), 0)
    lane3 = lax.broadcasted_iota(jnp.int32, (ROWS, SUB, LANES), 2)
    sub3 = lax.broadcasted_iota(jnp.int32, (ROWS, SUB, LANES), 1)
    lane1 = lax.broadcasted_iota(jnp.int32, (1, LANES), 1)

    def exists(d):
        dx, dz = STEPS[d]
        conds = []
        if dx < 0:
            conds.append(x > 0)
        if dx > 0:
            conds.append(x < nx - 1)
        if dz < 0:
            conds.append(z > 0)
        if dz > 0:
            conds.append(z < nz - 1)
        return functools.reduce(jnp.logical_and, conds)

    def at(d):
        dx, dz = STEPS[d]
        return (g, x + dx, z + dz)

    loads = [
        pltpu.make_async_copy(conduct, cbf, in_sem.at[0]),
        pltpu.make_async_copy(ice_mask, ice_v, in_sem.at[1]),
        pltpu.make_async_copy(grounded, ground_v, in_sem.at[2]),
        pltpu.make_async_copy(forcing.at[:, pl.ds(0, LANES)], fs.at[0], in_sem.at[3]),
        pltpu.make_async_copy(forcing.at[:, pl.ds(LANES, LANES)], fs.at[1], in_sem.at[4]),
        pltpu.make_async_copy(diag_add, dbf, in_sem.at[5]),
    ]
    for load in loads:
        load.start()

    def zero_rims(d):
        @pl.when(jnp.logical_not(exists(d)))
        def _():
            def body(e, carry):
                if d < 2:
                    for j in range(CHUNKS):
                        hx[e, j, d] = jnp.zeros((2, TILES, SUB, LANES), F32)
                elif d < 4:
                    hz[e, :, d - 2] = jnp.zeros((CHUNKS, SUB, LANES), F32)
                else:
                    hc[e, :, d - 4] = jnp.zeros((CHUNKS, 1, LANES), F32)
                return carry
            lax.fori_loop(0, FIELDS, body, 0)

    for d in range(8):
        zero_rims(d)

    barrier = pltpu.get_barrier_semaphore()

    def greet_x(i, carry):
        @pl.when(i != x)
        def _():
            pl.semaphore_signal(barrier, inc=1, device_id=(g, i, z), device_id_type=MESH)
        return carry

    def greet_z(i, carry):
        @pl.when(i != z)
        def _():
            pl.semaphore_signal(barrier, inc=1, device_id=(g, x, i), device_id_type=MESH)
        return carry

    lax.fori_loop(0, nx, greet_x, 0)
    lax.fori_loop(0, nz, greet_z, 0)
    pl.semaphore_signal(barrier, inc=1, device_id=(1 - g, x, z), device_id_type=MESH)
    for d in range(4, 8):
        @pl.when(exists(d))
        def _(d=d):
            pl.semaphore_signal(barrier, inc=1, device_id=at(d), device_id_type=MESH)

    acc[...] = jnp.zeros_like(acc)

    def clear(f, carry):
        for j in range(CHUNKS):
            wbuf[f, j + 1] = jnp.zeros((ROWS, TILES, SUB, LANES), F32)
        return carry

    lax.fori_loop(0, FIELDS + 1, clear, 0)

    loads[0].wait()
    loads[1].wait()
    loads[2].wait()
    is_ice = jnp.where(g == 0, 1.0, 0.0).astype(F32)
    ice = ice_v[...].astype(F32)
    ground = ground_v[...].astype(F32)
    active_v[...] = ice * (1.0 - (1.0 - is_ice) * ground)

    def couple(i, carry):
        part = pl.ds(pl.multiple_of(i * SUB * ROWS, SUB * ROWS), SUB * ROWS)
        for t in range(TILES):
            columns = slice(t * LANES, (t + 1) * LANES)
            value = jnp.sqrt(cbf[part, columns].astype(F32)).reshape(SUB, ROWS, LANES)
            cn[t, part] = (value * active_v[:, columns][None]).reshape(SUB * ROWS, LANES)
        return carry

    lax.fori_loop(0, CHUNKS, couple, 0)


    def pick(ref, j, t):
        return jnp.stack([ref[t, pl.ds(j * ROWS + r, SUB, stride=CHUNKS * ROWS), :] for r in range(ROWS)])

    def put(ref, j, t, value):
        for r in range(ROWS):
            ref[t, pl.ds(j * ROWS + r, SUB, stride=CHUNKS * ROWS), :] = value[r]

    def copies(e, j, d):
        f = COUPLING if isinstance(e, int) and e == 0 else e
        if d == 0:
            src, dst = wbuf.at[f, j + 1, pl.ds(0, 2)], hx.at[e, j, 1]
        elif d == 1:
            src, dst = wbuf.at[f, j + 1, pl.ds(ROWS - 2, 2)], hx.at[e, j, 0]
        elif d < 4:
            src, dst = pz.at[e, j], hz.at[e, j, 3 - d]
        else:
            src, dst = pc.at[e, j], hc.at[e, j, 7 - d]
        opposite = (1, 0, 3, 2, 7, 6, 5, 4)[d]
        return pltpu.make_async_remote_copy(
            src_ref=src, dst_ref=dst, send_sem=send_sem.at[d],
            recv_sem=recv_sem.at[e, j, opposite], device_id=at(d), device_id_type=MESH)

    def store_field(f, j, parts):
        for t in range(TILES):
            wbuf[f, j + 1, :, t] = parts[t]

        @pl.when(j == 0)
        def _():
            for t in range(TILES):
                wbuf[f, CHUNKS + 1, :, t] = jnp.where(sub3 < SUB - 1, roll(parts[t], SUB - 1, 1), 0.0)

        @pl.when(j == CHUNKS - 1)
        def _():
            for t in range(TILES):
                wbuf[f, 0, :, t] = jnp.where(sub3 > 0, roll(parts[t], 1, 1), 0.0)

    def pack_rims(e, j, parts):
        none = jnp.zeros((1, SUB, LANES), F32)
        crossed, scaled = [], []
        for t in range(TILES):
            wide = jnp.concatenate([none, parts[t], none], axis=0)
            crossed.append(parts[t] + cross_weight * (wide[0:8] + wide[2:10]))
            scaled.append(far_weight * parts[t])
        sources = (
            (jnp.where(lane3 == LANES - 1, crossed[1], 0.0), 1),
            (jnp.where(lane3 == 0, crossed[0], 0.0), -1),
            (jnp.where(lane3 >= LANES - 2, scaled[1], 0.0), 2),
            (jnp.where(lane3 < 2, scaled[0], 0.0), -2),
        )
        packed = None
        for source, shift in sources:
            for r in range(ROWS):
                moved = roll(source[r], 4 * (r + 1) + shift)
                packed = moved if packed is None else packed + moved
        pz[e, j] = packed
        corners = None
        for q in range(4):
            row, tile = (0, ROWS - 1)[q // 2], q % 2
            lane = (0, LANES - 1)[tile]
            only = jnp.where(lane2 == lane, cross_weight * parts[tile][row], 0.0)
            moved = pltpu.roll(only, (8 * q - lane) % LANES, 1, stride=1, stride_axis=0)
            corners = moved if corners is None else corners + moved
        pc[e, j] = jnp.sum(corners, axis=0, keepdims=True)

    def send_rims(e, j, wanted):
        for d in range(8):
            @pl.when(exists(d) if wanted is None else jnp.logical_and(exists(d), wanted))
            def _(d=d):
                copies(e, j, d).start()

    def await_rims(e, j):
        for d in range(8):
            @pl.when(exists(d))
            def _(d=d):
                opposite = (1, 0, 3, 2, 7, 6, 5, 4)[d]
                copies(e, j, opposite).wait_recv()

    def spread(f, e, j):
        centre = [wbuf[f, j + 1, :, t] for t in range(TILES)]
        beside, mixed, scaled = [], [], []
        for t in range(TILES):
            wide = jnp.concatenate([hx[e, j, 0, :, t], centre[t], hx[e, j, 1, :, t]], axis=0)
            near = wide[1:9] + wide[3:11]
            far = wide[0:8] + wide[4:12]
            vertical = wbuf[f, j, :, t] + wbuf[f, j + 2, :, t]
            beside.append(near + far_weight * far + vertical_weight * vertical)
            mixed.append(centre[t] + cross_weight * near)
            scaled.append(far_weight * centre[t])
        for source, shift in ((mixed, 1), (scaled, 2)):
            a, b = roll(source[0], shift), roll(source[1], shift)
            beside[0] = beside[0] + jnp.where(lane3 < shift, 0.0, a)
            beside[1] = beside[1] + jnp.where(lane3 < shift, a, b)
            a, b = roll(source[0], -shift), roll(source[1], -shift)
            beside[0] = beside[0] + jnp.where(lane3 >= LANES - shift, b, a)
            beside[1] = beside[1] + jnp.where(lane3 >= LANES - shift, 0.0, b)

        edge = jnp.where(lane2 % 4 < 2, hz[e, j, 0], hz[e, j, 1])
        rows = [roll(edge, -4 * (r + 1)) for r in range(ROWS)]
        corner = []
        for q in range(4):
            picked = jnp.where(lane2 == 8 * (3 - q) + sub2, jnp.broadcast_to(hc[e, j, q], (SUB, LANES)), 0.0)
            corner.append(jnp.sum(picked, axis=1, keepdims=True))
        rows[0] = rows[0] + jnp.where(lane2 == 0, corner[0], jnp.where(lane2 == LANES - 1, corner[1], 0.0))
        rows[-1] = rows[-1] + jnp.where(lane2 == 0, corner[2], jnp.where(lane2 == LANES - 1, corner[3], 0.0))
        rows = jnp.stack(rows)
        return [beside[0] + jnp.where(lane3 < 2, rows, 0.0),
                beside[1] + jnp.where(lane3 >= LANES - 2, rows, 0.0)]

    def dots(k, j, parts, count):
        weighted = [hbuf[j, :, t] * parts[t] for t in range(TILES)]
        for i in range(count):
            product = [jnp.sum(weighted[t] * wbuf[i + 1, j + 1, :, t], axis=0) for t in range(TILES)]
            acc[k, i] = acc[k, i] + (product[0] + product[1])

    beside_x = (x > 0).astype(jnp.int32) + (x < nx - 1).astype(jnp.int32)
    beside_z = (z > 0).astype(jnp.int32) + (z < nz - 1).astype(jnp.int32)
    pl.semaphore_wait(barrier, nx + nz - 1 + beside_x * beside_z)
    def first(j, carry):
        parts = [pick(cn, j, t) for t in range(TILES)]
        store_field(COUPLING, j, parts)
        pack_rims(0, j, parts)
        send_rims(0, j, None)
        return carry

    lax.fori_loop(0, CHUNKS, first, 0)

    loads[3].wait()
    loads[4].wait()
    edge = pl.ds(pl.multiple_of(g * ((LAYERS - 1) * ROWS), ROWS), ROWS)
    for t in range(TILES):
        mean = jnp.sum(fs[t].reshape(LAYERS, ROWS, LANES), axis=0) * (1.0 / LAYERS)
        value = active_v[:, t * LANES:(t + 1) * LANES] * mean
        shared_out[t] = value * cn[t, edge]
    loads[5].wait()

    def widen(i, carry):
        part = pl.ds(pl.multiple_of(i * SUB * ROWS, SUB * ROWS), SUB * ROWS)
        for t in range(TILES):
            dn[t, part] = dbf[part, t * LANES:(t + 1) * LANES].astype(F32)
        return carry

    lax.fori_loop(0, CHUNKS, widen, 0)
    for t in range(TILES):
        columns = slice(t * LANES, (t + 1) * LANES)
        friction = is_ice * friction_gain * (ground_v[:, columns].astype(F32) * ice_v[:, columns].astype(F32))
        dn[t, 0:ROWS] = dn[t, 0:ROWS] + friction

    share = pltpu.make_async_remote_copy(
        src_ref=shared_out, dst_ref=shared_in, send_sem=share_sem.at[0], recv_sem=share_sem.at[1],
        device_id=(1 - g, x, z), device_id_type=MESH)
    share.start()

    share.wait()
    for t in range(TILES):
        fs[t, edge] = fs[t, edge] + shared_in[t]

    def second(j, carry):
        await_rims(0, j)
        spreads = spread(COUPLING, 0, j)
        parts = []
        for t in range(TILES):
            c = wbuf[COUPLING, j + 1, :, t]
            diagonal = pick(dn, j, t) + c * spreads[t]
            ratio = c / diagonal
            inverse_c = jnp.where(c > 0.0, 1.0 / jnp.where(c > 0.0, c, 1.0), 0.0)
            back = diagonal * inverse_c
            ebuf[j, :, t] = 2.0 * ratio * c
            icbuf[j, :, t] = inverse_c
            gbuf[j, :, t] = back
            hbuf[j, :, t] = back * inverse_c
            parts.append(ratio * pick(fs, j, t))
        store_field(1, j, parts)
        pack_rims(1, j, parts)
        dots(0, j, parts, 1)
        send_rims(1, j, None)
        return carry

    lax.fori_loop(0, CHUNKS, second, 0)

    def stage(k, carry):
        def body(j, inner):
            await_rims(k, j)
            spreads = spread(k, k, j)
            parts = [ebuf[j, :, t] * spreads[t] - wbuf[k - 1, j + 1, :, t] for t in range(TILES)]
            store_field(k + 1, j, parts)
            pack_rims(k + 1, j, parts)
            dots(k, j, parts, FIELDS)
            send_rims(k + 1, j, k < ITERS)
            return inner

        return lax.fori_loop(0, CHUNKS, body, carry)

    lax.fori_loop(1, ITERS + 1, stage, 0)

    gram = jnp.zeros((SUB, LANES), F32)
    for k in range(FIELDS):
        column = jnp.sum(jnp.sum(acc[k], axis=1), axis=1, keepdims=True)
        gram = gram + jnp.where((lane2 == SUB * sub2 + k) & (sub2 <= k), column, 0.0)
    row = jnp.sum(gram, axis=0, keepdims=True)
    ar_own[...] = row

    def scatter(own, slots, me, count, offsets, device, sems):
        for offset in offsets:
            pltpu.make_async_remote_copy(
                src_ref=own, dst_ref=slots.at[me], send_sem=sems.at[0], recv_sem=sems.at[1],
                device_id=device((me + offset) % count), device_id_type=MESH).start()
        slots[me] = own[...]
        rest = slots.at[pl.ds(0, count - 1)]
        pltpu.make_async_copy(rest, rest, sems.at[1]).wait()
        return jnp.sum(slots[...], axis=0)

    ar_own2[...] = scatter(ar_own, ar_x, x, nx, far_first(nx), lambda i: (g, i, z), ar_sem.at[0])
    total = scatter(ar_own2, ar_z, z, nz, far_first(nz), lambda i: (g, x, i), ar_sem.at[1])

    total = jnp.broadcast_to(total, (SUB, LANES))

    def entry(i, k):
        lane = SUB * min(i, k) + max(i, k)
        return jnp.broadcast_to(total[:, lane:lane + 1], (SUB, LANES))

    gram = [[entry(i, k) for k in range(i, FIELDS)] for i in range(ITERS)]
    inner = lambda i, k: gram[min(i, k)][abs(i - k)]
    system = {(i, k): inner(i, k) - 0.5 * (inner(i, k + 1) + inner(i, k - 1) if k else inner(i, 1))
              for i in range(ITERS) for k in range(i, ITERS)}
    right = [inner(0, i) for i in range(ITERS)]
    inverse = []
    for p in range(ITERS):
        inverse.append(1.0 / system[p, p])
        for i in range(p + 1, ITERS):
            factor = system[p, i] * inverse[p]
            for k in range(i, ITERS):
                system[i, k] = system[i, k] - factor * system[p, k]
            right[i] = right[i] - factor * right[p]
    a = [None] * ITERS
    for p in reversed(range(ITERS)):
        value = right[p]
        for k in range(p + 1, ITERS):
            value = value - system[p, k] * a[k]
        a[p] = value * inverse[p]
    b = [None] * FIELDS
    b[0] = 1.0 - a[0] + 0.5 * a[1]
    for k in range(1, ITERS - 1):
        b[k] = 0.5 * (a[k - 1] + a[k + 1]) - a[k]
    b[ITERS - 1] = 0.5 * a[ITERS - 2] - a[ITERS - 1]
    b[ITERS] = 0.5 * a[ITERS - 1]
    def combine(j, carry):
        for t in range(TILES):
            fields = [wbuf[k + 1, j + 1, :, t] for k in range(FIELDS)]
            up = a[0][None] * fields[0]
            down = b[0][None] * fields[0]
            for k in range(1, ITERS):
                up = up + a[k][None] * fields[k]
                down = down + b[k][None] * fields[k]
            down = down + b[ITERS][None] * fields[ITERS]
            put(out_x, j, t, icbuf[j, :, t] * up)
            put(out_r, j, t, gbuf[j, :, t] * down)
        return carry

    lax.fori_loop(0, CHUNKS, combine, 0)
    for d in range(8):
        @pl.when(exists(d))
        def _(d=d):
            whole = hx.at[:, :, d] if d < 2 else hz.at[:, :, d - 2] if d < 4 else hc.at[:, :, d - 4]
            pltpu.make_async_copy(whole, whole, send_sem.at[d]).wait()
    sent = ar_x.at[pl.ds(0, nx - 1)]
    pltpu.make_async_copy(sent, sent, ar_sem.at[0, 0]).wait()
    sent = ar_z.at[pl.ds(0, nz - 1)]
    pltpu.make_async_copy(sent, sent, ar_sem.at[1, 0]).wait()


def on_device(nx, nz, forcing, conduct, diag_add, ice_mask, grounded):
    field = (CHUNKS, ROWS, TILES, SUB, LANES)
    native = (TILES, LAYERS * ROWS, LANES)
    wide = TILES * LANES
    hbm_space = pl.BlockSpec(memory_space=pltpu.HBM)
    vmem_space = pl.BlockSpec(memory_space=pltpu.VMEM)
    out = jax.ShapeDtypeStruct(native, F32)
    vmem = pltpu.VMEM
    flat = lambda array: array.reshape(LAYERS * ROWS, wide)
    outs = pl.pallas_call(
        functools.partial(kernel, nx, nz),
        out_shape=(out, out),
        in_specs=[hbm_space] * 5,
        out_specs=(vmem_space, vmem_space),
        scratch_shapes=[
            vmem((LAYERS * ROWS, wide), jnp.bfloat16),
            vmem((LAYERS * ROWS, wide), jnp.bfloat16),
            vmem((ROWS, wide), jnp.int32),
            vmem((ROWS, wide), jnp.int32),
            vmem((ROWS, wide), F32),
            vmem(native, F32),
            vmem(native, F32),
            vmem(native, F32),
            vmem((COUPLING + 1, CHUNKS + 2, ROWS, TILES, SUB, LANES), F32),
            vmem((FIELDS, CHUNKS, 2, 2, TILES, SUB, LANES), F32),
            vmem((FIELDS, CHUNKS, 2, SUB, LANES), F32),
            vmem((FIELDS, CHUNKS, 4, 1, LANES), F32),
            vmem((FIELDS + 1, CHUNKS, SUB, LANES), F32),
            vmem((FIELDS + 1, CHUNKS, 1, LANES), F32),
            vmem(field, F32),
            vmem(field, F32),
            vmem(field, F32),
            vmem(field, F32),
            vmem((SUB, SUB, SUB, LANES), F32),
            vmem((TILES, ROWS, LANES), F32),
            vmem((TILES, ROWS, LANES), F32),
            vmem((1, LANES), F32),
            vmem((nx, 1, LANES), F32),
            vmem((1, LANES), F32),
            vmem((nz, 1, LANES), F32),
            pltpu.SemaphoreType.DMA((6,)),
            pltpu.SemaphoreType.DMA((8,)),
            pltpu.SemaphoreType.DMA((FIELDS, CHUNKS, 8)),
            pltpu.SemaphoreType.DMA((2,)),
            pltpu.SemaphoreType.DMA((2, 2)),
        ],
        compiler_params=pltpu.CompilerParams(collective_id=0, has_side_effects=True, vmem_limit_bytes=40 * 1024 * 1024),
        name="coupled_solve",
    )(*[pltpu.with_memory_space_constraint(v, pltpu.HBM)
        for v in (flat(forcing), flat(conduct), flat(diag_add), ice_mask, grounded)])
    return tuple(
        v.reshape(TILES, LAYERS, ROWS, LANES).transpose(1, 2, 0, 3).reshape(1, LAYERS, ROWS, wide)
        for v in outs)


def solution(mesh):
    block = P("group", None, "gx", "gy")
    columns = P("gx", "gy")
    return jax.shard_map(
        functools.partial(on_device, mesh.shape["gx"], mesh.shape["gy"]),
        mesh=mesh,
        in_specs=(block, block, block, columns, columns),
        out_specs=(block, block),
        check_vma=False,
    )
```

```python
import functools

import jax
import jax.numpy as jnp
from jax import lax
from jax.experimental import pallas as pl
from jax.experimental.pallas import tpu as pltpu
from jax.sharding import PartitionSpec as P

ITERS = 6
FIELDS = ITERS + 1
COUPLING = FIELDS + 1
LAYERS = 80
ROWS = 8
SUB = 8
LANES = 128
TILES = 2
CHUNKS = LAYERS // SUB
MESH = pl.DeviceIdType.MESH
F32 = jnp.float32

far_weight = 0.25
cross_weight = 0.5
vertical_weight = 4.0
friction_gain = 8.0

STEPS = ((-1, 0), (1, 0), (0, -1), (0, 1), (-1, -1), (-1, 1), (1, -1), (1, 1))


def roll(value, shift, axis=None):
    return pltpu.roll(value, shift % value.shape[-1 if axis is None else axis],
                      value.ndim - 1 if axis is None else axis)


def far_first(count):
    return sorted(range(1, count), key=lambda i: -min(i, count - i))


def kernel(
    nx, nz,
    forcing, conduct, diag_add, ice_mask, grounded, out_x, out_r,
    cbf, dbf, ice_v, ground_v, active_v, fs, cn, dn,
    wbuf, hx, hz, hc, pz, pc, ebuf, hbuf, icbuf, gbuf, acc,
    shared_out, shared_in, ar_own, ar_x, ar_own2, ar_z,
    in_sem, send_sem, recv_sem, share_sem, ar_sem,
):
    g = lax.axis_index("group")
    x = lax.axis_index("gx")
    z = lax.axis_index("gy")

    lane2 = lax.broadcasted_iota(jnp.int32, (SUB, LANES), 1)
    sub2 = lax.broadcasted_iota(jnp.int32, (SUB, LANES), 0)
    lane3 = lax.broadcasted_iota(jnp.int32, (ROWS, SUB, LANES), 2)
    sub3 = lax.broadcasted_iota(jnp.int32, (ROWS, SUB, LANES), 1)
    lane1 = lax.broadcasted_iota(jnp.int32, (1, LANES), 1)

    beside_x = (x > 0).astype(jnp.int32) + (x < nx - 1).astype(jnp.int32)
    beside_z = (z > 0).astype(jnp.int32) + (z < nz - 1).astype(jnp.int32)

    def exists(d):
        dx, dz = STEPS[d]
        conds = []
        if dx < 0:
            conds.append(x > 0)
        if dx > 0:
            conds.append(x < nx - 1)
        if dz < 0:
            conds.append(z > 0)
        if dz > 0:
            conds.append(z < nz - 1)
        return functools.reduce(jnp.logical_and, conds)

    def at(d):
        dx, dz = STEPS[d]
        return (g, x + dx, z + dz)

    loads = [
        pltpu.make_async_copy(conduct, cbf, in_sem.at[0]),
        pltpu.make_async_copy(ice_mask, ice_v, in_sem.at[1]),
        pltpu.make_async_copy(grounded, ground_v, in_sem.at[2]),
        pltpu.make_async_copy(forcing.at[:, pl.ds(0, LANES)], fs.at[0], in_sem.at[3]),
        pltpu.make_async_copy(forcing.at[:, pl.ds(LANES, LANES)], fs.at[1], in_sem.at[4]),
        pltpu.make_async_copy(diag_add, dbf, in_sem.at[5]),
    ]
    for load in loads:
        load.start()

    def zero_rims(d):
        @pl.when(jnp.logical_not(exists(d)))
        def _():
            def body(e, carry):
                if d < 2:
                    for j in range(CHUNKS):
                        hx[e, j, d] = jnp.zeros((2, TILES, SUB, LANES), F32)
                elif d < 4:
                    hz[e, :, d - 2] = jnp.zeros((CHUNKS, SUB, LANES), F32)
                else:
                    hc[e, :, d - 4] = jnp.zeros((CHUNKS, 1, LANES), F32)
                return carry
            lax.fori_loop(0, FIELDS, body, 0)

    for d in range(8):
        zero_rims(d)

    barrier = pltpu.get_barrier_semaphore()

    def greet_x(i, carry):
        @pl.when(i != x)
        def _():
            pl.semaphore_signal(barrier, inc=1, device_id=(g, i, z), device_id_type=MESH)
        return carry

    def greet_z(i, carry):
        @pl.when(i != z)
        def _():
            pl.semaphore_signal(barrier, inc=1, device_id=(g, x, i), device_id_type=MESH)
        return carry

    lax.fori_loop(0, nx, greet_x, 0)
    lax.fori_loop(0, nz, greet_z, 0)
    pl.semaphore_signal(barrier, inc=1, device_id=(1 - g, x, z), device_id_type=MESH)
    for d in range(4, 8):
        @pl.when(exists(d))
        def _(d=d):
            pl.semaphore_signal(barrier, inc=1, device_id=at(d), device_id_type=MESH)

    acc[...] = jnp.zeros_like(acc)

    def clear(f, carry):
        for j in range(CHUNKS):
            wbuf[f, j + 1] = jnp.zeros((ROWS, TILES, SUB, LANES), F32)
        return carry

    lax.fori_loop(0, FIELDS + 1, clear, 0)

    loads[0].wait()
    loads[1].wait()
    loads[2].wait()
    is_ice = jnp.where(g == 0, 1.0, 0.0).astype(F32)
    ice = ice_v[...].astype(F32)
    ground = ground_v[...].astype(F32)
    active_v[...] = ice * (1.0 - (1.0 - is_ice) * ground)

    def couple(i, carry):
        part = pl.ds(pl.multiple_of(i * SUB * ROWS, SUB * ROWS), SUB * ROWS)
        for t in range(TILES):
            columns = slice(t * LANES, (t + 1) * LANES)
            value = jnp.sqrt(cbf[part, columns].astype(F32)).reshape(SUB, ROWS, LANES)
            cn[t, part] = (value * active_v[:, columns][None]).reshape(SUB * ROWS, LANES)
        return carry

    lax.fori_loop(0, CHUNKS, couple, 0)


    def pick(ref, j, t):
        return jnp.stack([ref[t, pl.ds(j * ROWS + r, SUB, stride=CHUNKS * ROWS), :] for r in range(ROWS)])

    def put(ref, j, t, value):
        for r in range(ROWS):
            ref[t, pl.ds(j * ROWS + r, SUB, stride=CHUNKS * ROWS), :] = value[r]

    def copies(e, j, d):
        f = COUPLING if isinstance(e, int) and e == 0 else e
        if d == 0:
            src, dst = wbuf.at[f, j + 1, pl.ds(0, 2)], hx.at[e, j, 1]
        elif d == 1:
            src, dst = wbuf.at[f, j + 1, pl.ds(ROWS - 2, 2)], hx.at[e, j, 0]
        elif d < 4:
            src, dst = pz.at[e, j], hz.at[e, j, 3 - d]
        else:
            src, dst = pc.at[e, j], hc.at[e, j, 7 - d]
        return pltpu.make_async_remote_copy(
            src_ref=src, dst_ref=dst, send_sem=send_sem.at[d],
            recv_sem=recv_sem.at[e % 2, j, min(d // 2, 2)], device_id=at(d), device_id_type=MESH)

    def store_field(f, j, parts):
        for t in range(TILES):
            wbuf[f, j + 1, :, t] = parts[t]

        @pl.when(j == 0)
        def _():
            for t in range(TILES):
                wbuf[f, CHUNKS + 1, :, t] = jnp.where(sub3 < SUB - 1, roll(parts[t], SUB - 1, 1), 0.0)

        @pl.when(j == CHUNKS - 1)
        def _():
            for t in range(TILES):
                wbuf[f, 0, :, t] = jnp.where(sub3 > 0, roll(parts[t], 1, 1), 0.0)

    def pack_rims(e, j, parts):
        none = jnp.zeros((1, SUB, LANES), F32)
        crossed, scaled = [], []
        for t in range(TILES):
            wide = jnp.concatenate([none, parts[t], none], axis=0)
            crossed.append(parts[t] + cross_weight * (wide[0:8] + wide[2:10]))
            scaled.append(far_weight * parts[t])
        sources = (
            (jnp.where(lane3 == LANES - 1, crossed[1], 0.0), 1),
            (jnp.where(lane3 == 0, crossed[0], 0.0), -1),
            (jnp.where(lane3 >= LANES - 2, scaled[1], 0.0), 2),
            (jnp.where(lane3 < 2, scaled[0], 0.0), -2),
        )
        packed = None
        for source, shift in sources:
            for r in range(ROWS):
                moved = roll(source[r], 4 * (r + 1) + shift)
                packed = moved if packed is None else packed + moved
        pz[e, j] = packed
        corners = None
        for q in range(4):
            row, tile = (0, ROWS - 1)[q // 2], q % 2
            lane = (0, LANES - 1)[tile]
            only = jnp.where(lane2 == lane, cross_weight * parts[tile][row], 0.0)
            moved = pltpu.roll(only, (8 * q - lane) % LANES, 1, stride=1, stride_axis=0)
            corners = moved if corners is None else corners + moved
        pc[e, j] = jnp.sum(corners, axis=0, keepdims=True)

    def send_rims(e, j, wanted):
        for d in (4, 5, 6, 7, 2, 3, 0, 1):
            @pl.when(exists(d) if wanted is None else jnp.logical_and(exists(d), wanted))
            def _(d=d):
                copies(e, j, d).start()

    def await_rims(e, j):
        def arrive(kind, condition, whole):
            @pl.when(condition)
            def _():
                pltpu.make_async_copy(whole, whole, recv_sem.at[e % 2, j, kind]).wait()

        both = beside_x * beside_z
        arrive(0, beside_x == 2, hx.at[e, j])
        arrive(0, beside_x == 1, hx.at[e, j, 0])
        arrive(1, beside_z == 2, hz.at[e, j])
        arrive(1, beside_z == 1, hz.at[e, j, 0])
        arrive(2, both == 4, hc.at[e, j])
        arrive(2, both == 2, hc.at[e, j, pl.ds(0, 2)])
        arrive(2, both == 1, hc.at[e, j, 0])

    def spread(f, e, j):
        centre = [wbuf[f, j + 1, :, t] for t in range(TILES)]
        beside, mixed, scaled = [], [], []
        for t in range(TILES):
            wide = jnp.concatenate([hx[e, j, 0, :, t], centre[t], hx[e, j, 1, :, t]], axis=0)
            near = wide[1:9] + wide[3:11]
            far = wide[0:8] + wide[4:12]
            vertical = wbuf[f, j, :, t] + wbuf[f, j + 2, :, t]
            beside.append(near + far_weight * far + vertical_weight * vertical)
            mixed.append(centre[t] + cross_weight * near)
            scaled.append(far_weight * centre[t])
        for source, shift in ((mixed, 1), (scaled, 2)):
            a, b = roll(source[0], shift), roll(source[1], shift)
            beside[0] = beside[0] + jnp.where(lane3 < shift, 0.0, a)
            beside[1] = beside[1] + jnp.where(lane3 < shift, a, b)
            a, b = roll(source[0], -shift), roll(source[1], -shift)
            beside[0] = beside[0] + jnp.where(lane3 >= LANES - shift, b, a)
            beside[1] = beside[1] + jnp.where(lane3 >= LANES - shift, 0.0, b)

        edge = jnp.where(lane2 % 4 < 2, hz[e, j, 0], hz[e, j, 1])
        rows = [roll(edge, -4 * (r + 1)) for r in range(ROWS)]
        corner = []
        for q in range(4):
            picked = jnp.where(lane2 == 8 * (3 - q) + sub2, jnp.broadcast_to(hc[e, j, q], (SUB, LANES)), 0.0)
            corner.append(jnp.sum(picked, axis=1, keepdims=True))
        rows[0] = rows[0] + jnp.where(lane2 == 0, corner[0], jnp.where(lane2 == LANES - 1, corner[1], 0.0))
        rows[-1] = rows[-1] + jnp.where(lane2 == 0, corner[2], jnp.where(lane2 == LANES - 1, corner[3], 0.0))
        rows = jnp.stack(rows)
        return [beside[0] + jnp.where(lane3 < 2, rows, 0.0),
                beside[1] + jnp.where(lane3 >= LANES - 2, rows, 0.0)]

    def dots(k, j, parts, count):
        weighted = [hbuf[j, :, t] * parts[t] for t in range(TILES)]
        for i in range(count):
            product = [jnp.sum(weighted[t] * wbuf[i + 1, j + 1, :, t], axis=0) for t in range(TILES)]
            acc[k, i] = acc[k, i] + (product[0] + product[1])

    pl.semaphore_wait(barrier, nx + nz - 1 + beside_x * beside_z)
    def first(j, carry):
        parts = [pick(cn, j, t) for t in range(TILES)]
        store_field(COUPLING, j, parts)
        pack_rims(0, j, parts)
        send_rims(0, j, None)
        return carry

    lax.fori_loop(0, CHUNKS, first, 0)

    loads[3].wait()
    loads[4].wait()
    edge = pl.ds(pl.multiple_of(g * ((LAYERS - 1) * ROWS), ROWS), ROWS)
    for t in range(TILES):
        mean = jnp.sum(fs[t].reshape(LAYERS, ROWS, LANES), axis=0) * (1.0 / LAYERS)
        value = active_v[:, t * LANES:(t + 1) * LANES] * mean
        shared_out[t] = value * cn[t, edge]
    loads[5].wait()

    def widen(i, carry):
        part = pl.ds(pl.multiple_of(i * SUB * ROWS, SUB * ROWS), SUB * ROWS)
        for t in range(TILES):
            dn[t, part] = dbf[part, t * LANES:(t + 1) * LANES].astype(F32)
        return carry

    lax.fori_loop(0, CHUNKS, widen, 0)
    for t in range(TILES):
        columns = slice(t * LANES, (t + 1) * LANES)
        friction = is_ice * friction_gain * (ground_v[:, columns].astype(F32) * ice_v[:, columns].astype(F32))
        dn[t, 0:ROWS] = dn[t, 0:ROWS] + friction

    share = pltpu.make_async_remote_copy(
        src_ref=shared_out, dst_ref=shared_in, send_sem=share_sem.at[0], recv_sem=share_sem.at[1],
        device_id=(1 - g, x, z), device_id_type=MESH)
    share.start()

    share.wait()
    for t in range(TILES):
        fs[t, edge] = fs[t, edge] + shared_in[t]

    def second(j, carry):
        await_rims(0, j)
        spreads = spread(COUPLING, 0, j)
        parts = []
        for t in range(TILES):
            c = wbuf[COUPLING, j + 1, :, t]
            diagonal = pick(dn, j, t) + c * spreads[t]
            ratio = c / diagonal
            inverse_c = jnp.where(c > 0.0, 1.0 / jnp.where(c > 0.0, c, 1.0), 0.0)
            back = diagonal * inverse_c
            ebuf[j, :, t] = 2.0 * ratio * c
            icbuf[j, :, t] = inverse_c
            gbuf[j, :, t] = back
            hbuf[j, :, t] = back * inverse_c
            parts.append(ratio * pick(fs, j, t))
        store_field(1, j, parts)
        pack_rims(1, j, parts)
        dots(0, j, parts, 1)
        send_rims(1, j, None)
        return carry

    lax.fori_loop(0, CHUNKS, second, 0)

    def stage(k, carry):
        def body(j, inner):
            await_rims(k, j)
            spreads = spread(k, k, j)
            parts = [ebuf[j, :, t] * spreads[t] - wbuf[k - 1, j + 1, :, t] for t in range(TILES)]
            store_field(k + 1, j, parts)
            pack_rims(k + 1, j, parts)
            dots(k, j, parts, FIELDS)
            send_rims(k + 1, j, k < ITERS)
            return inner

        return lax.fori_loop(0, CHUNKS, body, carry)

    lax.fori_loop(1, ITERS + 1, stage, 0)

    gram = jnp.zeros((SUB, LANES), F32)
    for k in range(FIELDS):
        column = jnp.sum(jnp.sum(acc[k], axis=1), axis=1, keepdims=True)
        gram = gram + jnp.where((lane2 == SUB * sub2 + k) & (sub2 <= k), column, 0.0)
    row = jnp.sum(gram, axis=0, keepdims=True)
    ar_own[...] = row

    def scatter(own, slots, me, count, offsets, device, sems):
        for offset in offsets:
            pltpu.make_async_remote_copy(
                src_ref=own, dst_ref=slots.at[me], send_sem=sems.at[0], recv_sem=sems.at[1],
                device_id=device((me + offset) % count), device_id_type=MESH).start()
        slots[me] = own[...]
        rest = slots.at[pl.ds(0, count - 1)]
        pltpu.make_async_copy(rest, rest, sems.at[1]).wait()
        return jnp.sum(slots[...], axis=0)

    ar_own2[...] = scatter(ar_own, ar_x, x, nx, far_first(nx), lambda i: (g, i, z), ar_sem.at[0])
    total = scatter(ar_own2, ar_z, z, nz, far_first(nz), lambda i: (g, x, i), ar_sem.at[1])

    total = jnp.broadcast_to(total, (SUB, LANES))

    def entry(i, k):
        lane = SUB * min(i, k) + max(i, k)
        return jnp.broadcast_to(total[:, lane:lane + 1], (SUB, LANES))

    gram = [[entry(i, k) for k in range(i, FIELDS)] for i in range(ITERS)]
    inner = lambda i, k: gram[min(i, k)][abs(i - k)]
    system = {(i, k): inner(i, k) - 0.5 * (inner(i, k + 1) + inner(i, k - 1) if k else inner(i, 1))
              for i in range(ITERS) for k in range(i, ITERS)}
    right = [inner(0, i) for i in range(ITERS)]
    inverse = []
    for p in range(ITERS):
        inverse.append(1.0 / system[p, p])
        for i in range(p + 1, ITERS):
            factor = system[p, i] * inverse[p]
            for k in range(i, ITERS):
                system[i, k] = system[i, k] - factor * system[p, k]
            right[i] = right[i] - factor * right[p]
    a = [None] * ITERS
    for p in reversed(range(ITERS)):
        value = right[p]
        for k in range(p + 1, ITERS):
            value = value - system[p, k] * a[k]
        a[p] = value * inverse[p]
    b = [None] * FIELDS
    b[0] = 1.0 - a[0] + 0.5 * a[1]
    for k in range(1, ITERS - 1):
        b[k] = 0.5 * (a[k - 1] + a[k + 1]) - a[k]
    b[ITERS - 1] = 0.5 * a[ITERS - 2] - a[ITERS - 1]
    b[ITERS] = 0.5 * a[ITERS - 1]
    def combine(j, carry):
        for t in range(TILES):
            fields = [wbuf[k + 1, j + 1, :, t] for k in range(FIELDS)]
            up = a[0][None] * fields[0]
            down = b[0][None] * fields[0]
            for k in range(1, ITERS):
                up = up + a[k][None] * fields[k]
                down = down + b[k][None] * fields[k]
            down = down + b[ITERS][None] * fields[ITERS]
            put(out_x, j, t, icbuf[j, :, t] * up)
            put(out_r, j, t, gbuf[j, :, t] * down)
        return carry

    lax.fori_loop(0, CHUNKS, combine, 0)
    for d in range(8):
        @pl.when(exists(d))
        def _(d=d):
            whole = hx.at[:, :, d] if d < 2 else hz.at[:, :, d - 2] if d < 4 else hc.at[:, :, d - 4]
            pltpu.make_async_copy(whole, whole, send_sem.at[d]).wait()
    sent = ar_x.at[pl.ds(0, nx - 1)]
    pltpu.make_async_copy(sent, sent, ar_sem.at[0, 0]).wait()
    sent = ar_z.at[pl.ds(0, nz - 1)]
    pltpu.make_async_copy(sent, sent, ar_sem.at[1, 0]).wait()


def on_device(nx, nz, forcing, conduct, diag_add, ice_mask, grounded):
    field = (CHUNKS, ROWS, TILES, SUB, LANES)
    native = (TILES, LAYERS * ROWS, LANES)
    wide = TILES * LANES
    hbm_space = pl.BlockSpec(memory_space=pltpu.HBM)
    vmem_space = pl.BlockSpec(memory_space=pltpu.VMEM)
    out = jax.ShapeDtypeStruct(native, F32)
    vmem = pltpu.VMEM
    flat = lambda array: array.reshape(LAYERS * ROWS, wide)
    outs = pl.pallas_call(
        functools.partial(kernel, nx, nz),
        out_shape=(out, out),
        in_specs=[hbm_space] * 5,
        out_specs=(vmem_space, vmem_space),
        scratch_shapes=[
            vmem((LAYERS * ROWS, wide), jnp.bfloat16),
            vmem((LAYERS * ROWS, wide), jnp.bfloat16),
            vmem((ROWS, wide), jnp.int32),
            vmem((ROWS, wide), jnp.int32),
            vmem((ROWS, wide), F32),
            vmem(native, F32),
            vmem(native, F32),
            vmem(native, F32),
            vmem((COUPLING + 1, CHUNKS + 2, ROWS, TILES, SUB, LANES), F32),
            vmem((FIELDS, CHUNKS, 2, 2, TILES, SUB, LANES), F32),
            vmem((FIELDS, CHUNKS, 2, SUB, LANES), F32),
            vmem((FIELDS, CHUNKS, 4, 1, LANES), F32),
            vmem((FIELDS + 1, CHUNKS, SUB, LANES), F32),
            vmem((FIELDS + 1, CHUNKS, 1, LANES), F32),
            vmem(field, F32),
            vmem(field, F32),
            vmem(field, F32),
            vmem(field, F32),
            vmem((SUB, SUB, SUB, LANES), F32),
            vmem((TILES, ROWS, LANES), F32),
            vmem((TILES, ROWS, LANES), F32),
            vmem((1, LANES), F32),
            vmem((nx, 1, LANES), F32),
            vmem((1, LANES), F32),
            vmem((nz, 1, LANES), F32),
            pltpu.SemaphoreType.DMA((6,)),
            pltpu.SemaphoreType.DMA((8,)),
            pltpu.SemaphoreType.DMA((2, CHUNKS, 3)),
            pltpu.SemaphoreType.DMA((2,)),
            pltpu.SemaphoreType.DMA((2, 2)),
        ],
        compiler_params=pltpu.CompilerParams(collective_id=0, has_side_effects=True, vmem_limit_bytes=40 * 1024 * 1024),
        name="coupled_solve",
    )(*[pltpu.with_memory_space_constraint(v, pltpu.HBM)
        for v in (flat(forcing), flat(conduct), flat(diag_add), ice_mask, grounded)])
    return tuple(
        v.reshape(TILES, LAYERS, ROWS, LANES).transpose(1, 2, 0, 3).reshape(1, LAYERS, ROWS, wide)
        for v in outs)


def solution(mesh):
    block = P("group", None, "gx", "gy")
    columns = P("gx", "gy")
    return jax.shard_map(
        functools.partial(on_device, mesh.shape["gx"], mesh.shape["gy"]),
        mesh=mesh,
        in_specs=(block, block, block, columns, columns),
        out_specs=(block, block),
        check_vma=False,
    )
```

```python
import functools

import jax
import jax.numpy as jnp
from jax import lax
from jax.experimental import pallas as pl
from jax.experimental.pallas import tpu as pltpu
from jax.sharding import PartitionSpec as P

ITERS = 6
FIELDS = ITERS + 1
COUPLING = FIELDS + 1
LAYERS = 80
ROWS = 8
SUB = 8
LANES = 128
TILES = 2
CHUNKS = LAYERS // SUB
EARLY = 4
MESH = pl.DeviceIdType.MESH
F32 = jnp.float32

far_weight = 0.25
cross_weight = 0.5
vertical_weight = 4.0
friction_gain = 8.0

STEPS = ((-1, 0), (1, 0), (0, -1), (0, 1), (-1, -1), (-1, 1), (1, -1), (1, 1))


def roll(value, shift, axis=None):
    return pltpu.roll(value, shift % value.shape[-1 if axis is None else axis],
                      value.ndim - 1 if axis is None else axis)


def far_first(count):
    return sorted(range(1, count), key=lambda i: -min(i, count - i))


def kernel(
    nx, nz,
    forcing, conduct, diag_add, ice_mask, grounded, out_x, out_r,
    cbf, dbf, ice_v, ground_v, active_v, fs, cn, dn,
    wbuf, hx, hz, hc, pz, pc, ebuf, hbuf, icbuf, gbuf, acc,
    shared_out, shared_in, ar_own, ar_x, ar_own2, ar_z,
    in_sem, send_sem, recv_sem, share_sem, ar_sem,
):
    g = lax.axis_index("group")
    x = lax.axis_index("gx")
    z = lax.axis_index("gy")

    lane2 = lax.broadcasted_iota(jnp.int32, (SUB, LANES), 1)
    sub2 = lax.broadcasted_iota(jnp.int32, (SUB, LANES), 0)
    lane3 = lax.broadcasted_iota(jnp.int32, (ROWS, SUB, LANES), 2)
    sub3 = lax.broadcasted_iota(jnp.int32, (ROWS, SUB, LANES), 1)
    lane1 = lax.broadcasted_iota(jnp.int32, (1, LANES), 1)

    beside_x = (x > 0).astype(jnp.int32) + (x < nx - 1).astype(jnp.int32)
    beside_z = (z > 0).astype(jnp.int32) + (z < nz - 1).astype(jnp.int32)

    def exists(d):
        dx, dz = STEPS[d]
        conds = []
        if dx < 0:
            conds.append(x > 0)
        if dx > 0:
            conds.append(x < nx - 1)
        if dz < 0:
            conds.append(z > 0)
        if dz > 0:
            conds.append(z < nz - 1)
        return functools.reduce(jnp.logical_and, conds)

    def at(d):
        dx, dz = STEPS[d]
        return (g, x + dx, z + dz)

    barrier = pltpu.get_barrier_semaphore()
    pl.semaphore_signal(barrier, inc=1, device_id=(g, (x + nx // 2) % nx, z), device_id_type=MESH)
    for d in (4, 5, 6, 7, 0, 1, 2, 3):
        @pl.when(exists(d))
        def _(d=d):
            pl.semaphore_signal(barrier, inc=1, device_id=at(d), device_id_type=MESH)
    pl.semaphore_signal(barrier, inc=1, device_id=(1 - g, x, z), device_id_type=MESH)

    loads = [
        pltpu.make_async_copy(conduct, cbf, in_sem.at[0]),
        pltpu.make_async_copy(ice_mask, ice_v, in_sem.at[1]),
        pltpu.make_async_copy(grounded, ground_v, in_sem.at[2]),
        pltpu.make_async_copy(forcing.at[:, pl.ds(0, LANES)], fs.at[0], in_sem.at[3]),
        pltpu.make_async_copy(forcing.at[:, pl.ds(LANES, LANES)], fs.at[1], in_sem.at[4]),
        pltpu.make_async_copy(diag_add, dbf, in_sem.at[5]),
    ]
    for load in loads:
        load.start()

    def zero_rims(d):
        @pl.when(jnp.logical_not(exists(d)))
        def _():
            def body(e, carry):
                if d < 2:
                    for j in range(CHUNKS):
                        hx[e, j, d] = jnp.zeros((2, TILES, SUB, LANES), F32)
                elif d < 4:
                    hz[e, :, d - 2] = jnp.zeros((CHUNKS, SUB, LANES), F32)
                else:
                    hc[e, :, d - 4] = jnp.zeros((CHUNKS, 1, LANES), F32)
                return carry
            lax.fori_loop(0, FIELDS, body, 0)

    for d in range(8):
        zero_rims(d)

    acc[...] = jnp.zeros_like(acc)

    def clear(f, carry):
        for j in range(CHUNKS):
            wbuf[f, j + 1] = jnp.zeros((ROWS, TILES, SUB, LANES), F32)
        return carry

    lax.fori_loop(0, FIELDS + 1, clear, 0)

    loads[0].wait()
    loads[1].wait()
    loads[2].wait()
    is_ice = jnp.where(g == 0, 1.0, 0.0).astype(F32)
    ice = ice_v[...].astype(F32)
    ground = ground_v[...].astype(F32)
    active_v[...] = ice * (1.0 - (1.0 - is_ice) * ground)

    def couple(i, carry):
        part = pl.ds(pl.multiple_of(i * SUB * ROWS, SUB * ROWS), SUB * ROWS)
        for t in range(TILES):
            columns = slice(t * LANES, (t + 1) * LANES)
            value = jnp.sqrt(cbf[part, columns].astype(F32)).reshape(SUB, ROWS, LANES)
            cn[t, part] = (value * active_v[:, columns][None]).reshape(SUB * ROWS, LANES)
        return carry

    lax.fori_loop(0, CHUNKS, couple, 0)


    def pick(ref, j, t):
        return jnp.stack([ref[t, pl.ds(j * ROWS + r, SUB, stride=CHUNKS * ROWS), :] for r in range(ROWS)])

    def put(ref, j, t, value):
        for r in range(ROWS):
            ref[t, pl.ds(j * ROWS + r, SUB, stride=CHUNKS * ROWS), :] = value[r]

    def copies(e, j, d):
        f = COUPLING if isinstance(e, int) and e == 0 else e
        if d == 0:
            src, dst = wbuf.at[f, j + 1, pl.ds(0, 2)], hx.at[e, j, 1]
        elif d == 1:
            src, dst = wbuf.at[f, j + 1, pl.ds(ROWS - 2, 2)], hx.at[e, j, 0]
        elif d < 4:
            src, dst = pz.at[e, j], hz.at[e, j, 3 - d]
        else:
            src, dst = pc.at[e, j], hc.at[e, j, 7 - d]
        return pltpu.make_async_remote_copy(
            src_ref=src, dst_ref=dst, send_sem=send_sem.at[min(d // 2, 2)],
            recv_sem=recv_sem.at[e % 2, j, min(d // 2, 2)], device_id=at(d), device_id_type=MESH)

    def store_field(f, j, parts):
        for t in range(TILES):
            wbuf[f, j + 1, :, t] = parts[t]

        @pl.when(j == 0)
        def _():
            for t in range(TILES):
                wbuf[f, CHUNKS + 1, :, t] = jnp.where(sub3 < SUB - 1, roll(parts[t], SUB - 1, 1), 0.0)

        @pl.when(j == CHUNKS - 1)
        def _():
            for t in range(TILES):
                wbuf[f, 0, :, t] = jnp.where(sub3 > 0, roll(parts[t], 1, 1), 0.0)

    def pack_rims(e, j, parts):
        none = jnp.zeros((1, SUB, LANES), F32)
        crossed, scaled = [], []
        for t in range(TILES):
            wide = jnp.concatenate([none, parts[t], none], axis=0)
            crossed.append(parts[t] + cross_weight * (wide[0:8] + wide[2:10]))
            scaled.append(far_weight * parts[t])
        sources = (
            (jnp.where(lane3 == LANES - 1, crossed[1], 0.0), 1),
            (jnp.where(lane3 == 0, crossed[0], 0.0), -1),
            (jnp.where(lane3 >= LANES - 2, scaled[1], 0.0), 2),
            (jnp.where(lane3 < 2, scaled[0], 0.0), -2),
        )
        packed = None
        for source, shift in sources:
            for r in range(ROWS):
                moved = roll(source[r], 4 * (r + 1) + shift)
                packed = moved if packed is None else packed + moved
        pz[e, j] = packed
        corners = None
        for q in range(4):
            row, tile = (0, ROWS - 1)[q // 2], q % 2
            lane = (0, LANES - 1)[tile]
            only = jnp.where(lane2 == lane, cross_weight * parts[tile][row], 0.0)
            moved = pltpu.roll(only, (8 * q - lane) % LANES, 1, stride=1, stride_axis=0)
            corners = moved if corners is None else corners + moved
        pc[e, j] = jnp.sum(corners, axis=0, keepdims=True)

    def send_rims(e, j, wanted):
        for d in (4, 5, 6, 7, 2, 3, 0, 1):
            @pl.when(exists(d) if wanted is None else jnp.logical_and(exists(d), wanted))
            def _(d=d):
                copies(e, j, d).start()

    def await_rims(e, j):
        def arrive(kind, condition, whole):
            @pl.when(condition)
            def _():
                pltpu.make_async_copy(whole, whole, recv_sem.at[e % 2, j, kind]).wait()

        both = beside_x * beside_z
        arrive(0, beside_x == 2, hx.at[e, j])
        arrive(0, beside_x == 1, hx.at[e, j, 0])
        arrive(1, beside_z == 2, hz.at[e, j])
        arrive(1, beside_z == 1, hz.at[e, j, 0])
        arrive(2, both == 4, hc.at[e, j])
        arrive(2, both == 2, hc.at[e, j, pl.ds(0, 2)])
        arrive(2, both == 1, hc.at[e, j, 0])

    def spread(f, e, j):
        centre = [wbuf[f, j + 1, :, t] for t in range(TILES)]
        beside, mixed, scaled = [], [], []
        for t in range(TILES):
            wide = jnp.concatenate([hx[e, j, 0, :, t], centre[t], hx[e, j, 1, :, t]], axis=0)
            near = wide[1:9] + wide[3:11]
            far = wide[0:8] + wide[4:12]
            vertical = wbuf[f, j, :, t] + wbuf[f, j + 2, :, t]
            beside.append(near + far_weight * far + vertical_weight * vertical)
            mixed.append(centre[t] + cross_weight * near)
            scaled.append(far_weight * centre[t])
        for source, shift in ((mixed, 1), (scaled, 2)):
            a, b = roll(source[0], shift), roll(source[1], shift)
            beside[0] = beside[0] + jnp.where(lane3 < shift, 0.0, a)
            beside[1] = beside[1] + jnp.where(lane3 < shift, a, b)
            a, b = roll(source[0], -shift), roll(source[1], -shift)
            beside[0] = beside[0] + jnp.where(lane3 >= LANES - shift, b, a)
            beside[1] = beside[1] + jnp.where(lane3 >= LANES - shift, 0.0, b)

        edge = jnp.where(lane2 % 4 < 2, hz[e, j, 0], hz[e, j, 1])
        rows = [roll(edge, -4 * (r + 1)) for r in range(ROWS)]
        corner = []
        for q in range(4):
            picked = jnp.where(lane2 == 8 * (3 - q) + sub2, jnp.broadcast_to(hc[e, j, q], (SUB, LANES)), 0.0)
            corner.append(jnp.sum(picked, axis=1, keepdims=True))
        rows[0] = rows[0] + jnp.where(lane2 == 0, corner[0], jnp.where(lane2 == LANES - 1, corner[1], 0.0))
        rows[-1] = rows[-1] + jnp.where(lane2 == 0, corner[2], jnp.where(lane2 == LANES - 1, corner[3], 0.0))
        rows = jnp.stack(rows)
        return [beside[0] + jnp.where(lane3 < 2, rows, 0.0),
                beside[1] + jnp.where(lane3 >= LANES - 2, rows, 0.0)]

    def dots(k, j, applied):
        field = [wbuf[k + 1, j + 1, :, t] for t in range(TILES)]
        weighted = [hbuf[j, :, t] * (field[t] - 0.5 * applied[t]) for t in range(TILES)]
        for i in range(ITERS):
            product = [jnp.sum(weighted[t] * wbuf[i + 1, j + 1, :, t], axis=0) for t in range(TILES)]
            acc[k, i] = acc[k, i] + (product[0] + product[1])
        product = [jnp.sum(hbuf[j, :, t] * field[t] * wbuf[1, j + 1, :, t], axis=0) for t in range(TILES)]
        acc[k, ITERS] = acc[k, ITERS] + (product[0] + product[1])

    def first(j, carry):
        parts = [pick(cn, j, t) for t in range(TILES)]
        store_field(COUPLING, j, parts)
        pack_rims(0, j, parts)
        return carry

    def send_first(j, carry):
        send_rims(0, j, None)
        return carry

    def first_and_send(j, carry):
        first(j, carry)
        return send_first(j, carry)

    lax.fori_loop(0, EARLY, first, 0)
    pl.semaphore_wait(barrier, 2 + beside_x + beside_z + beside_x * beside_z)
    lax.fori_loop(0, EARLY, send_first, 0)
    lax.fori_loop(EARLY, CHUNKS, first_and_send, 0)

    loads[3].wait()
    loads[4].wait()
    edge = pl.ds(pl.multiple_of(g * ((LAYERS - 1) * ROWS), ROWS), ROWS)
    for t in range(TILES):
        mean = jnp.sum(fs[t].reshape(LAYERS, ROWS, LANES), axis=0) * (1.0 / LAYERS)
        value = active_v[:, t * LANES:(t + 1) * LANES] * mean
        shared_out[t] = value * cn[t, edge]
    loads[5].wait()

    def widen(i, carry):
        part = pl.ds(pl.multiple_of(i * SUB * ROWS, SUB * ROWS), SUB * ROWS)
        for t in range(TILES):
            dn[t, part] = dbf[part, t * LANES:(t + 1) * LANES].astype(F32)
        return carry

    lax.fori_loop(0, CHUNKS, widen, 0)
    for t in range(TILES):
        columns = slice(t * LANES, (t + 1) * LANES)
        friction = is_ice * friction_gain * (ground_v[:, columns].astype(F32) * ice_v[:, columns].astype(F32))
        dn[t, 0:ROWS] = dn[t, 0:ROWS] + friction

    share = pltpu.make_async_remote_copy(
        src_ref=shared_out, dst_ref=shared_in, send_sem=share_sem.at[0], recv_sem=share_sem.at[1],
        device_id=(1 - g, x, z), device_id_type=MESH)
    share.start()

    share.wait()
    for t in range(TILES):
        fs[t, edge] = fs[t, edge] + shared_in[t]

    def second(j, carry):
        await_rims(0, j)
        spreads = spread(COUPLING, 0, j)
        parts = []
        for t in range(TILES):
            c = wbuf[COUPLING, j + 1, :, t]
            diagonal = pick(dn, j, t) + c * spreads[t]
            ratio = c / diagonal
            inverse_c = jnp.where(c > 0.0, 1.0 / jnp.where(c > 0.0, c, 1.0), 0.0)
            back = diagonal * inverse_c
            ebuf[j, :, t] = 2.0 * ratio * c
            icbuf[j, :, t] = inverse_c
            gbuf[j, :, t] = back
            hbuf[j, :, t] = back * inverse_c
            parts.append(ratio * pick(fs, j, t))
        store_field(1, j, parts)
        pack_rims(1, j, parts)
        send_rims(1, j, None)
        return carry

    lax.fori_loop(0, CHUNKS, second, 0)

    def stage(k, carry):
        def body(j, inner):
            await_rims(k, j)
            spreads = spread(k, k, j)
            applied = [ebuf[j, :, t] * spreads[t] for t in range(TILES)]
            parts = [applied[t] - wbuf[k - 1, j + 1, :, t] for t in range(TILES)]
            store_field(k + 1, j, parts)
            pack_rims(k + 1, j, parts)
            dots(k - 1, j, applied)
            send_rims(k + 1, j, k < ITERS)
            return inner

        return lax.fori_loop(0, CHUNKS, body, carry)

    lax.fori_loop(1, ITERS + 1, stage, 0)

    gram = jnp.zeros((SUB, LANES), F32)
    for k in range(ITERS):
        column = jnp.sum(jnp.sum(acc[k], axis=1), axis=1, keepdims=True)
        wanted = (lane2 == SUB * sub2 + k) & ((sub2 <= k) | (sub2 == ITERS))
        gram = gram + jnp.where(wanted, column, 0.0)
    row = jnp.sum(gram, axis=0, keepdims=True)
    ar_own[...] = row

    def scatter(own, slots, me, count, offsets, device, sems):
        for offset in offsets:
            pltpu.make_async_remote_copy(
                src_ref=own, dst_ref=slots.at[me], send_sem=sems.at[0], recv_sem=sems.at[1],
                device_id=device((me + offset) % count), device_id_type=MESH).start()
        slots[me] = own[...]
        rest = slots.at[pl.ds(0, count - 1)]
        pltpu.make_async_copy(rest, rest, sems.at[1]).wait()
        return jnp.sum(slots[...], axis=0)

    ar_own2[...] = scatter(ar_own, ar_x, x, nx, far_first(nx), lambda i: (g, i, z), ar_sem.at[0])
    total = scatter(ar_own2, ar_z, z, nz, far_first(nz), lambda i: (g, x, i), ar_sem.at[1])

    total = jnp.broadcast_to(total, (SUB, LANES))

    def entry(i, k):
        lane = SUB * i + k
        return jnp.broadcast_to(total[:, lane:lane + 1], (SUB, LANES))

    system = {(i, k): entry(i, k) for k in range(ITERS) for i in range(k + 1)}
    right = [entry(ITERS, k) for k in range(ITERS)]
    inverse = []
    for p in range(ITERS):
        inverse.append(1.0 / system[p, p])
        for i in range(p + 1, ITERS):
            factor = system[p, i] * inverse[p]
            for k in range(i, ITERS):
                system[i, k] = system[i, k] - factor * system[p, k]
            right[i] = right[i] - factor * right[p]
    a = [None] * ITERS
    for p in reversed(range(ITERS)):
        value = right[p]
        for k in range(p + 1, ITERS):
            value = value - system[p, k] * a[k]
        a[p] = value * inverse[p]
    b = [None] * FIELDS
    b[0] = 1.0 - a[0] + 0.5 * a[1]
    for k in range(1, ITERS - 1):
        b[k] = 0.5 * (a[k - 1] + a[k + 1]) - a[k]
    b[ITERS - 1] = 0.5 * a[ITERS - 2] - a[ITERS - 1]
    b[ITERS] = 0.5 * a[ITERS - 1]
    def combine(j, carry):
        for t in range(TILES):
            fields = [wbuf[k + 1, j + 1, :, t] for k in range(FIELDS)]
            up = a[0][None] * fields[0]
            down = b[0][None] * fields[0]
            for k in range(1, ITERS):
                up = up + a[k][None] * fields[k]
                down = down + b[k][None] * fields[k]
            down = down + b[ITERS][None] * fields[ITERS]
            put(out_x, j, t, icbuf[j, :, t] * up)
            put(out_r, j, t, gbuf[j, :, t] * down)
        return carry

    lax.fori_loop(0, CHUNKS, combine, 0)
    def left(kind, condition, whole):
        @pl.when(condition)
        def _():
            pltpu.make_async_copy(whole, whole, send_sem.at[kind]).wait()

    both = beside_x * beside_z
    left(0, beside_x == 2, hx)
    left(0, beside_x == 1, hx.at[:, :, 0])
    left(1, beside_z == 2, hz)
    left(1, beside_z == 1, hz.at[:, :, 0])
    left(2, both == 4, hc)
    left(2, both == 2, hc.at[:, :, pl.ds(0, 2)])
    left(2, both == 1, hc.at[:, :, 0])
    sent = ar_x.at[pl.ds(0, nx - 1)]
    pltpu.make_async_copy(sent, sent, ar_sem.at[0, 0]).wait()
    sent = ar_z.at[pl.ds(0, nz - 1)]
    pltpu.make_async_copy(sent, sent, ar_sem.at[1, 0]).wait()


def on_device(nx, nz, forcing, conduct, diag_add, ice_mask, grounded):
    field = (CHUNKS, ROWS, TILES, SUB, LANES)
    native = (TILES, LAYERS * ROWS, LANES)
    wide = TILES * LANES
    hbm_space = pl.BlockSpec(memory_space=pltpu.HBM)
    vmem_space = pl.BlockSpec(memory_space=pltpu.VMEM)
    out = jax.ShapeDtypeStruct(native, F32)
    vmem = pltpu.VMEM
    flat = lambda array: array.reshape(LAYERS * ROWS, wide)
    outs = pl.pallas_call(
        functools.partial(kernel, nx, nz),
        out_shape=(out, out),
        in_specs=[hbm_space] * 5,
        out_specs=(vmem_space, vmem_space),
        scratch_shapes=[
            vmem((LAYERS * ROWS, wide), jnp.bfloat16),
            vmem((LAYERS * ROWS, wide), jnp.bfloat16),
            vmem((ROWS, wide), jnp.int32),
            vmem((ROWS, wide), jnp.int32),
            vmem((ROWS, wide), F32),
            vmem(native, F32),
            vmem(native, F32),
            vmem(native, F32),
            vmem((COUPLING + 1, CHUNKS + 2, ROWS, TILES, SUB, LANES), F32),
            vmem((FIELDS, CHUNKS, 2, 2, TILES, SUB, LANES), F32),
            vmem((FIELDS, CHUNKS, 2, SUB, LANES), F32),
            vmem((FIELDS, CHUNKS, 4, 1, LANES), F32),
            vmem((FIELDS + 1, CHUNKS, SUB, LANES), F32),
            vmem((FIELDS + 1, CHUNKS, 1, LANES), F32),
            vmem(field, F32),
            vmem(field, F32),
            vmem(field, F32),
            vmem(field, F32),
            vmem((SUB, SUB, SUB, LANES), F32),
            vmem((TILES, ROWS, LANES), F32),
            vmem((TILES, ROWS, LANES), F32),
            vmem((1, LANES), F32),
            vmem((nx, 1, LANES), F32),
            vmem((1, LANES), F32),
            vmem((nz, 1, LANES), F32),
            pltpu.SemaphoreType.DMA((6,)),
            pltpu.SemaphoreType.DMA((3,)),
            pltpu.SemaphoreType.DMA((2, CHUNKS, 3)),
            pltpu.SemaphoreType.DMA((2,)),
            pltpu.SemaphoreType.DMA((2, 2)),
        ],
        compiler_params=pltpu.CompilerParams(collective_id=0, has_side_effects=True, vmem_limit_bytes=40 * 1024 * 1024),
        name="coupled_solve",
    )(*[pltpu.with_memory_space_constraint(v, pltpu.HBM)
        for v in (flat(forcing), flat(conduct), flat(diag_add), ice_mask, grounded)])
    return tuple(
        v.reshape(TILES, LAYERS, ROWS, LANES).transpose(1, 2, 0, 3).reshape(1, LAYERS, ROWS, wide)
        for v in outs)


def solution(mesh):
    block = P("group", None, "gx", "gy")
    columns = P("gx", "gy")
    return jax.shard_map(
        functools.partial(on_device, mesh.shape["gx"], mesh.shape["gy"]),
        mesh=mesh,
        in_specs=(block, block, block, columns, columns),
        out_specs=(block, block),
        check_vma=False,
    )
```

```python
import functools

import jax
import jax.numpy as jnp
from jax import lax
from jax.experimental import pallas as pl
from jax.experimental.pallas import tpu as pltpu
from jax.sharding import PartitionSpec as P

ITERS = 6
FIELDS = ITERS + 1
COUPLING = FIELDS + 1
LAYERS = 80
ROWS = 8
SUB = 8
LANES = 128
TILES = 2
CHUNKS = LAYERS // SUB
MESH = pl.DeviceIdType.MESH
F32 = jnp.float32

far_weight = 0.25
cross_weight = 0.5
vertical_weight = 4.0
friction_gain = 8.0

STEPS = ((-1, 0), (1, 0), (0, -1), (0, 1), (-1, -1), (-1, 1), (1, -1), (1, 1))


def roll(value, shift, axis=None):
    return pltpu.roll(value, shift % value.shape[-1 if axis is None else axis],
                      value.ndim - 1 if axis is None else axis)


def far_first(nx, nz):
    def hops(step):
        dx, dz = step
        return min(dx % 4, -dx % 4) + min(dx // 4, 4 - dx // 4) + min(dz, nz - dz)

    steps = [(dx, dz) for dx in range(nx) for dz in range(nz)]
    return sorted(steps[1:], key=lambda step: -hops(step))


def kernel(
    nx, nz,
    forcing, conduct, diag_add, ice_mask, grounded, out_x, out_r,
    cbf, dbf, ice_v, ground_v, active_v, fs, cn, dn,
    wbuf, hx, hz, hc, pz, pc, ebuf, hbuf, icbuf, gbuf, acc,
    shared_out, shared_in, ar_own, ar_all,
    in_sem, send_sem, recv_sem, share_sem, ar_sem,
):
    g = lax.axis_index("group")
    x = lax.axis_index("gx")
    z = lax.axis_index("gy")

    lane2 = lax.broadcasted_iota(jnp.int32, (SUB, LANES), 1)
    sub2 = lax.broadcasted_iota(jnp.int32, (SUB, LANES), 0)
    lane3 = lax.broadcasted_iota(jnp.int32, (ROWS, SUB, LANES), 2)
    sub3 = lax.broadcasted_iota(jnp.int32, (ROWS, SUB, LANES), 1)
    lane1 = lax.broadcasted_iota(jnp.int32, (1, LANES), 1)

    beside_x = (x > 0).astype(jnp.int32) + (x < nx - 1).astype(jnp.int32)
    beside_z = (z > 0).astype(jnp.int32) + (z < nz - 1).astype(jnp.int32)

    def exists(d):
        dx, dz = STEPS[d]
        conds = []
        if dx < 0:
            conds.append(x > 0)
        if dx > 0:
            conds.append(x < nx - 1)
        if dz < 0:
            conds.append(z > 0)
        if dz > 0:
            conds.append(z < nz - 1)
        return functools.reduce(jnp.logical_and, conds)

    def at(d):
        dx, dz = STEPS[d]
        return (g, x + dx, z + dz)

    barrier = pltpu.get_barrier_semaphore()
    pl.semaphore_signal(barrier, inc=1, device_id=(g, (x + nx // 2) % nx, z), device_id_type=MESH)
    for d in (4, 5, 6, 7, 0, 1, 2, 3):
        @pl.when(exists(d))
        def _(d=d):
            pl.semaphore_signal(barrier, inc=1, device_id=at(d), device_id_type=MESH)
    pl.semaphore_signal(barrier, inc=1, device_id=(1 - g, x, z), device_id_type=MESH)

    loads = [
        pltpu.make_async_copy(conduct.at[:, pl.ds(0, ROWS)], cbf.at[:, pl.ds(0, ROWS)], in_sem.at[0]),
        pltpu.make_async_copy(ice_mask, ice_v, in_sem.at[1]),
        pltpu.make_async_copy(grounded, ground_v, in_sem.at[2]),
        pltpu.make_async_copy(forcing.at[:, pl.ds(0, LANES)], fs.at[0], in_sem.at[3]),
        pltpu.make_async_copy(forcing.at[:, pl.ds(LANES, LANES)], fs.at[1], in_sem.at[4]),
        pltpu.make_async_copy(diag_add, dbf, in_sem.at[5]),
        pltpu.make_async_copy(conduct.at[:, pl.ds(ROWS, LAYERS - ROWS)], cbf.at[:, pl.ds(ROWS, LAYERS - ROWS)], in_sem.at[6]),
    ]
    for n in (0, 1, 2, 6, 3, 4, 5):
        loads[n].start()

    def zero_rims(d):
        @pl.when(jnp.logical_not(exists(d)))
        def _():
            def body(e, carry):
                if d < 2:
                    for j in range(CHUNKS):
                        hx[e, j, d] = jnp.zeros((2, TILES, SUB, LANES), F32)
                elif d < 4:
                    hz[e, :, d - 2] = jnp.zeros((CHUNKS, SUB, LANES), F32)
                else:
                    hc[e, :, d - 4] = jnp.zeros((CHUNKS, 1, LANES), F32)
                return carry
            lax.fori_loop(0, FIELDS, body, 0)

    for d in range(8):
        zero_rims(d)

    acc[...] = jnp.zeros_like(acc)

    def clear(f, carry):
        for j in range(CHUNKS):
            wbuf[f, j + 1] = jnp.zeros((ROWS, TILES, SUB, LANES), F32)
        return carry

    lax.fori_loop(0, FIELDS + 1, clear, 0)

    loads[0].wait()
    loads[1].wait()
    loads[2].wait()
    is_ice = jnp.where(g == 0, 1.0, 0.0).astype(F32)
    ice = ice_v[...].astype(F32)
    ground = ground_v[...].astype(F32)
    active_v[...] = ice * (1.0 - (1.0 - is_ice) * ground)

    def pick(ref, j, t):
        return jnp.stack([ref[t, pl.ds(j * ROWS + r, SUB, stride=CHUNKS * ROWS), :] for r in range(ROWS)])

    def couple(j):
        rows = pl.ds(pl.multiple_of(j * ROWS, ROWS), ROWS)
        base = pl.multiple_of(j * SUB * ROWS, SUB * ROWS)
        parts = []
        for t in range(TILES):
            columns = slice(t * LANES, (t + 1) * LANES)
            value = jnp.sqrt(cbf[:, rows, columns].astype(F32)) * active_v[:, columns][None]
            cn[t, pl.ds(base, SUB * ROWS)] = value.reshape(SUB * ROWS, LANES)
        for t in range(TILES):
            parts.append(jnp.stack([cn[t, pl.ds(base + r, SUB, stride=ROWS), :] for r in range(ROWS)]))
        return parts

    def put(ref, j, t, value):
        for r in range(ROWS):
            ref[t, pl.ds(j * ROWS + r, SUB, stride=CHUNKS * ROWS), :] = value[r]

    def copies(e, j, d):
        f = COUPLING if isinstance(e, int) and e == 0 else e
        if d == 0:
            src, dst = wbuf.at[f, j + 1, pl.ds(0, 2)], hx.at[e, j, 1]
        elif d == 1:
            src, dst = wbuf.at[f, j + 1, pl.ds(ROWS - 2, 2)], hx.at[e, j, 0]
        elif d < 4:
            src, dst = pz.at[e, j], hz.at[e, j, 3 - d]
        else:
            src, dst = pc.at[e, j], hc.at[e, j, 7 - d]
        return pltpu.make_async_remote_copy(
            src_ref=src, dst_ref=dst, send_sem=send_sem.at[min(d // 2, 2)],
            recv_sem=recv_sem.at[e % 2, j, min(d // 2, 2)], device_id=at(d), device_id_type=MESH)

    def store_field(f, j, parts):
        for t in range(TILES):
            wbuf[f, j + 1, :, t] = parts[t]

        @pl.when(j == 0)
        def _():
            for t in range(TILES):
                wbuf[f, CHUNKS + 1, :, t] = jnp.where(sub3 < SUB - 1, roll(parts[t], SUB - 1, 1), 0.0)

        @pl.when(j == CHUNKS - 1)
        def _():
            for t in range(TILES):
                wbuf[f, 0, :, t] = jnp.where(sub3 > 0, roll(parts[t], 1, 1), 0.0)

    def pack_rims(e, j, parts):
        none = jnp.zeros((1, SUB, LANES), F32)
        crossed, scaled = [], []
        for t in range(TILES):
            wide = jnp.concatenate([none, parts[t], none], axis=0)
            crossed.append(parts[t] + cross_weight * (wide[0:8] + wide[2:10]))
            scaled.append(far_weight * parts[t])
        sources = (
            (jnp.where(lane3 == LANES - 1, crossed[1], 0.0), 1),
            (jnp.where(lane3 == 0, crossed[0], 0.0), -1),
            (jnp.where(lane3 >= LANES - 2, scaled[1], 0.0), 2),
            (jnp.where(lane3 < 2, scaled[0], 0.0), -2),
        )
        packed = None
        for source, shift in sources:
            for r in range(ROWS):
                moved = roll(source[r], 4 * (r + 1) + shift)
                packed = moved if packed is None else packed + moved
        pz[e, j] = packed
        corners = None
        for q in range(4):
            row, tile = (0, ROWS - 1)[q // 2], q % 2
            lane = (0, LANES - 1)[tile]
            only = jnp.where(lane2 == lane, cross_weight * parts[tile][row], 0.0)
            moved = pltpu.roll(only, (8 * q - lane) % LANES, 1, stride=1, stride_axis=0)
            corners = moved if corners is None else corners + moved
        pc[e, j] = jnp.sum(corners, axis=0, keepdims=True)

    def send_rims(e, j):
        for d in (4, 5, 6, 7, 2, 3, 0, 1):
            @pl.when(exists(d))
            def _(d=d):
                copies(e, j, d).start()

    def arrive(e, j, kind, condition, whole):
        @pl.when(condition)
        def _():
            pltpu.make_async_copy(whole, whole, recv_sem.at[e % 2, j, kind]).wait()

    def await_rims(e, j):
        arrive(e, j, 0, beside_x == 2, hx.at[e, j])
        arrive(e, j, 0, beside_x == 1, hx.at[e, j, 0])
        arrive(e, j, 1, beside_z == 2, hz.at[e, j])
        arrive(e, j, 1, beside_z == 1, hz.at[e, j, 0])

    def await_corners(e, j):
        both = beside_x * beside_z
        arrive(e, j, 2, both == 4, hc.at[e, j])
        arrive(e, j, 2, both == 2, hc.at[e, j, pl.ds(0, 2)])
        arrive(e, j, 2, both == 1, hc.at[e, j, 0])

    def spread(f, e, j, late):
        await_rims(e, j)
        if not late:
            await_corners(e, j)
        centre = [wbuf[f, j + 1, :, t] for t in range(TILES)]
        beside, mixed, scaled = [], [], []
        for t in range(TILES):
            wide = jnp.concatenate([hx[e, j, 0, :, t], centre[t], hx[e, j, 1, :, t]], axis=0)
            near = wide[1:9] + wide[3:11]
            far = wide[0:8] + wide[4:12]
            vertical = wbuf[f, j, :, t] + wbuf[f, j + 2, :, t]
            beside.append(near + far_weight * far + vertical_weight * vertical)
            mixed.append(centre[t] + cross_weight * near)
            scaled.append(far_weight * centre[t])
        for source, shift in ((mixed, 1), (scaled, 2)):
            a, b = roll(source[0], shift), roll(source[1], shift)
            beside[0] = beside[0] + jnp.where(lane3 < shift, 0.0, a)
            beside[1] = beside[1] + jnp.where(lane3 < shift, a, b)
            a, b = roll(source[0], -shift), roll(source[1], -shift)
            beside[0] = beside[0] + jnp.where(lane3 >= LANES - shift, b, a)
            beside[1] = beside[1] + jnp.where(lane3 >= LANES - shift, 0.0, b)

        edge = jnp.where(lane2 % 4 < 2, hz[e, j, 0], hz[e, j, 1])
        rows = jnp.stack([roll(edge, -4 * (r + 1)) for r in range(ROWS)])
        beside[0] = beside[0] + jnp.where(lane3 < 2, rows, 0.0)
        beside[1] = beside[1] + jnp.where(lane3 >= LANES - 2, rows, 0.0)
        if late:
            await_corners(e, j)
        corner = []
        for q in range(4):
            picked = jnp.where(lane2 == 8 * (3 - q) + sub2, jnp.broadcast_to(hc[e, j, q], (SUB, LANES)), 0.0)
            corner.append(jnp.sum(picked, axis=1, keepdims=True))
        for t, lane in ((0, 0), (1, LANES - 1)):
            low, high = [jnp.where(lane2 == lane, corner[q + t], 0.0)[None] for q in (0, 2)]
            beside[t] = jnp.concatenate([beside[t][:1] + low, beside[t][1:-1], beside[t][-1:] + high], axis=0)
        return beside

    def dots(k, j, applied):
        field = [wbuf[k + 1, j + 1, :, t] for t in range(TILES)]
        weighted = [hbuf[j, :, t] * (field[t] - 0.5 * applied[t]) for t in range(TILES)]
        for i in range(ITERS):
            product = [jnp.sum(weighted[t] * wbuf[i + 1, j + 1, :, t], axis=0) for t in range(TILES)]
            acc[k, i] = acc[k, i] + (product[0] + product[1])
        product = [jnp.sum(hbuf[j, :, t] * field[t] * wbuf[1, j + 1, :, t], axis=0) for t in range(TILES)]
        acc[k, ITERS] = acc[k, ITERS] + (product[0] + product[1])

    def first(j):
        parts = couple(j)
        store_field(COUPLING, j, parts)
        pack_rims(0, j, parts)

    def first_and_send(j, carry):
        first(j)
        send_rims(0, j)
        return carry

    first(jnp.int32(0))
    pl.semaphore_wait(barrier, 2 + beside_x + beside_z + beside_x * beside_z)
    send_rims(0, jnp.int32(0))
    loads[6].wait()
    lax.fori_loop(1, CHUNKS, first_and_send, 0)

    loads[3].wait()
    loads[4].wait()
    edge = pl.ds(pl.multiple_of(g * ((LAYERS - 1) * ROWS), ROWS), ROWS)
    for t in range(TILES):
        mean = jnp.sum(fs[t].reshape(LAYERS, ROWS, LANES), axis=0) * (1.0 / LAYERS)
        value = active_v[:, t * LANES:(t + 1) * LANES] * mean
        shared_out[t] = value * cn[t, edge]
    share = pltpu.make_async_remote_copy(
        src_ref=shared_out, dst_ref=shared_in, send_sem=share_sem.at[0], recv_sem=share_sem.at[1],
        device_id=(1 - g, x, z), device_id_type=MESH)
    share.start()
    loads[5].wait()

    def widen(i, carry):
        part = pl.ds(pl.multiple_of(i * SUB * ROWS, SUB * ROWS), SUB * ROWS)
        for t in range(TILES):
            dn[t, part] = dbf[part, t * LANES:(t + 1) * LANES].astype(F32)
        return carry

    lax.fori_loop(0, CHUNKS, widen, 0)
    for t in range(TILES):
        columns = slice(t * LANES, (t + 1) * LANES)
        friction = is_ice * friction_gain * (ground_v[:, columns].astype(F32) * ice_v[:, columns].astype(F32))
        dn[t, 0:ROWS] = dn[t, 0:ROWS] + friction

    def turn(source, target):
        def body(j, carry):
            for t in range(TILES):
                target[j, :, t] = pick(source, j, t)
            return carry

        lax.fori_loop(0, CHUNKS, body, 0)

    turn(dn, gbuf)
    share.wait()
    for t in range(TILES):
        fs[t, edge] = fs[t, edge] + shared_in[t]
    turn(fs, hbuf)

    def second(j, late):
        spreads = spread(COUPLING, 0, j, late)
        couplings = [wbuf[COUPLING, j + 1, :, t] for t in range(TILES)]
        diagonals = [gbuf[j, :, t] + couplings[t] * spreads[t] for t in range(TILES)]
        ratios = [couplings[t] / diagonals[t] for t in range(TILES)]
        parts = [ratios[t] * hbuf[j, :, t] for t in range(TILES)]
        store_field(1, j, parts)
        pack_rims(1, j, parts)
        for t in range(TILES):
            c = couplings[t]
            inverse_c = jnp.where(c > 0.0, 1.0 / jnp.where(c > 0.0, c, 1.0), 0.0)
            back = diagonals[t] * inverse_c
            ebuf[j, :, t] = 2.0 * ratios[t] * c
            icbuf[j, :, t] = inverse_c
            gbuf[j, :, t] = back
            hbuf[j, :, t] = back * inverse_c
        send_rims(1, j)

    def chunks(step):
        def body(j, carry):
            step(j, False)
            return carry

        step(jnp.int32(0), True)
        lax.fori_loop(1, CHUNKS, body, 0)

    chunks(second)

    def stage(k, last):
        def step(j, late):
            spreads = spread(k, k, j, late)
            applied = [ebuf[j, :, t] * spreads[t] for t in range(TILES)]
            parts = [applied[t] - wbuf[k - 1, j + 1, :, t] for t in range(TILES)]
            if last:
                wbuf[k + 1, j + 1] = jnp.stack(parts, axis=1)
            else:
                store_field(k + 1, j, parts)
                pack_rims(k + 1, j, parts)
                if not late:
                    dots(k - 1, j, applied)
                send_rims(k + 1, j)
            if last or late:
                dots(k - 1, j, applied)

        chunks(step)

    def middle(k, carry):
        stage(k, False)
        return carry

    lax.fori_loop(1, ITERS, middle, 0)
    stage(ITERS, True)

    gram = jnp.zeros((SUB, LANES), F32)
    for k in range(ITERS):
        column = jnp.sum(jnp.sum(acc[k], axis=1), axis=1, keepdims=True)
        wanted = (lane2 == SUB * sub2 + k) & ((sub2 <= k) | (sub2 == ITERS))
        gram = gram + jnp.where(wanted, column, 0.0)
    row = jnp.sum(gram, axis=0, keepdims=True)
    ar_own[...] = row
    mine = x * nz + z
    for dx, dz in far_first(nx, nz):
        to_x, to_z = (x + dx) % nx, (z + dz) % nz
        pltpu.make_async_remote_copy(
            src_ref=ar_own, dst_ref=ar_all.at[mine], send_sem=ar_sem.at[0], recv_sem=ar_sem.at[1],
            device_id=(g, to_x, to_z), device_id_type=MESH).start()
    ar_all[mine] = row
    rest = ar_all.at[pl.ds(0, nx * nz - 1)]
    pltpu.make_async_copy(rest, rest, ar_sem.at[1]).wait()
    total = ar_all[...].reshape(nx, nz, 1, LANES)
    total = jnp.sum(jnp.sum(total, axis=0), axis=0)

    total = jnp.broadcast_to(total, (SUB, LANES))

    def entry(i, k):
        lane = SUB * i + k
        return jnp.broadcast_to(total[:, lane:lane + 1], (SUB, LANES))

    system = {(i, k): entry(i, k) for k in range(ITERS) for i in range(k + 1)}
    right = [entry(ITERS, k) for k in range(ITERS)]
    inverse = []
    for p in range(ITERS):
        inverse.append(1.0 / system[p, p])
        for i in range(p + 1, ITERS):
            factor = system[p, i] * inverse[p]
            for k in range(i, ITERS):
                system[i, k] = system[i, k] - factor * system[p, k]
            right[i] = right[i] - factor * right[p]
    a = [None] * ITERS
    for p in reversed(range(ITERS)):
        value = right[p]
        for k in range(p + 1, ITERS):
            value = value - system[p, k] * a[k]
        a[p] = value * inverse[p]
    b = [None] * FIELDS
    b[0] = 1.0 - a[0] + 0.5 * a[1]
    for k in range(1, ITERS - 1):
        b[k] = 0.5 * (a[k - 1] + a[k + 1]) - a[k]
    b[ITERS - 1] = 0.5 * a[ITERS - 2] - a[ITERS - 1]
    b[ITERS] = 0.5 * a[ITERS - 1]
    def combine(j, carry):
        for t in range(TILES):
            fields = [wbuf[k + 1, j + 1, :, t] for k in range(FIELDS)]
            up = a[0][None] * fields[0]
            down = b[0][None] * fields[0]
            for k in range(1, ITERS):
                up = up + a[k][None] * fields[k]
                down = down + b[k][None] * fields[k]
            down = down + b[ITERS][None] * fields[ITERS]
            put(out_x, j, t, icbuf[j, :, t] * up)
            put(out_r, j, t, gbuf[j, :, t] * down)
        return carry

    lax.fori_loop(0, CHUNKS, combine, 0)
    def left(kind, condition, whole):
        @pl.when(condition)
        def _():
            pltpu.make_async_copy(whole, whole, send_sem.at[kind]).wait()

    both = beside_x * beside_z
    left(0, beside_x == 2, hx)
    left(0, beside_x == 1, hx.at[:, :, 0])
    left(1, beside_z == 2, hz)
    left(1, beside_z == 1, hz.at[:, :, 0])
    left(2, both == 4, hc)
    left(2, both == 2, hc.at[:, :, pl.ds(0, 2)])
    left(2, both == 1, hc.at[:, :, 0])
    pltpu.make_async_copy(rest, rest, ar_sem.at[0]).wait()


def on_device(nx, nz, forcing, conduct, diag_add, ice_mask, grounded):
    field = (CHUNKS, ROWS, TILES, SUB, LANES)
    native = (TILES, LAYERS * ROWS, LANES)
    wide = TILES * LANES
    hbm_space = pl.BlockSpec(memory_space=pltpu.HBM)
    vmem_space = pl.BlockSpec(memory_space=pltpu.VMEM)
    out = jax.ShapeDtypeStruct(native, F32)
    vmem = pltpu.VMEM
    flat = lambda array: array.reshape(LAYERS * ROWS, wide)
    outs = pl.pallas_call(
        functools.partial(kernel, nx, nz),
        out_shape=(out, out),
        in_specs=[hbm_space] * 5,
        out_specs=(vmem_space, vmem_space),
        scratch_shapes=[
            vmem((SUB, CHUNKS * ROWS, wide), jnp.bfloat16),
            vmem((LAYERS * ROWS, wide), jnp.bfloat16),
            vmem((ROWS, wide), jnp.int32),
            vmem((ROWS, wide), jnp.int32),
            vmem((ROWS, wide), F32),
            vmem(native, F32),
            vmem(native, F32),
            vmem(native, F32),
            vmem((COUPLING + 1, CHUNKS + 2, ROWS, TILES, SUB, LANES), F32),
            vmem((FIELDS, CHUNKS, 2, 2, TILES, SUB, LANES), F32),
            vmem((FIELDS, CHUNKS, 2, SUB, LANES), F32),
            vmem((FIELDS, CHUNKS, 4, 1, LANES), F32),
            vmem((FIELDS, CHUNKS, SUB, LANES), F32),
            vmem((FIELDS, CHUNKS, 1, LANES), F32),
            vmem(field, F32),
            vmem(field, F32),
            vmem(field, F32),
            vmem(field, F32),
            vmem((SUB, SUB, SUB, LANES), F32),
            vmem((TILES, ROWS, LANES), F32),
            vmem((TILES, ROWS, LANES), F32),
            vmem((1, LANES), F32),
            vmem((nx * nz, 1, LANES), F32),
            pltpu.SemaphoreType.DMA((7,)),
            pltpu.SemaphoreType.DMA((3,)),
            pltpu.SemaphoreType.DMA((2, CHUNKS, 3)),
            pltpu.SemaphoreType.DMA((2,)),
            pltpu.SemaphoreType.DMA((2,)),
        ],
        compiler_params=pltpu.CompilerParams(collective_id=0, has_side_effects=True, vmem_limit_bytes=40 * 1024 * 1024),
        name="coupled_solve",
    )(*[pltpu.with_memory_space_constraint(v, pltpu.HBM)
        for v in (flat(forcing), conduct.reshape(SUB, CHUNKS * ROWS, wide), flat(diag_add), ice_mask, grounded)])
    return tuple(
        v.reshape(TILES, LAYERS, ROWS, LANES).transpose(1, 2, 0, 3).reshape(1, LAYERS, ROWS, wide)
        for v in outs)


def solution(mesh):
    block = P("group", None, "gx", "gy")
    columns = P("gx", "gy")
    return jax.shard_map(
        functools.partial(on_device, mesh.shape["gx"], mesh.shape["gy"]),
        mesh=mesh,
        in_specs=(block, block, block, columns, columns),
        out_specs=(block, block),
        check_vma=False,
    )
```

```python
import functools

import jax
import jax.numpy as jnp
from jax import lax
from jax.experimental import pallas as pl
from jax.experimental.pallas import tpu as pltpu
from jax.sharding import PartitionSpec as P

ITERS = 6
FIELDS = ITERS + 1
CORNERED = FIELDS - 1
COUPLING = FIELDS + 1
LAYERS = 80
ROWS = 8
SUB = 8
LANES = 128
TILES = 2
CHUNKS = LAYERS // SUB
MESH = pl.DeviceIdType.MESH
F32 = jnp.float32

far_weight = 0.25
cross_weight = 0.5
vertical_weight = 4.0
friction_gain = 8.0

STEPS = ((-1, 0), (1, 0), (0, -1), (0, 1), (-1, -1), (-1, 1), (1, -1), (1, 1))


def roll(value, shift, axis=None):
    return pltpu.roll(value, shift % value.shape[-1 if axis is None else axis],
                      value.ndim - 1 if axis is None else axis)


def far_first(nx, nz):
    def hops(step):
        dx, dz = step
        return min(dx % 4, -dx % 4) + min(dx // 4, 4 - dx // 4) + min(dz, nz - dz)

    steps = [(dx, dz) for dx in range(nx) for dz in range(nz)]
    return sorted(steps[1:], key=lambda step: -hops(step))


def kernel(
    nx, nz,
    forcing, conduct, diag_add, ice_mask, grounded, out_x, out_r,
    cbf, dbf, ice_v, ground_v, active_v, fs, cn, dn,
    wbuf, hx, hz, hc, pz, pc, ebuf, hbuf, icbuf, gbuf, wcbuf, ecbuf, acc,
    shared_out, shared_in, ar_own, ar_all,
    in_sem, send_sem, recv_sem, corner_sem, share_sem, ar_sem,
):
    g = lax.axis_index("group")
    x = lax.axis_index("gx")
    z = lax.axis_index("gy")

    lane2 = lax.broadcasted_iota(jnp.int32, (SUB, LANES), 1)
    sub2 = lax.broadcasted_iota(jnp.int32, (SUB, LANES), 0)
    lane3 = lax.broadcasted_iota(jnp.int32, (ROWS, SUB, LANES), 2)
    sub3 = lax.broadcasted_iota(jnp.int32, (ROWS, SUB, LANES), 1)
    lane1 = lax.broadcasted_iota(jnp.int32, (1, LANES), 1)

    beside_x = (x > 0).astype(jnp.int32) + (x < nx - 1).astype(jnp.int32)
    beside_z = (z > 0).astype(jnp.int32) + (z < nz - 1).astype(jnp.int32)

    def exists(d):
        dx, dz = STEPS[d]
        conds = []
        if dx < 0:
            conds.append(x > 0)
        if dx > 0:
            conds.append(x < nx - 1)
        if dz < 0:
            conds.append(z > 0)
        if dz > 0:
            conds.append(z < nz - 1)
        return functools.reduce(jnp.logical_and, conds)

    def at(d):
        dx, dz = STEPS[d]
        return (g, x + dx, z + dz)

    barrier = pltpu.get_barrier_semaphore()
    far = sorted({(a * nx // 4, b * nz // 2) for a in range(4) for b in range(2)} - {(0, 0)})
    for dx, dz in far:
        pl.semaphore_signal(
            barrier, inc=1, device_id=(g, (x + dx) % nx, (z + dz) % nz), device_id_type=MESH)
    for d in (4, 5, 6, 7, 0, 1, 2, 3):
        @pl.when(exists(d))
        def _(d=d):
            pl.semaphore_signal(barrier, inc=1, device_id=at(d), device_id_type=MESH)
    pl.semaphore_signal(barrier, inc=1, device_id=(1 - g, x, z), device_id_type=MESH)

    loads = [
        pltpu.make_async_copy(conduct.at[:, pl.ds(0, ROWS)], cbf.at[:, pl.ds(0, ROWS)], in_sem.at[0]),
        pltpu.make_async_copy(ice_mask, ice_v, in_sem.at[1]),
        pltpu.make_async_copy(grounded, ground_v, in_sem.at[2]),
        pltpu.make_async_copy(forcing.at[:, pl.ds(0, LANES)], fs.at[0], in_sem.at[3]),
        pltpu.make_async_copy(forcing.at[:, pl.ds(LANES, LANES)], fs.at[1], in_sem.at[4]),
        pltpu.make_async_copy(diag_add, dbf, in_sem.at[5]),
        pltpu.make_async_copy(conduct.at[:, pl.ds(ROWS, LAYERS - ROWS)], cbf.at[:, pl.ds(ROWS, LAYERS - ROWS)], in_sem.at[6]),
    ]
    for n in (0, 1, 2, 6, 3, 4, 5):
        loads[n].start()

    def zero_rims(d):
        @pl.when(jnp.logical_not(exists(d)))
        def _():
            def body(e, carry):
                if d < 2:
                    for j in range(CHUNKS):
                        hx[e, j, d] = jnp.zeros((2, TILES, SUB, LANES), F32)
                elif d < 4:
                    hz[e, :, d - 2] = jnp.zeros((CHUNKS, SUB, LANES), F32)
                else:
                    hc[e, :, d - 4] = jnp.zeros((CHUNKS, 1, LANES), F32)
                return carry
            lax.fori_loop(0, FIELDS if d < 4 else CORNERED, body, 0)

    for d in range(8):
        zero_rims(d)

    acc[...] = jnp.zeros_like(acc)

    def clear(f, carry):
        for j in range(CHUNKS):
            wbuf[f, j + 1] = jnp.zeros((ROWS, TILES, SUB, LANES), F32)
        return carry

    lax.fori_loop(0, FIELDS + 1, clear, 0)
    wcbuf[0] = jnp.zeros((CHUNKS + 2, 2, SUB, LANES), F32)

    loads[0].wait()
    loads[1].wait()
    loads[2].wait()
    is_ice = jnp.where(g == 0, 1.0, 0.0).astype(F32)
    ice = ice_v[...].astype(F32)
    ground = ground_v[...].astype(F32)
    active_v[...] = ice * (1.0 - (1.0 - is_ice) * ground)

    def pick(ref, j, t):
        return jnp.stack([ref[t, pl.ds(j * ROWS + r, SUB, stride=CHUNKS * ROWS), :] for r in range(ROWS)])

    def couple(j):
        rows = pl.ds(pl.multiple_of(j * ROWS, ROWS), ROWS)
        base = pl.multiple_of(j * SUB * ROWS, SUB * ROWS)
        parts = []
        for t in range(TILES):
            columns = slice(t * LANES, (t + 1) * LANES)
            value = jnp.sqrt(cbf[:, rows, columns].astype(F32)) * active_v[:, columns][None]
            cn[t, pl.ds(base, SUB * ROWS)] = value.reshape(SUB * ROWS, LANES)
        for t in range(TILES):
            parts.append(jnp.stack([cn[t, pl.ds(base + r, SUB, stride=ROWS), :] for r in range(ROWS)]))
        return parts

    def put(ref, j, t, value):
        for r in range(ROWS):
            ref[t, pl.ds(j * ROWS + r, SUB, stride=CHUNKS * ROWS), :] = value[r]

    def copies(e, j, d):
        f = COUPLING if isinstance(e, int) and e == 0 else e
        if d == 0:
            src, dst = wbuf.at[f, j + 1, pl.ds(0, 2)], hx.at[e, j, 1]
        elif d == 1:
            src, dst = wbuf.at[f, j + 1, pl.ds(ROWS - 2, 2)], hx.at[e, j, 0]
        elif d < 4:
            src, dst = pz.at[e, j], hz.at[e, j, 3 - d]
        else:
            src, dst = pc.at[e, j], hc.at[e, j, 7 - d]
        return pltpu.make_async_remote_copy(
            src_ref=src, dst_ref=dst, send_sem=send_sem.at[min(d // 2, 2)],
            recv_sem=recv_sem.at[e % 2, j, d // 2] if d < 4 else corner_sem.at[e % 4, j],
            device_id=at(d), device_id_type=MESH)

    def store_field(f, j, parts):
        for t in range(TILES):
            wbuf[f, j + 1, :, t] = parts[t]

        @pl.when(j == 0)
        def _():
            for t in range(TILES):
                wbuf[f, CHUNKS + 1, :, t] = jnp.where(sub3 < SUB - 1, roll(parts[t], SUB - 1, 1), 0.0)

        @pl.when(j == CHUNKS - 1)
        def _():
            for t in range(TILES):
                wbuf[f, 0, :, t] = jnp.where(sub3 > 0, roll(parts[t], 1, 1), 0.0)

    def store_corners(f, j, corners):
        for p in range(2):
            wcbuf[f, j + 1, p] = corners[p]

        @pl.when(j == 0)
        def _():
            for p in range(2):
                wcbuf[f, CHUNKS + 1, p] = jnp.where(sub2 < SUB - 1, roll(corners[p], SUB - 1, 0), 0.0)

        @pl.when(j == CHUNKS - 1)
        def _():
            for p in range(2):
                wcbuf[f, 0, p] = jnp.where(sub2 > 0, roll(corners[p], 1, 0), 0.0)

    def pack_rims(e, j, parts, raw=None, ahead=True, scale=None):
        none = jnp.zeros((1, SUB, LANES), F32)
        crossed, scaled = [], []
        for t in range(TILES):
            wide = jnp.concatenate([none, parts[t], none], axis=0)
            crossed.append(parts[t] + cross_weight * (wide[0:8] + wide[2:10]))
            scaled.append(far_weight * parts[t])
        sources = (
            (jnp.where(lane3 == LANES - 1, crossed[1], 0.0), 1),
            (jnp.where(lane3 == 0, crossed[0], 0.0), -1),
            (jnp.where(lane3 >= LANES - 2, scaled[1], 0.0), 2),
            (jnp.where(lane3 < 2, scaled[0], 0.0), -2),
        )
        packed = None
        for source, shift in sources:
            for r in range(ROWS):
                moved = roll(source[r], 4 * (r + 1) + shift)
                packed = moved if packed is None else packed + moved
        for base, row, inner in ((0, 0, 1), (4 * (ROWS + 1), ROWS - 1, ROWS - 2)):
            for tile, lane, way in ((1, LANES - 1, 1), (0, 0, -1)):
                straight = parts[tile][row] + far_weight * parts[tile][inner]
                packed = packed + roll(jnp.where(lane2 == lane, straight, 0.0), base + way)
                across = jnp.where(lane2 == lane - way, cross_weight * parts[tile][row], 0.0)
                packed = packed + roll(across, base + 2 * way)
        pz[e, j] = packed
        moved = []

        def place(value, lane, target):
            only = jnp.where(lane2 == lane, value, 0.0)
            moved.append(pltpu.roll(only, (target - lane) % LANES, 1, stride=1, stride_axis=0))

        for q in range(4):
            tile = q % 2
            lane, way = ((0, 1), (LANES - 1, -1))[tile]
            edge, one, two = ((0, 1, 2), (ROWS - 1, ROWS - 2, ROWS - 3))[q // 2]
            field = parts[tile]
            if raw is not None:
                place(field[edge], lane, 8 * q)
            if ahead:
                place(field[one] + far_weight * field[two], lane, 32 + 8 * q)
                place(field[edge] + cross_weight * field[one], lane + way, 32 + 8 * q)
                place(far_weight * field[edge], lane + 2 * way, 32 + 8 * q)
            if scale is not None:
                place(scale[tile][edge], lane, 64 + 8 * q)
        pc[e, j] = jnp.sum(functools.reduce(jnp.add, moved), axis=0, keepdims=True)

    def send_rims(e, j, directions, wanted=None):
        for d in directions:
            @pl.when(exists(d) if wanted is None else jnp.logical_and(exists(d), wanted))
            def _(d=d):
                copies(e, j, d).start()

    ALONG_X, BESIDE = (0, 1), (2, 3, 4, 5, 6, 7)

    def arrive(semaphore, condition, whole):
        @pl.when(condition)
        def _():
            pltpu.make_async_copy(whole, whole, semaphore).wait()

    def await_rims(e, j):
        arrive(recv_sem.at[e % 2, j, 0], beside_x == 2, hx.at[e, j])
        arrive(recv_sem.at[e % 2, j, 0], beside_x == 1, hx.at[e, j, 0])
        arrive(recv_sem.at[e % 2, j, 1], beside_z == 2, hz.at[e, j])
        arrive(recv_sem.at[e % 2, j, 1], beside_z == 1, hz.at[e, j, 0])

    def await_corners(e, j, wanted=None):
        def when(count):
            here = beside_x * beside_z == count
            return here if wanted is None else jnp.logical_and(here, wanted)

        arrive(corner_sem.at[e % 4, j], when(4), hc.at[e, j])
        arrive(corner_sem.at[e % 4, j], when(2), hc.at[e, j, pl.ds(0, 2)])
        arrive(corner_sem.at[e % 4, j], when(1), hc.at[e, j, 0])

    def corner_values(e, j, base):
        values = []
        for q in range(4):
            here = lane2 == base + 8 * (3 - q) + sub2
            picked = jnp.where(here, jnp.broadcast_to(hc[e, j, q], (SUB, LANES)), 0.0)
            values.append(jnp.sum(picked, axis=1, keepdims=True))
        return [at_ends(jnp.broadcast_to(values[2 * p], (SUB, LANES)),
                        jnp.broadcast_to(values[2 * p + 1], (SUB, LANES))) for p in range(2)]

    def at_ends(low, high):
        return jnp.where(lane2 == 0, low, jnp.where(lane2 == LANES - 1, high, 0.0))

    def next_corners(k, j):
        e = k - 1
        alone = corner_values(e, j, 32)
        edge = jnp.where(lane2 % 4 < 2, hz[e, j, 0], hz[e, j, 1])
        corners = []
        for p in range(2):
            near = [hx[e, j, p, 1 - p, t] for t in range(TILES)]
            outer = [hx[e, j, p, p, t] for t in range(TILES)]
            row = p * (ROWS - 1)
            total = at_ends(near[0], near[1]) + cross_weight * at_ends(outer[0], outer[1])
            total = total + far_weight * at_ends(roll(near[0], -1), roll(near[1], 1))
            total = total + cross_weight * at_ends(wbuf[e, j + 1, row, 0], wbuf[e, j + 1, row, 1])
            beyond = edge if p == 0 else roll(edge, -4 * (ROWS + 1))
            total = total + at_ends(beyond, beyond) + alone[p]
            total = total + vertical_weight * (wcbuf[k - 1, j, p] + wcbuf[k - 1, j + 2, p])
            corners.append(ecbuf[j, p] * total - wcbuf[k - 2, j + 1, p])
        return corners

    def spread(f, e, j, corners):
        centre = [wbuf[f, j + 1, :, t] for t in range(TILES)]
        beside, mixed, scaled = [], [], []
        for t in range(TILES):
            wide = jnp.concatenate([hx[e, j, 0, :, t], centre[t], hx[e, j, 1, :, t]], axis=0)
            near = wide[1:9] + wide[3:11]
            far = wide[0:8] + wide[4:12]
            vertical = wbuf[f, j, :, t] + wbuf[f, j + 2, :, t]
            beside.append(near + far_weight * far + vertical_weight * vertical)
            mixed.append(centre[t] + cross_weight * near)
            scaled.append(far_weight * centre[t])
        for source, shift in ((mixed, 1), (scaled, 2)):
            a, b = roll(source[0], shift), roll(source[1], shift)
            beside[0] = beside[0] + jnp.where(lane3 < shift, 0.0, a)
            beside[1] = beside[1] + jnp.where(lane3 < shift, a, b)
            a, b = roll(source[0], -shift), roll(source[1], -shift)
            beside[0] = beside[0] + jnp.where(lane3 >= LANES - shift, b, a)
            beside[1] = beside[1] + jnp.where(lane3 >= LANES - shift, 0.0, b)

        edge = jnp.where(lane2 % 4 < 2, hz[e, j, 0], hz[e, j, 1])
        rows = [roll(edge, -4 * (r + 1)) for r in range(ROWS)]
        corners = corners() if callable(corners) else corners
        rows[0] = rows[0] + cross_weight * corners[0]
        rows[-1] = rows[-1] + cross_weight * corners[1]
        rows = jnp.stack(rows)
        return [beside[0] + jnp.where(lane3 < 2, rows, 0.0),
                beside[1] + jnp.where(lane3 >= LANES - 2, rows, 0.0)]

    def dots(k, j, applied):
        field = [wbuf[k + 1, j + 1, :, t] for t in range(TILES)]
        weighted = [hbuf[j, :, t] * (field[t] - 0.5 * applied[t]) for t in range(TILES)]
        for i in range(ITERS):
            product = [jnp.sum(weighted[t] * wbuf[i + 1, j + 1, :, t], axis=0) for t in range(TILES)]
            acc[k, i] = acc[k, i] + (product[0] + product[1])
        product = [jnp.sum(hbuf[j, :, t] * field[t] * wbuf[1, j + 1, :, t], axis=0) for t in range(TILES)]
        acc[k, ITERS] = acc[k, ITERS] + (product[0] + product[1])

    def first(j):
        parts = couple(j)
        store_field(COUPLING, j, parts)
        pack_rims(0, j, parts, raw=True, ahead=False)

    def first_and_send(j, carry):
        first(j)
        send_rims(0, j, BESIDE + ALONG_X)
        return carry

    first(jnp.int32(0))
    pl.semaphore_wait(barrier, 1 + len(far) + beside_x + beside_z + beside_x * beside_z)
    send_rims(0, jnp.int32(0), BESIDE[2:] + BESIDE[:2] + ALONG_X)
    loads[6].wait()
    lax.fori_loop(1, CHUNKS, first_and_send, 0)

    loads[3].wait()
    loads[4].wait()
    edge = pl.ds(pl.multiple_of(g * ((LAYERS - 1) * ROWS), ROWS), ROWS)
    for t in range(TILES):
        mean = jnp.sum(fs[t].reshape(LAYERS, ROWS, LANES), axis=0) * (1.0 / LAYERS)
        value = active_v[:, t * LANES:(t + 1) * LANES] * mean
        shared_out[t] = value * cn[t, edge]
    share = pltpu.make_async_remote_copy(
        src_ref=shared_out, dst_ref=shared_in, send_sem=share_sem.at[0], recv_sem=share_sem.at[1],
        device_id=(1 - g, x, z), device_id_type=MESH)
    share.start()
    loads[5].wait()

    def widen(i, carry):
        part = pl.ds(pl.multiple_of(i * SUB * ROWS, SUB * ROWS), SUB * ROWS)
        for t in range(TILES):
            dn[t, part] = dbf[part, t * LANES:(t + 1) * LANES].astype(F32)
        return carry

    lax.fori_loop(0, CHUNKS, widen, 0)
    for t in range(TILES):
        columns = slice(t * LANES, (t + 1) * LANES)
        friction = is_ice * friction_gain * (ground_v[:, columns].astype(F32) * ice_v[:, columns].astype(F32))
        dn[t, 0:ROWS] = dn[t, 0:ROWS] + friction

    def turn(source, target):
        def body(j, carry):
            for t in range(TILES):
                target[j, :, t] = pick(source, j, t)
            return carry

        lax.fori_loop(0, CHUNKS, body, 0)

    turn(dn, gbuf)
    share.wait()
    for t in range(TILES):
        fs[t, edge] = fs[t, edge] + shared_in[t]
    turn(fs, hbuf)

    def second(j, late):
        await_rims(0, j)
        await_corners(0, j)
        spreads = spread(COUPLING, 0, j, corner_values(0, j, 0))
        couplings = [wbuf[COUPLING, j + 1, :, t] for t in range(TILES)]
        diagonals = [gbuf[j, :, t] + couplings[t] * spreads[t] for t in range(TILES)]
        ratios = [couplings[t] / diagonals[t] for t in range(TILES)]
        parts = [ratios[t] * hbuf[j, :, t] for t in range(TILES)]
        store_field(1, j, parts)
        scale = [2.0 * ratios[t] * couplings[t] for t in range(TILES)]
        pack_rims(1, j, parts, raw=True, scale=scale)
        for t in range(TILES):
            c = couplings[t]
            inverse_c = jnp.where(c > 0.0, 1.0 / jnp.where(c > 0.0, c, 1.0), 0.0)
            back = diagonals[t] * inverse_c
            ebuf[j, :, t] = scale[t]
            icbuf[j, :, t] = inverse_c
            gbuf[j, :, t] = back
            hbuf[j, :, t] = back * inverse_c
        send_rims(1, j, BESIDE[2:] + BESIDE[:2] + ALONG_X)

    def chunks(step):
        def body(j, carry):
            step(j, False)
            return carry

        step(jnp.int32(0), True)
        lax.fori_loop(1, CHUNKS, body, 0)

    chunks(second)

    def stage(k, place):
        def step(j, late):
            if place == "first":
                await_rims(k, j)
                await_corners(k, j)
                corners = corner_values(k, j, 0)
                scales = corner_values(k, j, 64)
                for p in range(2):
                    ecbuf[j, p] = scales[p]
            else:
                if not late:
                    await_rims(k, j)
                await_corners(k - 1, j, None if place == "last" else k > 2)
                corners = next_corners(k, j)
                if late:
                    store_corners(k, j, corners)
                    await_rims(k, j)
            spreads = spread(k, k, j, corners)
            applied = [ebuf[j, :, t] * spreads[t] for t in range(TILES)]
            parts = [applied[t] - wbuf[k - 1, j + 1, :, t] for t in range(TILES)]
            if place == "last":
                for t in range(TILES):
                    wbuf[k + 1, j + 1, :, t] = parts[t]
                dots(k - 1, j, applied)
                return
            store_field(k + 1, j, parts)
            if late:
                send_rims(k + 1, j, ALONG_X)
            pack_rims(k + 1, j, parts)
            if place == "first" or not late:
                store_corners(k, j, corners)
            if not late:
                dots(k - 1, j, applied)
                send_rims(k + 1, j, ALONG_X)
            send_rims(k + 1, j, BESIDE[:2])
            send_rims(k + 1, j, BESIDE[2:], None if place == "first" else k < ITERS - 1)
            if late:
                dots(k - 1, j, applied)

        chunks(step)

    def middle(k, carry):
        stage(k, "middle")
        return carry

    stage(1, "first")
    lax.fori_loop(2, ITERS, middle, 0)
    stage(ITERS, "last")

    gram = jnp.zeros((SUB, LANES), F32)
    for k in range(ITERS):
        column = jnp.sum(jnp.sum(acc[k], axis=1), axis=1, keepdims=True)
        wanted = (lane2 == SUB * sub2 + k) & ((sub2 <= k) | (sub2 == ITERS))
        gram = gram + jnp.where(wanted, column, 0.0)
    row = jnp.sum(gram, axis=0, keepdims=True)
    ar_own[...] = row
    mine = x * nz + z
    for dx, dz in far_first(nx, nz):
        to_x, to_z = (x + dx) % nx, (z + dz) % nz
        pltpu.make_async_remote_copy(
            src_ref=ar_own, dst_ref=ar_all.at[mine], send_sem=ar_sem.at[0], recv_sem=ar_sem.at[1],
            device_id=(g, to_x, to_z), device_id_type=MESH).start()
    ar_all[mine] = row
    rest = ar_all.at[pl.ds(0, nx * nz - 1)]
    pltpu.make_async_copy(rest, rest, ar_sem.at[1]).wait()
    total = ar_all[...].reshape(nx, nz, 1, LANES)
    total = jnp.sum(jnp.sum(total, axis=0), axis=0)

    total = jnp.broadcast_to(total, (SUB, LANES))

    def entry(i, k):
        lane = SUB * i + k
        return jnp.broadcast_to(total[:, lane:lane + 1], (SUB, LANES))

    system = {(i, k): entry(i, k) for k in range(ITERS) for i in range(k + 1)}
    right = [entry(ITERS, k) for k in range(ITERS)]
    inverse = []
    for p in range(ITERS):
        inverse.append(1.0 / system[p, p])
        for i in range(p + 1, ITERS):
            factor = system[p, i] * inverse[p]
            for k in range(i, ITERS):
                system[i, k] = system[i, k] - factor * system[p, k]
            right[i] = right[i] - factor * right[p]
    a = [None] * ITERS
    for p in reversed(range(ITERS)):
        value = right[p]
        for k in range(p + 1, ITERS):
            value = value - system[p, k] * a[k]
        a[p] = value * inverse[p]
    b = [None] * FIELDS
    b[0] = 1.0 - a[0] + 0.5 * a[1]
    for k in range(1, ITERS - 1):
        b[k] = 0.5 * (a[k - 1] + a[k + 1]) - a[k]
    b[ITERS - 1] = 0.5 * a[ITERS - 2] - a[ITERS - 1]
    b[ITERS] = 0.5 * a[ITERS - 1]
    def combine(j, carry):
        for t in range(TILES):
            fields = [wbuf[k + 1, j + 1, :, t] for k in range(FIELDS)]
            up = a[0][None] * fields[0]
            down = b[0][None] * fields[0]
            for k in range(1, ITERS):
                up = up + a[k][None] * fields[k]
                down = down + b[k][None] * fields[k]
            down = down + b[ITERS][None] * fields[ITERS]
            put(out_x, j, t, icbuf[j, :, t] * up)
            put(out_r, j, t, gbuf[j, :, t] * down)
        return carry

    lax.fori_loop(0, CHUNKS, combine, 0)
    def left(kind, condition, whole):
        @pl.when(condition)
        def _():
            pltpu.make_async_copy(whole, whole, send_sem.at[kind]).wait()

    both = beside_x * beside_z
    left(0, beside_x == 2, hx)
    left(0, beside_x == 1, hx.at[:, :, 0])
    left(1, beside_z == 2, hz)
    left(1, beside_z == 1, hz.at[:, :, 0])
    left(2, both == 4, hc)
    left(2, both == 2, hc.at[:, :, pl.ds(0, 2)])
    left(2, both == 1, hc.at[:, :, 0])
    pltpu.make_async_copy(rest, rest, ar_sem.at[0]).wait()


def on_device(nx, nz, forcing, conduct, diag_add, ice_mask, grounded):
    field = (CHUNKS, ROWS, TILES, SUB, LANES)
    native = (TILES, LAYERS * ROWS, LANES)
    wide = TILES * LANES
    hbm_space = pl.BlockSpec(memory_space=pltpu.HBM)
    vmem_space = pl.BlockSpec(memory_space=pltpu.VMEM)
    out = jax.ShapeDtypeStruct(native, F32)
    vmem = pltpu.VMEM
    flat = lambda array: array.reshape(LAYERS * ROWS, wide)
    outs = pl.pallas_call(
        functools.partial(kernel, nx, nz),
        out_shape=(out, out),
        in_specs=[hbm_space] * 5,
        out_specs=(vmem_space, vmem_space),
        scratch_shapes=[
            vmem((SUB, CHUNKS * ROWS, wide), jnp.bfloat16),
            vmem((LAYERS * ROWS, wide), jnp.bfloat16),
            vmem((ROWS, wide), jnp.int32),
            vmem((ROWS, wide), jnp.int32),
            vmem((ROWS, wide), F32),
            vmem(native, F32),
            vmem(native, F32),
            vmem(native, F32),
            vmem((COUPLING + 1, CHUNKS + 2, ROWS, TILES, SUB, LANES), F32),
            vmem((FIELDS, CHUNKS, 2, 2, TILES, SUB, LANES), F32),
            vmem((FIELDS, CHUNKS, 2, SUB, LANES), F32),
            vmem((CORNERED, CHUNKS, 4, 1, LANES), F32),
            vmem((FIELDS, CHUNKS, SUB, LANES), F32),
            vmem((FIELDS, CHUNKS, 1, LANES), F32),
            vmem(field, F32),
            vmem(field, F32),
            vmem(field, F32),
            vmem(field, F32),
            vmem((FIELDS, CHUNKS + 2, 2, SUB, LANES), F32),
            vmem((CHUNKS, 2, SUB, LANES), F32),
            vmem((SUB, SUB, SUB, LANES), F32),
            vmem((TILES, ROWS, LANES), F32),
            vmem((TILES, ROWS, LANES), F32),
            vmem((1, LANES), F32),
            vmem((nx * nz, 1, LANES), F32),
            pltpu.SemaphoreType.DMA((7,)),
            pltpu.SemaphoreType.DMA((3,)),
            pltpu.SemaphoreType.DMA((2, CHUNKS, 2)),
            pltpu.SemaphoreType.DMA((4, CHUNKS)),
            pltpu.SemaphoreType.DMA((2,)),
            pltpu.SemaphoreType.DMA((2,)),
        ],
        compiler_params=pltpu.CompilerParams(collective_id=0, has_side_effects=True, vmem_limit_bytes=40 * 1024 * 1024),
        name="coupled_solve",
    )(*[pltpu.with_memory_space_constraint(v, pltpu.HBM)
        for v in (flat(forcing), conduct.reshape(SUB, CHUNKS * ROWS, wide), flat(diag_add), ice_mask, grounded)])
    return tuple(
        v.reshape(TILES, LAYERS, ROWS, LANES).transpose(1, 2, 0, 3).reshape(1, LAYERS, ROWS, wide)
        for v in outs)


def solution(mesh):
    block = P("group", None, "gx", "gy")
    columns = P("gx", "gy")
    return jax.shard_map(
        functools.partial(on_device, mesh.shape["gx"], mesh.shape["gy"]),
        mesh=mesh,
        in_specs=(block, block, block, columns, columns),
        out_specs=(block, block),
        check_vma=False,
    )
```

```python
import functools

import jax
import jax.numpy as jnp
from jax import lax
from jax.experimental import pallas as pl
from jax.experimental.pallas import tpu as pltpu
from jax.sharding import PartitionSpec as P

ITERS = 6
FIELDS = ITERS + 1
CORNERED = FIELDS - 1
COUPLING = FIELDS + 1
LAYERS = 80
ROWS = 8
SUB = 8
LANES = 128
TILES = 2
CHUNKS = LAYERS // SUB
HALF = CHUNKS // 2
MESH = pl.DeviceIdType.MESH
F32 = jnp.float32

far_weight = 0.25
cross_weight = 0.5
vertical_weight = 4.0
friction_gain = 8.0

STEPS = ((-1, 0), (1, 0), (0, -1), (0, 1), (-1, -1), (-1, 1), (1, -1), (1, 1))


def roll(value, shift, axis=None):
    return pltpu.roll(value, shift % value.shape[-1 if axis is None else axis],
                      value.ndim - 1 if axis is None else axis)


def far_first(nx, nz):
    def hops(step):
        dx, dz = step
        return min(dx % 4, -dx % 4) + min(dx // 4, 4 - dx // 4) + min(dz, nz - dz)

    steps = [(dx, dz) for dx in range(nx) for dz in range(nz)]
    return sorted(steps[1:], key=lambda step: -hops(step))


def kernel(
    nx, nz,
    forcing, conduct, diag_add, ice_mask, grounded, out_x, out_r,
    cbf, dbf, ice_v, ground_v, active_v, fs, cn, dn,
    wbuf, hx, hz, hc, pz, pc, ebuf, hbuf, icbuf, gbuf, wcbuf, ecbuf, abuf, acc,
    shared_out, shared_in, ar_own, ar_all,
    in_sem, send_sem, recv_sem, corner_sem, half_sem, share_sem, ar_sem, far_sem,
):
    g = lax.axis_index("group")
    x = lax.axis_index("gx")
    z = lax.axis_index("gy")

    lane2 = lax.broadcasted_iota(jnp.int32, (SUB, LANES), 1)
    sub2 = lax.broadcasted_iota(jnp.int32, (SUB, LANES), 0)
    lane3 = lax.broadcasted_iota(jnp.int32, (ROWS, SUB, LANES), 2)
    sub3 = lax.broadcasted_iota(jnp.int32, (ROWS, SUB, LANES), 1)
    lane1 = lax.broadcasted_iota(jnp.int32, (1, LANES), 1)

    beside_x = (x > 0).astype(jnp.int32) + (x < nx - 1).astype(jnp.int32)
    beside_z = (z > 0).astype(jnp.int32) + (z < nz - 1).astype(jnp.int32)

    def exists(d):
        dx, dz = STEPS[d]
        conds = []
        if dx < 0:
            conds.append(x > 0)
        if dx > 0:
            conds.append(x < nx - 1)
        if dz < 0:
            conds.append(z > 0)
        if dz > 0:
            conds.append(z < nz - 1)
        return functools.reduce(jnp.logical_and, conds)

    def at(d):
        dx, dz = STEPS[d]
        return (g, x + dx, z + dz)

    barrier = pltpu.get_barrier_semaphore()
    pl.semaphore_signal(barrier, inc=1, device_id=(g, (x + nx // 2) % nx, z), device_id_type=MESH)
    for d in (4, 5, 6, 7, 0, 1, 2, 3):
        @pl.when(exists(d))
        def _(d=d):
            pl.semaphore_signal(barrier, inc=1, device_id=at(d), device_id_type=MESH)
    pl.semaphore_signal(barrier, inc=1, device_id=(1 - g, x, z), device_id_type=MESH)

    loads = [
        pltpu.make_async_copy(conduct.at[:, pl.ds(0, ROWS)], cbf.at[:, pl.ds(0, ROWS)], in_sem.at[0]),
        pltpu.make_async_copy(ice_mask, ice_v, in_sem.at[1]),
        pltpu.make_async_copy(grounded, ground_v, in_sem.at[2]),
        pltpu.make_async_copy(forcing.at[:, pl.ds(0, LANES)], fs.at[0], in_sem.at[3]),
        pltpu.make_async_copy(forcing.at[:, pl.ds(LANES, LANES)], fs.at[1], in_sem.at[4]),
        pltpu.make_async_copy(diag_add, dbf, in_sem.at[5]),
        pltpu.make_async_copy(conduct.at[:, pl.ds(ROWS, LAYERS - ROWS)], cbf.at[:, pl.ds(ROWS, LAYERS - ROWS)], in_sem.at[6]),
    ]
    for n in (0, 1, 2, 6, 3, 4, 5):
        loads[n].start()

    def zero_rims(d):
        @pl.when(jnp.logical_not(exists(d)))
        def _():
            def body(e, carry):
                if d < 2:
                    for j in range(CHUNKS):
                        hx[e, j, d] = jnp.zeros((2, TILES, SUB, LANES), F32)
                elif d < 4:
                    hz[e, :, d - 2] = jnp.zeros((CHUNKS, SUB, LANES), F32)
                else:
                    hc[e, :, d - 4] = jnp.zeros((CHUNKS, 1, LANES), F32)
                return carry
            lax.fori_loop(0, FIELDS if d < 4 else CORNERED, body, 0)

    for d in range(8):
        zero_rims(d)

    acc[...] = jnp.zeros_like(acc)

    def clear(f, carry):
        for j in range(CHUNKS):
            wbuf[f, j + 1] = jnp.zeros((ROWS, TILES, SUB, LANES), F32)
        return carry

    lax.fori_loop(0, FIELDS + 1, clear, 0)
    wcbuf[0] = jnp.zeros((CHUNKS + 2, 2, SUB, LANES), F32)

    loads[0].wait()
    loads[1].wait()
    loads[2].wait()
    is_ice = jnp.where(g == 0, 1.0, 0.0).astype(F32)
    ice = ice_v[...].astype(F32)
    ground = ground_v[...].astype(F32)
    active_v[...] = ice * (1.0 - (1.0 - is_ice) * ground)

    def pick(ref, j, t):
        return jnp.stack([ref[t, pl.ds(j * ROWS + r, SUB, stride=CHUNKS * ROWS), :] for r in range(ROWS)])

    def couple(j):
        rows = pl.ds(pl.multiple_of(j * ROWS, ROWS), ROWS)
        base = pl.multiple_of(j * SUB * ROWS, SUB * ROWS)
        parts = []
        for t in range(TILES):
            columns = slice(t * LANES, (t + 1) * LANES)
            value = jnp.sqrt(cbf[:, rows, columns].astype(F32)) * active_v[:, columns][None]
            cn[t, pl.ds(base, SUB * ROWS)] = value.reshape(SUB * ROWS, LANES)
        for t in range(TILES):
            parts.append(jnp.stack([cn[t, pl.ds(base + r, SUB, stride=ROWS), :] for r in range(ROWS)]))
        return parts

    def put(ref, j, t, value):
        for r in range(ROWS):
            ref[t, pl.ds(j * ROWS + r, SUB, stride=CHUNKS * ROWS), :] = value[r]

    def copies(e, j, d):
        f = COUPLING if isinstance(e, int) and e == 0 else e
        if d == 0:
            src, dst = wbuf.at[f, j + 1, pl.ds(0, 2)], hx.at[e, j, 1]
        elif d == 1:
            src, dst = wbuf.at[f, j + 1, pl.ds(ROWS - 2, 2)], hx.at[e, j, 0]
        elif d < 4:
            src, dst = pz.at[e, j], hz.at[e, j, 3 - d]
        else:
            src, dst = pc.at[e, j], hc.at[e, j, 7 - d]
        return pltpu.make_async_remote_copy(
            src_ref=src, dst_ref=dst, send_sem=send_sem.at[min(d // 2, 2)],
            recv_sem=recv_sem.at[e % 2, j, d // 2] if d < 4 else corner_sem.at[e % 2, j],
            device_id=at(d), device_id_type=MESH)

    def store_field(f, j, parts):
        for t in range(TILES):
            wbuf[f, j + 1, :, t] = parts[t]

        @pl.when(j == 0)
        def _():
            for t in range(TILES):
                wbuf[f, CHUNKS + 1, :, t] = jnp.where(sub3 < SUB - 1, roll(parts[t], SUB - 1, 1), 0.0)

        @pl.when(j == CHUNKS - 1)
        def _():
            for t in range(TILES):
                wbuf[f, 0, :, t] = jnp.where(sub3 > 0, roll(parts[t], 1, 1), 0.0)

    def store_corners(f, j, corners):
        for p in range(2):
            wcbuf[f, j + 1, p] = corners[p]

        @pl.when(j == 0)
        def _():
            for p in range(2):
                wcbuf[f, CHUNKS + 1, p] = jnp.where(sub2 < SUB - 1, roll(corners[p], SUB - 1, 0), 0.0)

        @pl.when(j == CHUNKS - 1)
        def _():
            for p in range(2):
                wcbuf[f, 0, p] = jnp.where(sub2 > 0, roll(corners[p], 1, 0), 0.0)

    def pack_rims(e, j, parts, raw=None, ahead=True, scale=None):
        none = jnp.zeros((1, SUB, LANES), F32)
        crossed, scaled = [], []
        for t in range(TILES):
            wide = jnp.concatenate([none, parts[t], none], axis=0)
            crossed.append(parts[t] + cross_weight * (wide[0:8] + wide[2:10]))
            scaled.append(far_weight * parts[t])
        sources = (
            (jnp.where(lane3 == LANES - 1, crossed[1], 0.0), 1),
            (jnp.where(lane3 == 0, crossed[0], 0.0), -1),
            (jnp.where(lane3 >= LANES - 2, scaled[1], 0.0), 2),
            (jnp.where(lane3 < 2, scaled[0], 0.0), -2),
        )
        packed = None
        for source, shift in sources:
            for r in range(ROWS):
                moved = roll(source[r], 4 * (r + 1) + shift)
                packed = moved if packed is None else packed + moved
        for base, row, inner in ((0, 0, 1), (4 * (ROWS + 1), ROWS - 1, ROWS - 2)):
            for tile, lane, way in ((1, LANES - 1, 1), (0, 0, -1)):
                straight = parts[tile][row] + far_weight * parts[tile][inner]
                packed = packed + roll(jnp.where(lane2 == lane, straight, 0.0), base + way)
                across = jnp.where(lane2 == lane - way, cross_weight * parts[tile][row], 0.0)
                packed = packed + roll(across, base + 2 * way)
        pz[e, j] = packed
        moved = []

        def place(value, lane, target):
            only = jnp.where(lane2 == lane, value, 0.0)
            moved.append(pltpu.roll(only, (target - lane) % LANES, 1, stride=1, stride_axis=0))

        for q in range(4):
            tile = q % 2
            lane, way = ((0, 1), (LANES - 1, -1))[tile]
            edge, one, two = ((0, 1, 2), (ROWS - 1, ROWS - 2, ROWS - 3))[q // 2]
            field = parts[tile]
            if raw is not None:
                place(field[edge], lane, 8 * q)
            if ahead:
                place(field[one] + far_weight * field[two], lane, 32 + 8 * q)
                place(field[edge] + cross_weight * field[one], lane + way, 32 + 8 * q)
                place(far_weight * field[edge], lane + 2 * way, 32 + 8 * q)
            if scale is not None:
                place(scale[tile][edge], lane, 64 + 8 * q)
        pc[e, j] = jnp.sum(functools.reduce(jnp.add, moved), axis=0, keepdims=True)

    def send_rims(e, j, directions, wanted=None):
        for d in directions:
            @pl.when(exists(d) if wanted is None else jnp.logical_and(exists(d), wanted))
            def _(d=d):
                copies(e, j, d).start()

    ALONG_X, BESIDE = (0, 1), (2, 3, 4, 5, 6, 7)

    def arrive(semaphore, condition, whole):
        @pl.when(condition)
        def _():
            pltpu.make_async_copy(whole, whole, semaphore).wait()

    def await_rims(e, j):
        arrive(recv_sem.at[e % 2, j, 0], beside_x == 2, hx.at[e, j])
        arrive(recv_sem.at[e % 2, j, 0], beside_x == 1, hx.at[e, j, 0])
        arrive(recv_sem.at[e % 2, j, 1], beside_z == 2, hz.at[e, j])
        arrive(recv_sem.at[e % 2, j, 1], beside_z == 1, hz.at[e, j, 0])

    def await_corners(e, j):
        both = beside_x * beside_z
        arrive(corner_sem.at[e % 2, j], both == 4, hc.at[e, j])
        arrive(corner_sem.at[e % 2, j], both == 2, hc.at[e, j, pl.ds(0, 2)])
        arrive(corner_sem.at[e % 2, j], both == 1, hc.at[e, j, 0])

    def await_half(e, half, wanted):
        both, part = beside_x * beside_z, pl.ds(half * HALF, HALF)
        semaphore = half_sem.at[e % 4, half]
        arrive(semaphore, jnp.logical_and(both == 4, wanted), hc.at[e, part])
        arrive(semaphore, jnp.logical_and(both == 2, wanted), hc.at[e, part, pl.ds(0, 2)])
        arrive(semaphore, jnp.logical_and(both == 1, wanted), hc.at[e, part, 0])

    def send_half(e, half, wanted):
        part = pl.ds(half * HALF, HALF)
        for d in range(4, 8):
            @pl.when(jnp.logical_and(exists(d), wanted))
            def _(d=d):
                pltpu.make_async_remote_copy(
                    src_ref=pc.at[e, part], dst_ref=hc.at[e, part, 7 - d],
                    send_sem=send_sem.at[2], recv_sem=half_sem.at[e % 4, half],
                    device_id=at(d), device_id_type=MESH).start()

    def corner_values(e, j, base):
        values = []
        for q in range(4):
            here = lane2 == base + 8 * (3 - q) + sub2
            picked = jnp.where(here, jnp.broadcast_to(hc[e, j, q], (SUB, LANES)), 0.0)
            values.append(jnp.sum(picked, axis=1, keepdims=True))
        return [at_ends(jnp.broadcast_to(values[2 * p], (SUB, LANES)),
                        jnp.broadcast_to(values[2 * p + 1], (SUB, LANES))) for p in range(2)]

    def at_ends(low, high):
        return jnp.where(lane2 == 0, low, jnp.where(lane2 == LANES - 1, high, 0.0))

    def next_corners(k, j):
        e = k - 1
        alone = corner_values(e, j, 32)
        edge = jnp.where(lane2 % 4 < 2, hz[e, j, 0], hz[e, j, 1])
        corners = []
        for p in range(2):
            near = [hx[e, j, p, 1 - p, t] for t in range(TILES)]
            outer = [hx[e, j, p, p, t] for t in range(TILES)]
            row = p * (ROWS - 1)
            total = at_ends(near[0], near[1]) + cross_weight * at_ends(outer[0], outer[1])
            total = total + far_weight * at_ends(roll(near[0], -1), roll(near[1], 1))
            total = total + cross_weight * at_ends(wbuf[e, j + 1, row, 0], wbuf[e, j + 1, row, 1])
            beyond = edge if p == 0 else roll(edge, -4 * (ROWS + 1))
            total = total + at_ends(beyond, beyond) + alone[p]
            total = total + vertical_weight * (wcbuf[k - 1, j, p] + wcbuf[k - 1, j + 2, p])
            corners.append(ecbuf[j, p] * total - wcbuf[k - 2, j + 1, p])
        return corners

    def spread(f, e, j, corners):
        centre = [wbuf[f, j + 1, :, t] for t in range(TILES)]
        beside, mixed, scaled = [], [], []
        for t in range(TILES):
            wide = jnp.concatenate([hx[e, j, 0, :, t], centre[t], hx[e, j, 1, :, t]], axis=0)
            near = wide[1:9] + wide[3:11]
            far = wide[0:8] + wide[4:12]
            vertical = wbuf[f, j, :, t] + wbuf[f, j + 2, :, t]
            beside.append(near + far_weight * far + vertical_weight * vertical)
            mixed.append(centre[t] + cross_weight * near)
            scaled.append(far_weight * centre[t])
        for source, shift in ((mixed, 1), (scaled, 2)):
            a, b = roll(source[0], shift), roll(source[1], shift)
            beside[0] = beside[0] + jnp.where(lane3 < shift, 0.0, a)
            beside[1] = beside[1] + jnp.where(lane3 < shift, a, b)
            a, b = roll(source[0], -shift), roll(source[1], -shift)
            beside[0] = beside[0] + jnp.where(lane3 >= LANES - shift, b, a)
            beside[1] = beside[1] + jnp.where(lane3 >= LANES - shift, 0.0, b)

        edge = jnp.where(lane2 % 4 < 2, hz[e, j, 0], hz[e, j, 1])
        rows = [roll(edge, -4 * (r + 1)) for r in range(ROWS)]
        corners = corners() if callable(corners) else corners
        rows[0] = rows[0] + cross_weight * corners[0]
        rows[-1] = rows[-1] + cross_weight * corners[1]
        rows = jnp.stack(rows)
        return [beside[0] + jnp.where(lane3 < 2, rows, 0.0),
                beside[1] + jnp.where(lane3 >= LANES - 2, rows, 0.0)]

    def dots(k, j, applied):
        field = [wbuf[k + 1, j + 1, :, t] for t in range(TILES)]
        weighted = [hbuf[j, :, t] * (field[t] - 0.5 * applied[t]) for t in range(TILES)]
        for i in range(ITERS):
            product = [jnp.sum(weighted[t] * wbuf[i + 1, j + 1, :, t], axis=0) for t in range(TILES)]
            acc[k, i] = acc[k, i] + (product[0] + product[1])
        product = [jnp.sum(hbuf[j, :, t] * field[t] * wbuf[1, j + 1, :, t], axis=0) for t in range(TILES)]
        acc[k, ITERS] = acc[k, ITERS] + (product[0] + product[1])

    def first(j):
        parts = couple(j)
        store_field(COUPLING, j, parts)
        pack_rims(0, j, parts, raw=True, ahead=False)

    def first_and_send(j, carry):
        first(j)
        send_rims(0, j, BESIDE + ALONG_X)
        return carry

    first(jnp.int32(0))
    pl.semaphore_wait(barrier, 2 + beside_x + beside_z + beside_x * beside_z)
    send_rims(0, jnp.int32(0), BESIDE[2:] + BESIDE[:2] + ALONG_X)
    loads[6].wait()
    lax.fori_loop(1, CHUNKS, first_and_send, 0)

    loads[3].wait()
    loads[4].wait()
    edge = pl.ds(pl.multiple_of(g * ((LAYERS - 1) * ROWS), ROWS), ROWS)
    for t in range(TILES):
        mean = jnp.sum(fs[t].reshape(LAYERS, ROWS, LANES), axis=0) * (1.0 / LAYERS)
        value = active_v[:, t * LANES:(t + 1) * LANES] * mean
        shared_out[t] = value * cn[t, edge]
    share = pltpu.make_async_remote_copy(
        src_ref=shared_out, dst_ref=shared_in, send_sem=share_sem.at[0], recv_sem=share_sem.at[1],
        device_id=(1 - g, x, z), device_id_type=MESH)
    share.start()
    loads[5].wait()

    def widen(i, carry):
        part = pl.ds(pl.multiple_of(i * SUB * ROWS, SUB * ROWS), SUB * ROWS)
        for t in range(TILES):
            dn[t, part] = dbf[part, t * LANES:(t + 1) * LANES].astype(F32)
        return carry

    lax.fori_loop(0, CHUNKS, widen, 0)
    for t in range(TILES):
        columns = slice(t * LANES, (t + 1) * LANES)
        friction = is_ice * friction_gain * (ground_v[:, columns].astype(F32) * ice_v[:, columns].astype(F32))
        dn[t, 0:ROWS] = dn[t, 0:ROWS] + friction

    def turn(source, target):
        def body(j, carry):
            for t in range(TILES):
                target[j, :, t] = pick(source, j, t)
            return carry

        lax.fori_loop(0, CHUNKS, body, 0)

    turn(dn, gbuf)
    share.wait()
    for t in range(TILES):
        fs[t, edge] = fs[t, edge] + shared_in[t]
    turn(fs, hbuf)

    def second(j, late):
        await_rims(0, j)
        await_corners(0, j)
        spreads = spread(COUPLING, 0, j, corner_values(0, j, 0))
        couplings = [wbuf[COUPLING, j + 1, :, t] for t in range(TILES)]
        diagonals = [gbuf[j, :, t] + couplings[t] * spreads[t] for t in range(TILES)]
        ratios = [couplings[t] / diagonals[t] for t in range(TILES)]
        parts = [ratios[t] * hbuf[j, :, t] for t in range(TILES)]
        store_field(1, j, parts)
        scale = [2.0 * ratios[t] * couplings[t] for t in range(TILES)]
        pack_rims(1, j, parts, raw=True, scale=scale)
        for t in range(TILES):
            c = couplings[t]
            inverse_c = jnp.where(c > 0.0, 1.0 / jnp.where(c > 0.0, c, 1.0), 0.0)
            back = diagonals[t] * inverse_c
            ebuf[j, :, t] = scale[t]
            icbuf[j, :, t] = inverse_c
            gbuf[j, :, t] = back
            hbuf[j, :, t] = back * inverse_c
        send_rims(1, j, BESIDE[2:] + BESIDE[:2] + ALONG_X)

    def chunks(step):
        def body(j, carry):
            step(j, False)
            return carry

        step(jnp.int32(0), True)
        lax.fori_loop(1, CHUNKS, body, 0)

    chunks(second)

    def stage(k, place):
        def step(j, late):
            if not late:
                await_rims(k, j)
            if place == "first":
                await_corners(k, j)
                corners = corner_values(k, j, 0)
                scales = corner_values(k, j, 64)
                for p in range(2):
                    ecbuf[j, p] = scales[p]
            else:
                ahead = jnp.bool_(True) if place == "last" else k > 2
                if late:
                    await_half(k - 1, 0, ahead)
                else:
                    await_half(k - 1, 1, jnp.logical_and(ahead, j == HALF))
                corners = next_corners(k, j)
            if late:
                store_corners(k, j, corners)
                await_rims(k, j)
            spreads = spread(k, k, j, corners)
            applied = [ebuf[j, :, t] * spreads[t] for t in range(TILES)]
            parts = [applied[t] - wbuf[k - 1, j + 1, :, t] for t in range(TILES)]
            if place == "last":
                for t in range(TILES):
                    wbuf[k + 1, j + 1, :, t] = parts[t]
                dots(k - 1, j, applied)
                return
            if not late:
                rest(j - 1)
            for t in range(TILES):
                abuf[:, t] = applied[t]
            store_field(k + 1, j, parts)
            send_rims(k + 1, j, ALONG_X)
            if not late:
                store_corners(k, j, corners)
                send_rims(k + 1, j - 1, BESIDE[:2])
                send_half(k + 1, 0, jnp.logical_and(j == HALF, sends_corners))

        def rest(j):
            pack_rims(k + 1, j, [wbuf[k + 1, j + 1, :, t] for t in range(TILES)])
            dots(k - 1, j, [abuf[:, t] for t in range(TILES)])

        sends_corners = jnp.bool_(True) if place == "first" else k < ITERS - 1
        chunks(step)
        if place != "last":
            final = jnp.int32(CHUNKS - 1)
            rest(final)
            send_rims(k + 1, final, BESIDE[:2])
            send_half(k + 1, 1, sends_corners)

    def middle(k, carry):
        stage(k, "middle")
        return carry

    stage(1, "first")
    lax.fori_loop(2, ITERS, middle, 0)
    far = {(0, nz // 2)} | {(a * nx // 4, 0) for a in range(4)} | {(nx // 2, nz // 2)}
    far = sorted(far - {(0, 0)})
    for dx, dz in far:
        pl.semaphore_signal(
            far_sem, inc=1, device_id=(g, (x + dx) % nx, (z + dz) % nz), device_id_type=MESH)
    stage(ITERS, "last")
    pl.semaphore_wait(far_sem, len(far))

    gram = jnp.zeros((SUB, LANES), F32)
    for k in range(ITERS):
        column = jnp.sum(jnp.sum(acc[k], axis=1), axis=1, keepdims=True)
        wanted = (lane2 == SUB * sub2 + k) & ((sub2 <= k) | (sub2 == ITERS))
        gram = gram + jnp.where(wanted, column, 0.0)
    row = jnp.sum(gram, axis=0, keepdims=True)
    ar_own[...] = row
    mine = x * nz + z
    for dx, dz in far_first(nx, nz):
        to_x, to_z = (x + dx) % nx, (z + dz) % nz
        pltpu.make_async_remote_copy(
            src_ref=ar_own, dst_ref=ar_all.at[mine], send_sem=ar_sem.at[0], recv_sem=ar_sem.at[1],
            device_id=(g, to_x, to_z), device_id_type=MESH).start()
    ar_all[mine] = row
    rest = ar_all.at[pl.ds(0, nx * nz - 1)]
    pltpu.make_async_copy(rest, rest, ar_sem.at[1]).wait()
    total = ar_all[...].reshape(nx, nz, 1, LANES)
    total = jnp.sum(jnp.sum(total, axis=0), axis=0)

    total = jnp.broadcast_to(total, (SUB, LANES))

    def entry(i, k):
        lane = SUB * i + k
        return jnp.broadcast_to(total[:, lane:lane + 1], (SUB, LANES))

    system = {(i, k): entry(i, k) for k in range(ITERS) for i in range(k + 1)}
    right = [entry(ITERS, k) for k in range(ITERS)]
    inverse = []
    for p in range(ITERS):
        inverse.append(1.0 / system[p, p])
        for i in range(p + 1, ITERS):
            factor = system[p, i] * inverse[p]
            for k in range(i, ITERS):
                system[i, k] = system[i, k] - factor * system[p, k]
            right[i] = right[i] - factor * right[p]
    a = [None] * ITERS
    for p in reversed(range(ITERS)):
        value = right[p]
        for k in range(p + 1, ITERS):
            value = value - system[p, k] * a[k]
        a[p] = value * inverse[p]
    b = [None] * FIELDS
    b[0] = 1.0 - a[0] + 0.5 * a[1]
    for k in range(1, ITERS - 1):
        b[k] = 0.5 * (a[k - 1] + a[k + 1]) - a[k]
    b[ITERS - 1] = 0.5 * a[ITERS - 2] - a[ITERS - 1]
    b[ITERS] = 0.5 * a[ITERS - 1]
    def combine(j, carry):
        for t in range(TILES):
            fields = [wbuf[k + 1, j + 1, :, t] for k in range(FIELDS)]
            up = a[0][None] * fields[0]
            down = b[0][None] * fields[0]
            for k in range(1, ITERS):
                up = up + a[k][None] * fields[k]
                down = down + b[k][None] * fields[k]
            down = down + b[ITERS][None] * fields[ITERS]
            put(out_x, j, t, icbuf[j, :, t] * up)
            put(out_r, j, t, gbuf[j, :, t] * down)
        return carry

    lax.fori_loop(0, CHUNKS, combine, 0)
    def left(kind, condition, whole):
        @pl.when(condition)
        def _():
            pltpu.make_async_copy(whole, whole, send_sem.at[kind]).wait()

    both = beside_x * beside_z
    left(0, beside_x == 2, hx)
    left(0, beside_x == 1, hx.at[:, :, 0])
    left(1, beside_z == 2, hz)
    left(1, beside_z == 1, hz.at[:, :, 0])
    left(2, both == 4, hc)
    left(2, both == 2, hc.at[:, :, pl.ds(0, 2)])
    left(2, both == 1, hc.at[:, :, 0])
    pltpu.make_async_copy(rest, rest, ar_sem.at[0]).wait()


def on_device(nx, nz, forcing, conduct, diag_add, ice_mask, grounded):
    field = (CHUNKS, ROWS, TILES, SUB, LANES)
    native = (TILES, LAYERS * ROWS, LANES)
    wide = TILES * LANES
    hbm_space = pl.BlockSpec(memory_space=pltpu.HBM)
    vmem_space = pl.BlockSpec(memory_space=pltpu.VMEM)
    out = jax.ShapeDtypeStruct(native, F32)
    vmem = pltpu.VMEM
    flat = lambda array: array.reshape(LAYERS * ROWS, wide)
    outs = pl.pallas_call(
        functools.partial(kernel, nx, nz),
        out_shape=(out, out),
        in_specs=[hbm_space] * 5,
        out_specs=(vmem_space, vmem_space),
        scratch_shapes=[
            vmem((SUB, CHUNKS * ROWS, wide), jnp.bfloat16),
            vmem((LAYERS * ROWS, wide), jnp.bfloat16),
            vmem((ROWS, wide), jnp.int32),
            vmem((ROWS, wide), jnp.int32),
            vmem((ROWS, wide), F32),
            vmem(native, F32),
            vmem(native, F32),
            vmem(native, F32),
            vmem((COUPLING + 1, CHUNKS + 2, ROWS, TILES, SUB, LANES), F32),
            vmem((FIELDS, CHUNKS, 2, 2, TILES, SUB, LANES), F32),
            vmem((FIELDS, CHUNKS, 2, SUB, LANES), F32),
            vmem((CORNERED, CHUNKS, 4, 1, LANES), F32),
            vmem((FIELDS, CHUNKS, SUB, LANES), F32),
            vmem((FIELDS, CHUNKS, 1, LANES), F32),
            vmem(field, F32),
            vmem(field, F32),
            vmem(field, F32),
            vmem(field, F32),
            vmem((FIELDS, CHUNKS + 2, 2, SUB, LANES), F32),
            vmem((CHUNKS, 2, SUB, LANES), F32),
            vmem((ROWS, TILES, SUB, LANES), F32),
            vmem((SUB, SUB, SUB, LANES), F32),
            vmem((TILES, ROWS, LANES), F32),
            vmem((TILES, ROWS, LANES), F32),
            vmem((1, LANES), F32),
            vmem((nx * nz, 1, LANES), F32),
            pltpu.SemaphoreType.DMA((7,)),
            pltpu.SemaphoreType.DMA((3,)),
            pltpu.SemaphoreType.DMA((2, CHUNKS, 2)),
            pltpu.SemaphoreType.DMA((2, CHUNKS)),
            pltpu.SemaphoreType.DMA((4, 2)),
            pltpu.SemaphoreType.DMA((2,)),
            pltpu.SemaphoreType.DMA((2,)),
            pltpu.SemaphoreType.REGULAR,
        ],
        compiler_params=pltpu.CompilerParams(collective_id=0, has_side_effects=True, vmem_limit_bytes=40 * 1024 * 1024),
        name="coupled_solve",
    )(*[pltpu.with_memory_space_constraint(v, pltpu.HBM)
        for v in (flat(forcing), conduct.reshape(SUB, CHUNKS * ROWS, wide), flat(diag_add), ice_mask, grounded)])
    return tuple(
        v.reshape(TILES, LAYERS, ROWS, LANES).transpose(1, 2, 0, 3).reshape(1, LAYERS, ROWS, wide)
        for v in outs)


def solution(mesh):
    block = P("group", None, "gx", "gy")
    columns = P("gx", "gy")
    return jax.shard_map(
        functools.partial(on_device, mesh.shape["gx"], mesh.shape["gy"]),
        mesh=mesh,
        in_specs=(block, block, block, columns, columns),
        out_specs=(block, block),
        check_vma=False,
    )
```

```python
import functools

import jax
import jax.numpy as jnp
from jax import lax
from jax.experimental import pallas as pl
from jax.experimental.pallas import tpu as pltpu
from jax.sharding import PartitionSpec as P

ITERS = 6
FIELDS = ITERS + 1
CORNERED = FIELDS - 1
COUPLING = FIELDS + 1
LAYERS = 80
ROWS = 8
SUB = 8
LANES = 128
TILES = 2
CHUNKS = LAYERS // SUB
HALF = CHUNKS // 2
MESH = pl.DeviceIdType.MESH
F32 = jnp.float32

far_weight = 0.25
cross_weight = 0.5
vertical_weight = 4.0
friction_gain = 8.0

STEPS = ((-1, 0), (1, 0), (0, -1), (0, 1), (-1, -1), (-1, 1), (1, -1), (1, 1))


def roll(value, shift, axis=None):
    return pltpu.roll(value, shift % value.shape[-1 if axis is None else axis],
                      value.ndim - 1 if axis is None else axis)


def far_first(nx, nz):
    def hops(step):
        dx, dz = step
        return min(dx % 4, -dx % 4) + min(dx // 4, 4 - dx // 4) + min(dz, nz - dz)

    steps = [(dx, dz) for dx in range(nx) for dz in range(nz)]
    return sorted(steps[1:], key=lambda step: -hops(step))


def kernel(
    nx, nz,
    forcing, conduct, diag_add, ice_mask, grounded, out_x, out_r,
    cbf, dbf, ice_v, ground_v, active_v, fs, cn, dn,
    wbuf, hx, hz, hc, pz, pc, ebuf, hbuf, icbuf, gbuf, wcbuf, ecbuf, abuf, acc,
    shared_out, shared_in, ar_own, ar_all,
    in_sem, send_sem, recv_sem, corner_sem, half_sem, share_sem, ar_sem, far_sem,
):
    g = lax.axis_index("group")
    x = lax.axis_index("gx")
    z = lax.axis_index("gy")

    lane2 = lax.broadcasted_iota(jnp.int32, (SUB, LANES), 1)
    sub2 = lax.broadcasted_iota(jnp.int32, (SUB, LANES), 0)
    lane3 = lax.broadcasted_iota(jnp.int32, (ROWS, SUB, LANES), 2)
    sub3 = lax.broadcasted_iota(jnp.int32, (ROWS, SUB, LANES), 1)
    lane1 = lax.broadcasted_iota(jnp.int32, (1, LANES), 1)

    beside_x = (x > 0).astype(jnp.int32) + (x < nx - 1).astype(jnp.int32)
    beside_z = (z > 0).astype(jnp.int32) + (z < nz - 1).astype(jnp.int32)

    def exists(d):
        dx, dz = STEPS[d]
        conds = []
        if dx < 0:
            conds.append(x > 0)
        if dx > 0:
            conds.append(x < nx - 1)
        if dz < 0:
            conds.append(z > 0)
        if dz > 0:
            conds.append(z < nz - 1)
        return functools.reduce(jnp.logical_and, conds)

    def at(d):
        dx, dz = STEPS[d]
        return (g, x + dx, z + dz)

    barrier = pltpu.get_barrier_semaphore()
    pl.semaphore_signal(barrier, inc=1, device_id=(g, (x + nx // 2) % nx, z), device_id_type=MESH)
    for d in (4, 5, 6, 7, 0, 1, 2, 3):
        @pl.when(exists(d))
        def _(d=d):
            pl.semaphore_signal(barrier, inc=1, device_id=at(d), device_id_type=MESH)
    pl.semaphore_signal(barrier, inc=1, device_id=(1 - g, x, z), device_id_type=MESH)

    loads = [
        pltpu.make_async_copy(conduct.at[:, pl.ds(0, ROWS)], cbf.at[:, pl.ds(0, ROWS)], in_sem.at[0]),
        pltpu.make_async_copy(ice_mask, ice_v, in_sem.at[1]),
        pltpu.make_async_copy(grounded, ground_v, in_sem.at[2]),
        pltpu.make_async_copy(forcing.at[:, pl.ds(0, LANES)], fs.at[0], in_sem.at[3]),
        pltpu.make_async_copy(forcing.at[:, pl.ds(LANES, LANES)], fs.at[1], in_sem.at[4]),
        pltpu.make_async_copy(diag_add, dbf, in_sem.at[5]),
        pltpu.make_async_copy(conduct.at[:, pl.ds(ROWS, LAYERS - ROWS)], cbf.at[:, pl.ds(ROWS, LAYERS - ROWS)], in_sem.at[6]),
    ]
    for n in (0, 1, 2, 6, 3, 4, 5):
        loads[n].start()

    def zero_rims(d):
        @pl.when(jnp.logical_not(exists(d)))
        def _():
            def body(e, carry):
                if d < 2:
                    for j in range(CHUNKS):
                        hx[e, j, d] = jnp.zeros((2, TILES, SUB, LANES), F32)
                elif d < 4:
                    hz[e, :, d - 2] = jnp.zeros((CHUNKS, SUB, LANES), F32)
                else:
                    hc[e, :, d - 4] = jnp.zeros((CHUNKS, 1, LANES), F32)
                return carry
            lax.fori_loop(0, FIELDS if d < 4 else CORNERED, body, 0)

    for d in range(8):
        zero_rims(d)

    acc[...] = jnp.zeros_like(acc)

    def clear(f, carry):
        for j in range(CHUNKS):
            wbuf[f, j + 1] = jnp.zeros((ROWS, TILES, SUB, LANES), F32)
        return carry

    lax.fori_loop(0, FIELDS + 1, clear, 0)
    wcbuf[0] = jnp.zeros((CHUNKS + 2, 2, SUB, LANES), F32)

    loads[0].wait()
    loads[1].wait()
    loads[2].wait()
    is_ice = jnp.where(g == 0, 1.0, 0.0).astype(F32)
    ice = ice_v[...].astype(F32)
    ground = ground_v[...].astype(F32)
    active_v[...] = ice * (1.0 - (1.0 - is_ice) * ground)

    def pick(ref, j, t):
        return jnp.stack([ref[t, pl.ds(j * ROWS + r, SUB, stride=CHUNKS * ROWS), :] for r in range(ROWS)])

    def couple(j):
        rows = pl.ds(pl.multiple_of(j * ROWS, ROWS), ROWS)
        base = pl.multiple_of(j * SUB * ROWS, SUB * ROWS)
        parts = []
        for t in range(TILES):
            columns = slice(t * LANES, (t + 1) * LANES)
            value = jnp.sqrt(cbf[:, rows, columns].astype(F32)) * active_v[:, columns][None]
            cn[t, pl.ds(base, SUB * ROWS)] = value.reshape(SUB * ROWS, LANES)
        for t in range(TILES):
            parts.append(jnp.stack([cn[t, pl.ds(base + r, SUB, stride=ROWS), :] for r in range(ROWS)]))
        return parts

    def put(ref, j, t, value):
        for r in range(ROWS):
            ref[t, pl.ds(j * ROWS + r, SUB, stride=CHUNKS * ROWS), :] = value[r]

    def copies(e, j, d):
        f = COUPLING if isinstance(e, int) and e == 0 else e
        if d == 0:
            src, dst = wbuf.at[f, j + 1, pl.ds(0, 2)], hx.at[e, j, 1]
        elif d == 1:
            src, dst = wbuf.at[f, j + 1, pl.ds(ROWS - 2, 2)], hx.at[e, j, 0]
        elif d < 4:
            src, dst = pz.at[e, j], hz.at[e, j, 3 - d]
        else:
            src, dst = pc.at[e, j], hc.at[e, j, 7 - d]
        return pltpu.make_async_remote_copy(
            src_ref=src, dst_ref=dst, send_sem=send_sem.at[min(d // 2, 2)],
            recv_sem=recv_sem.at[e % 2, j, d // 2] if d < 4 else corner_sem.at[e % 2, j],
            device_id=at(d), device_id_type=MESH)

    def store_field(f, j, parts):
        store_chunk(f, j, parts)
        store_ends(f, j, parts)

    def store_chunk(f, j, parts):
        for t in range(TILES):
            wbuf[f, j + 1, :, t] = parts[t]

    def store_ends(f, j, parts):
        @pl.when(j == 0)
        def _():
            for t in range(TILES):
                wbuf[f, CHUNKS + 1, :, t] = jnp.where(sub3 < SUB - 1, roll(parts[t], SUB - 1, 1), 0.0)

        @pl.when(j == CHUNKS - 1)
        def _():
            for t in range(TILES):
                wbuf[f, 0, :, t] = jnp.where(sub3 > 0, roll(parts[t], 1, 1), 0.0)

    def store_corners(f, j, corners):
        for p in range(2):
            wcbuf[f, j + 1, p] = corners[p]

        @pl.when(j == 0)
        def _():
            for p in range(2):
                wcbuf[f, CHUNKS + 1, p] = jnp.where(sub2 < SUB - 1, roll(corners[p], SUB - 1, 0), 0.0)

        @pl.when(j == CHUNKS - 1)
        def _():
            for p in range(2):
                wcbuf[f, 0, p] = jnp.where(sub2 > 0, roll(corners[p], 1, 0), 0.0)

    def pack_rims(e, j, parts, raw=None, ahead=True, scale=None):
        none = jnp.zeros((1, SUB, LANES), F32)
        crossed, scaled = [], []
        for t in range(TILES):
            wide = jnp.concatenate([none, parts[t], none], axis=0)
            crossed.append(parts[t] + cross_weight * (wide[0:8] + wide[2:10]))
            scaled.append(far_weight * parts[t])
        sources = (
            (jnp.where(lane3 == LANES - 1, crossed[1], 0.0), 1),
            (jnp.where(lane3 == 0, crossed[0], 0.0), -1),
            (jnp.where(lane3 >= LANES - 2, scaled[1], 0.0), 2),
            (jnp.where(lane3 < 2, scaled[0], 0.0), -2),
        )
        packed = None
        for source, shift in sources:
            for r in range(ROWS):
                moved = roll(source[r], 4 * (r + 1) + shift)
                packed = moved if packed is None else packed + moved
        for base, row, inner in ((0, 0, 1), (4 * (ROWS + 1), ROWS - 1, ROWS - 2)):
            for tile, lane, way in ((1, LANES - 1, 1), (0, 0, -1)):
                straight = parts[tile][row] + far_weight * parts[tile][inner]
                packed = packed + roll(jnp.where(lane2 == lane, straight, 0.0), base + way)
                across = jnp.where(lane2 == lane - way, cross_weight * parts[tile][row], 0.0)
                packed = packed + roll(across, base + 2 * way)
        pz[e, j] = packed
        moved = []

        def place(value, lane, target):
            only = jnp.where(lane2 == lane, value, 0.0)
            moved.append(pltpu.roll(only, (target - lane) % LANES, 1, stride=1, stride_axis=0))

        for q in range(4):
            tile = q % 2
            lane, way = ((0, 1), (LANES - 1, -1))[tile]
            edge, one, two = ((0, 1, 2), (ROWS - 1, ROWS - 2, ROWS - 3))[q // 2]
            field = parts[tile]
            if raw is not None:
                place(field[edge], lane, 8 * q)
            if ahead:
                place(field[one] + far_weight * field[two], lane, 32 + 8 * q)
                place(field[edge] + cross_weight * field[one], lane + way, 32 + 8 * q)
                place(far_weight * field[edge], lane + 2 * way, 32 + 8 * q)
            if scale is not None:
                place(scale[tile][edge], lane, 64 + 8 * q)
        pc[e, j] = jnp.sum(functools.reduce(jnp.add, moved), axis=0, keepdims=True)

    def send_rims(e, j, directions, wanted=None):
        for d in directions:
            @pl.when(exists(d) if wanted is None else jnp.logical_and(exists(d), wanted))
            def _(d=d):
                copies(e, j, d).start()

    ALONG_X, BESIDE = (0, 1), (2, 3, 4, 5, 6, 7)

    def arrive(semaphore, condition, whole):
        @pl.when(condition)
        def _():
            pltpu.make_async_copy(whole, whole, semaphore).wait()

    def await_rims(e, j):
        arrive(recv_sem.at[e % 2, j, 0], beside_x == 2, hx.at[e, j])
        arrive(recv_sem.at[e % 2, j, 0], beside_x == 1, hx.at[e, j, 0])
        arrive(recv_sem.at[e % 2, j, 1], beside_z == 2, hz.at[e, j])
        arrive(recv_sem.at[e % 2, j, 1], beside_z == 1, hz.at[e, j, 0])

    def await_corners(e, j):
        both = beside_x * beside_z
        arrive(corner_sem.at[e % 2, j], both == 4, hc.at[e, j])
        arrive(corner_sem.at[e % 2, j], both == 2, hc.at[e, j, pl.ds(0, 2)])
        arrive(corner_sem.at[e % 2, j], both == 1, hc.at[e, j, 0])

    def await_half(e, half, wanted):
        both, part = beside_x * beside_z, pl.ds(half * HALF, HALF)
        semaphore = half_sem.at[e % 4, half]
        arrive(semaphore, jnp.logical_and(both == 4, wanted), hc.at[e, part])
        arrive(semaphore, jnp.logical_and(both == 2, wanted), hc.at[e, part, pl.ds(0, 2)])
        arrive(semaphore, jnp.logical_and(both == 1, wanted), hc.at[e, part, 0])

    def send_half(e, half, wanted):
        part = pl.ds(half * HALF, HALF)
        for d in range(4, 8):
            @pl.when(jnp.logical_and(exists(d), wanted))
            def _(d=d):
                pltpu.make_async_remote_copy(
                    src_ref=pc.at[e, part], dst_ref=hc.at[e, part, 7 - d],
                    send_sem=send_sem.at[2], recv_sem=half_sem.at[e % 4, half],
                    device_id=at(d), device_id_type=MESH).start()

    def corner_values(e, j, base):
        values = []
        for q in range(4):
            here = lane2 == base + 8 * (3 - q) + sub2
            picked = jnp.where(here, jnp.broadcast_to(hc[e, j, q], (SUB, LANES)), 0.0)
            values.append(jnp.sum(picked, axis=1, keepdims=True))
        return [at_ends(jnp.broadcast_to(values[2 * p], (SUB, LANES)),
                        jnp.broadcast_to(values[2 * p + 1], (SUB, LANES))) for p in range(2)]

    def at_ends(low, high):
        return jnp.where(lane2 == 0, low, jnp.where(lane2 == LANES - 1, high, 0.0))

    def next_corners(k, j):
        e = k - 1
        alone = corner_values(e, j, 32)
        edge = jnp.where(lane2 % 4 < 2, hz[e, j, 0], hz[e, j, 1])
        corners = []
        for p in range(2):
            near = [hx[e, j, p, 1 - p, t] for t in range(TILES)]
            outer = [hx[e, j, p, p, t] for t in range(TILES)]
            row = p * (ROWS - 1)
            total = at_ends(near[0], near[1]) + cross_weight * at_ends(outer[0], outer[1])
            total = total + far_weight * at_ends(roll(near[0], -1), roll(near[1], 1))
            total = total + cross_weight * at_ends(wbuf[e, j + 1, row, 0], wbuf[e, j + 1, row, 1])
            beyond = edge if p == 0 else roll(edge, -4 * (ROWS + 1))
            total = total + at_ends(beyond, beyond) + alone[p]
            total = total + vertical_weight * (wcbuf[k - 1, j, p] + wcbuf[k - 1, j + 2, p])
            corners.append(ecbuf[j, p] * total - wcbuf[k - 2, j + 1, p])
        return corners

    def spread(f, e, j, corners):
        centre = [wbuf[f, j + 1, :, t] for t in range(TILES)]
        beside, mixed, scaled = [], [], []
        for t in range(TILES):
            wide = jnp.concatenate([hx[e, j, 0, :, t], centre[t], hx[e, j, 1, :, t]], axis=0)
            near = wide[1:9] + wide[3:11]
            far = wide[0:8] + wide[4:12]
            vertical = wbuf[f, j, :, t] + wbuf[f, j + 2, :, t]
            beside.append(near + far_weight * far + vertical_weight * vertical)
            mixed.append(centre[t] + cross_weight * near)
            scaled.append(far_weight * centre[t])
        for source, shift in ((mixed, 1), (scaled, 2)):
            a, b = roll(source[0], shift), roll(source[1], shift)
            beside[0] = beside[0] + jnp.where(lane3 < shift, 0.0, a)
            beside[1] = beside[1] + jnp.where(lane3 < shift, a, b)
            a, b = roll(source[0], -shift), roll(source[1], -shift)
            beside[0] = beside[0] + jnp.where(lane3 >= LANES - shift, b, a)
            beside[1] = beside[1] + jnp.where(lane3 >= LANES - shift, 0.0, b)

        edge = jnp.where(lane2 % 4 < 2, hz[e, j, 0], hz[e, j, 1])
        rows = [roll(edge, -4 * (r + 1)) for r in range(ROWS)]
        corners = corners() if callable(corners) else corners
        rows[0] = rows[0] + cross_weight * corners[0]
        rows[-1] = rows[-1] + cross_weight * corners[1]
        rows = jnp.stack(rows)
        return [beside[0] + jnp.where(lane3 < 2, rows, 0.0),
                beside[1] + jnp.where(lane3 >= LANES - 2, rows, 0.0)]

    def dots(k, j, applied):
        field = [wbuf[k + 1, j + 1, :, t] for t in range(TILES)]
        weighted = [hbuf[j, :, t] * (field[t] - 0.5 * applied[t]) for t in range(TILES)]
        for i in range(ITERS):
            product = [jnp.sum(weighted[t] * wbuf[i + 1, j + 1, :, t], axis=0) for t in range(TILES)]
            acc[k, i] = acc[k, i] + (product[0] + product[1])
        product = [jnp.sum(hbuf[j, :, t] * field[t] * wbuf[1, j + 1, :, t], axis=0) for t in range(TILES)]
        acc[k, ITERS] = acc[k, ITERS] + (product[0] + product[1])

    def first(j):
        parts = couple(j)
        store_field(COUPLING, j, parts)
        pack_rims(0, j, parts, raw=True, ahead=False)

    def first_and_send(j, carry):
        first(j)
        send_rims(0, j, BESIDE + ALONG_X)
        return carry

    first(jnp.int32(0))
    pl.semaphore_wait(barrier, 2 + beside_x + beside_z + beside_x * beside_z)
    send_rims(0, jnp.int32(0), BESIDE[2:] + BESIDE[:2] + ALONG_X)
    loads[6].wait()
    lax.fori_loop(1, CHUNKS, first_and_send, 0)

    loads[3].wait()
    loads[4].wait()
    edge = pl.ds(pl.multiple_of(g * ((LAYERS - 1) * ROWS), ROWS), ROWS)
    for t in range(TILES):
        mean = jnp.sum(fs[t].reshape(LAYERS, ROWS, LANES), axis=0) * (1.0 / LAYERS)
        value = active_v[:, t * LANES:(t + 1) * LANES] * mean
        shared_out[t] = value * cn[t, edge]
    share = pltpu.make_async_remote_copy(
        src_ref=shared_out, dst_ref=shared_in, send_sem=share_sem.at[0], recv_sem=share_sem.at[1],
        device_id=(1 - g, x, z), device_id_type=MESH)
    share.start()
    loads[5].wait()

    def widen(i, carry):
        part = pl.ds(pl.multiple_of(i * SUB * ROWS, SUB * ROWS), SUB * ROWS)
        for t in range(TILES):
            dn[t, part] = dbf[part, t * LANES:(t + 1) * LANES].astype(F32)
        return carry

    lax.fori_loop(0, CHUNKS, widen, 0)
    for t in range(TILES):
        columns = slice(t * LANES, (t + 1) * LANES)
        friction = is_ice * friction_gain * (ground_v[:, columns].astype(F32) * ice_v[:, columns].astype(F32))
        dn[t, 0:ROWS] = dn[t, 0:ROWS] + friction

    def turn(source, target):
        def body(j, carry):
            for t in range(TILES):
                target[j, :, t] = pick(source, j, t)
            return carry

        lax.fori_loop(0, CHUNKS, body, 0)

    turn(dn, gbuf)
    share.wait()
    for t in range(TILES):
        fs[t, edge] = fs[t, edge] + shared_in[t]
    turn(fs, hbuf)

    def second(j, late):
        def fetch():
            await_corners(0, j)
            return corner_values(0, j, 0)

        await_rims(0, j)
        spreads = spread(COUPLING, 0, j, fetch if late else fetch())
        couplings = [wbuf[COUPLING, j + 1, :, t] for t in range(TILES)]
        diagonals = [gbuf[j, :, t] + couplings[t] * spreads[t] for t in range(TILES)]
        ratios = [couplings[t] / diagonals[t] for t in range(TILES)]
        parts = [ratios[t] * hbuf[j, :, t] for t in range(TILES)]
        store_field(1, j, parts)
        scale = [2.0 * ratios[t] * couplings[t] for t in range(TILES)]
        pack_rims(1, j, parts, raw=True, scale=scale)
        for t in range(TILES):
            c = couplings[t]
            inverse_c = jnp.where(c > 0.0, 1.0 / jnp.where(c > 0.0, c, 1.0), 0.0)
            back = diagonals[t] * inverse_c
            ebuf[j, :, t] = scale[t]
            icbuf[j, :, t] = inverse_c
            gbuf[j, :, t] = back
            hbuf[j, :, t] = back * inverse_c
        send_rims(1, j, BESIDE[2:] + BESIDE[:2] + ALONG_X)

    def chunks(step):
        def body(j, carry):
            step(j, False)
            return carry

        step(jnp.int32(0), True)
        lax.fori_loop(1, CHUNKS, body, 0)

    chunks(second)

    def stage(k, place):
        def step(j, late):
            if not late:
                await_rims(k, j)
            held = []

            def fetch():
                await_corners(k, j)
                held.extend(corner_values(k, j, 0))
                return held

            if place == "first":
                corners = fetch if late else fetch()
            else:
                ahead = jnp.bool_(True) if place == "last" else k > 2
                if late:
                    await_half(k - 1, 0, ahead)
                else:
                    await_half(k - 1, 1, jnp.logical_and(ahead, j == HALF))
                corners = next_corners(k, j)
            if late:
                if place != "first":
                    store_corners(k, j, corners)
                await_rims(k, j)
            spreads = spread(k, k, j, corners)
            applied = [ebuf[j, :, t] * spreads[t] for t in range(TILES)]
            parts = [applied[t] - wbuf[k - 1, j + 1, :, t] for t in range(TILES)]
            if place == "last":
                for t in range(TILES):
                    wbuf[k + 1, j + 1, :, t] = parts[t]
                dots(k - 1, j, applied)
                return
            if not late:
                rest(j - 1)
            store_chunk(k + 1, j, parts)
            if not late:
                store_ends(k + 1, j, parts)
            send_rims(k + 1, j, ALONG_X)
            if late:
                store_ends(k + 1, j, parts)
            for t in range(TILES):
                abuf[:, t] = applied[t]
            if place == "first":
                scales = corner_values(k, j, 64)
                for p in range(2):
                    ecbuf[j, p] = scales[p]
                store_corners(k, j, held)
            elif not late:
                store_corners(k, j, corners)
            if not late:
                send_rims(k + 1, j - 1, BESIDE[:2])
                send_half(k + 1, 0, jnp.logical_and(j == HALF, sends_corners))

        def rest(j):
            pack_rims(k + 1, j, [wbuf[k + 1, j + 1, :, t] for t in range(TILES)])
            dots(k - 1, j, [abuf[:, t] for t in range(TILES)])

        sends_corners = jnp.bool_(True) if place == "first" else k < ITERS - 1
        chunks(step)
        if place != "last":
            final = jnp.int32(CHUNKS - 1)
            rest(final)
            send_rims(k + 1, final, BESIDE[:2])
            send_half(k + 1, 1, sends_corners)

    def middle(k, carry):
        stage(k, "middle")
        return carry

    stage(1, "first")
    lax.fori_loop(2, ITERS, middle, 0)
    far = {(0, nz // 2)} | {(a * nx // 4, 0) for a in range(4)} | {(nx // 2, nz // 2)}
    far = sorted(far - {(0, 0)})
    for dx, dz in far:
        pl.semaphore_signal(
            far_sem, inc=1, device_id=(g, (x + dx) % nx, (z + dz) % nz), device_id_type=MESH)
    stage(ITERS, "last")
    pl.semaphore_wait(far_sem, len(far))

    gram = jnp.zeros((SUB, LANES), F32)
    for k in range(ITERS):
        column = jnp.sum(jnp.sum(acc[k], axis=1), axis=1, keepdims=True)
        wanted = (lane2 == SUB * sub2 + k) & ((sub2 <= k) | (sub2 == ITERS))
        gram = gram + jnp.where(wanted, column, 0.0)
    row = jnp.sum(gram, axis=0, keepdims=True)
    ar_own[...] = row
    mine = x * nz + z
    for dx, dz in far_first(nx, nz):
        to_x, to_z = (x + dx) % nx, (z + dz) % nz
        pltpu.make_async_remote_copy(
            src_ref=ar_own, dst_ref=ar_all.at[mine], send_sem=ar_sem.at[0], recv_sem=ar_sem.at[1],
            device_id=(g, to_x, to_z), device_id_type=MESH).start()
    ar_all[mine] = row
    rest = ar_all.at[pl.ds(0, nx * nz - 1)]
    pltpu.make_async_copy(rest, rest, ar_sem.at[1]).wait()
    total = ar_all[...].reshape(nx, nz, 1, LANES)
    total = jnp.sum(jnp.sum(total, axis=0), axis=0)

    total = jnp.broadcast_to(total, (SUB, LANES))

    def entry(i, k):
        lane = SUB * i + k
        return jnp.broadcast_to(total[:, lane:lane + 1], (SUB, LANES))

    system = {(i, k): entry(i, k) for k in range(ITERS) for i in range(k + 1)}
    right = [entry(ITERS, k) for k in range(ITERS)]
    inverse = []
    for p in range(ITERS):
        inverse.append(1.0 / system[p, p])
        for i in range(p + 1, ITERS):
            factor = system[p, i] * inverse[p]
            for k in range(i, ITERS):
                system[i, k] = system[i, k] - factor * system[p, k]
            right[i] = right[i] - factor * right[p]
    a = [None] * ITERS
    for p in reversed(range(ITERS)):
        value = right[p]
        for k in range(p + 1, ITERS):
            value = value - system[p, k] * a[k]
        a[p] = value * inverse[p]
    b = [None] * FIELDS
    b[0] = 1.0 - a[0] + 0.5 * a[1]
    for k in range(1, ITERS - 1):
        b[k] = 0.5 * (a[k - 1] + a[k + 1]) - a[k]
    b[ITERS - 1] = 0.5 * a[ITERS - 2] - a[ITERS - 1]
    b[ITERS] = 0.5 * a[ITERS - 1]
    def combine(j, carry):
        for t in range(TILES):
            fields = [wbuf[k + 1, j + 1, :, t] for k in range(FIELDS)]
            up = a[0][None] * fields[0]
            down = b[0][None] * fields[0]
            for k in range(1, ITERS):
                up = up + a[k][None] * fields[k]
                down = down + b[k][None] * fields[k]
            down = down + b[ITERS][None] * fields[ITERS]
            put(out_x, j, t, icbuf[j, :, t] * up)
            put(out_r, j, t, gbuf[j, :, t] * down)
        return carry

    lax.fori_loop(0, CHUNKS, combine, 0)
    def left(kind, condition, whole):
        @pl.when(condition)
        def _():
            pltpu.make_async_copy(whole, whole, send_sem.at[kind]).wait()

    both = beside_x * beside_z
    left(0, beside_x == 2, hx)
    left(0, beside_x == 1, hx.at[:, :, 0])
    left(1, beside_z == 2, hz)
    left(1, beside_z == 1, hz.at[:, :, 0])
    left(2, both == 4, hc)
    left(2, both == 2, hc.at[:, :, pl.ds(0, 2)])
    left(2, both == 1, hc.at[:, :, 0])
    pltpu.make_async_copy(rest, rest, ar_sem.at[0]).wait()


def on_device(nx, nz, forcing, conduct, diag_add, ice_mask, grounded):
    field = (CHUNKS, ROWS, TILES, SUB, LANES)
    native = (TILES, LAYERS * ROWS, LANES)
    wide = TILES * LANES
    hbm_space = pl.BlockSpec(memory_space=pltpu.HBM)
    vmem_space = pl.BlockSpec(memory_space=pltpu.VMEM)
    out = jax.ShapeDtypeStruct(native, F32)
    vmem = pltpu.VMEM
    flat = lambda array: array.reshape(LAYERS * ROWS, wide)
    outs = pl.pallas_call(
        functools.partial(kernel, nx, nz),
        out_shape=(out, out),
        in_specs=[hbm_space] * 5,
        out_specs=(vmem_space, vmem_space),
        scratch_shapes=[
            vmem((SUB, CHUNKS * ROWS, wide), jnp.bfloat16),
            vmem((LAYERS * ROWS, wide), jnp.bfloat16),
            vmem((ROWS, wide), jnp.int32),
            vmem((ROWS, wide), jnp.int32),
            vmem((ROWS, wide), F32),
            vmem(native, F32),
            vmem(native, F32),
            vmem(native, F32),
            vmem((COUPLING + 1, CHUNKS + 2, ROWS, TILES, SUB, LANES), F32),
            vmem((FIELDS, CHUNKS, 2, 2, TILES, SUB, LANES), F32),
            vmem((FIELDS, CHUNKS, 2, SUB, LANES), F32),
            vmem((CORNERED, CHUNKS, 4, 1, LANES), F32),
            vmem((FIELDS, CHUNKS, SUB, LANES), F32),
            vmem((FIELDS, CHUNKS, 1, LANES), F32),
            vmem(field, F32),
            vmem(field, F32),
            vmem(field, F32),
            vmem(field, F32),
            vmem((FIELDS, CHUNKS + 2, 2, SUB, LANES), F32),
            vmem((CHUNKS, 2, SUB, LANES), F32),
            vmem((ROWS, TILES, SUB, LANES), F32),
            vmem((SUB, SUB, SUB, LANES), F32),
            vmem((TILES, ROWS, LANES), F32),
            vmem((TILES, ROWS, LANES), F32),
            vmem((1, LANES), F32),
            vmem((nx * nz, 1, LANES), F32),
            pltpu.SemaphoreType.DMA((7,)),
            pltpu.SemaphoreType.DMA((3,)),
            pltpu.SemaphoreType.DMA((2, CHUNKS, 2)),
            pltpu.SemaphoreType.DMA((2, CHUNKS)),
            pltpu.SemaphoreType.DMA((4, 2)),
            pltpu.SemaphoreType.DMA((2,)),
            pltpu.SemaphoreType.DMA((2,)),
            pltpu.SemaphoreType.REGULAR,
        ],
        compiler_params=pltpu.CompilerParams(collective_id=0, has_side_effects=True, vmem_limit_bytes=40 * 1024 * 1024),
        name="coupled_solve",
    )(*[pltpu.with_memory_space_constraint(v, pltpu.HBM)
        for v in (flat(forcing), conduct.reshape(SUB, CHUNKS * ROWS, wide), flat(diag_add), ice_mask, grounded)])
    return tuple(
        v.reshape(TILES, LAYERS, ROWS, LANES).transpose(1, 2, 0, 3).reshape(1, LAYERS, ROWS, wide)
        for v in outs)


def solution(mesh):
    block = P("group", None, "gx", "gy")
    columns = P("gx", "gy")
    return jax.shard_map(
        functools.partial(on_device, mesh.shape["gx"], mesh.shape["gy"]),
        mesh=mesh,
        in_specs=(block, block, block, columns, columns),
        out_specs=(block, block),
        check_vma=False,
    )
```
